32 devices in a mesh: gx: 4 (over y, core), yz: 8 (over z, x).
Axes of the slice: x: 2, y: 2, z: 4, core: 2. Of those that a mesh axis runs over, the one named last changes fastest.
Arguments:
- gas_state: float32 [5, 64, 128, 256], P(None, 'gx', 'yz'), may hold values from -6 to 6
- parcel_speed: float32 [4, 8, 32, 4, 3, 128], P('gx', 'yz'), may hold values from -6 to 6
- parcel_mass: float32 [4, 8, 32, 4, 128], P('gx', 'yz'), may hold values from 0.3 to 3
- offsets: float32 [4, 8, 32, 4, 3, 128], P('gx', 'yz'), may hold values from 0 to 1
- cell_base: int32 [4, 8, 32, 4, 3, 128], P('gx', 'yz'), may hold values from 0 to 6, as said below
- block_tile: int32 [4, 8, 32, 4], P('gx', 'yz'), may hold values from 0 to 511
- block_count: int32 [4, 8, 32], P('gx', 'yz'), may hold values from 0 to 4, as said below
Outputs:
- gas_next: float32 [5, 64, 128, 256], P(None, 'gx', 'yz')
- speed_next: float32 [4, 8, 32, 4, 3, 128], P('gx', 'yz')
- mass_next: float32 [4, 8, 32, 4, 128], P('gx', 'yz')
The draws below stay inside these ranges and needn't reach their ends.
Inputs may be any that keep to these rules, and one draw needn't show every extreme that they name: `block_count`: A device's live blocks for an owner are its first ones; in every draw some owner receives 4 live blocks from every device. `cell_base`: component 0, 1, 2 is at most 2, 2, 6, so that the base cell and the next cell along each dimension lie in the tile.
All inputs are finite; a program needn't handle non-finite values.
Results may differ from the reference program's by a relative error of at most 0.0003.
Values sent between devices are 32-bit elements; how exact they have to be, the bound alone decides.
No kernel may reach another device: no remote copies, remote signals or barrier semaphores. Data moves between devices by JAX's collectives and lax.ppermute only.
A program may use at most 128 MiB of HBM per device.

```python
import math
import jax
import jax.numpy as jnp
from jax import lax

CX = 16
CY = 16
NZ = 256
CAP = 4
PB = 128
TILE_X = 4
TILE_Y = 4
TILE_Z = 8
NX = 64
NY = 128
TILES_DEV = 512
N_GX = 4
N_YZ = 8
DEVICES = 32


def draw_cell_base(key, part):
    folded = jax.random.fold_in(key, 11)
    raw = jax.random.randint(folded, (N_GX, N_YZ, DEVICES, CAP, 3, PB), 0, 1 << 20, dtype=jnp.int32)
    limits = jnp.array([TILE_X - 1, TILE_Y - 1, TILE_Z - 1], dtype=jnp.int32).reshape(3, 1)
    return raw % limits


def draw_block_count(key, part):
    folded = jax.random.fold_in(key, 23)
    first_key, second_key = jax.random.split(folded)
    owners = jnp.arange(DEVICES, dtype=jnp.int32)
    row_index = owners // N_YZ
    col_index = owners % N_YZ
    heat = N_GX - row_index + (N_YZ // 2 - jnp.abs(col_index - N_YZ // 2))
    ceiling = N_GX + N_YZ // 2
    raw = jax.random.randint(first_key, (N_GX, N_YZ, DEVICES), 0, 2 * CAP + 2, dtype=jnp.int32)
    counted = jnp.minimum(CAP, raw * heat // ceiling)
    chosen = jax.random.randint(second_key, (), 0, DEVICES, dtype=jnp.int32)
    return jnp.where(owners == chosen, CAP, counted).astype(jnp.int32)


def with_ends(result, stream_key, least, top_value):
    place = [jax.random.randint(jax.random.fold_in(stream_key, axis), (), 0, length) for axis, length in enumerate(result.shape)]
    main_axis = result.shape.index(max(result.shape))
    next_to = place[:main_axis] + [(place[main_axis] + 1) % result.shape[main_axis]] + place[main_axis + 1:]
    return result.at[tuple(place)].set(least).at[tuple(next_to)].set(top_value)


def shard_levels(own_key, shape, cuts, smallest, top_value):
    loudness, own = 1.0, jax.random.fold_in(own_key, 6)
    for dim, blocks in cuts:
        steps = jnp.exp(jax.random.uniform(jax.random.fold_in(own, dim), (blocks,), jnp.float32, smallest / len(cuts), top_value / len(cuts)))
        loudness = loudness * jnp.repeat(steps, shape[dim] // blocks).reshape([-1 if axis == dim else 1 for axis in range(len(shape))])
    return loudness


def bell_draw(stream_key, dims, deviation, limit, cuts=(), kind=jnp.bfloat16):
    result = deviation * jax.random.normal(stream_key, dims, jnp.float32)
    if cuts:
        result = result * shard_levels(stream_key, dims, cuts, -0.22, 0.18)
    return jnp.clip(result, -limit, limit).astype(kind)


def setup_inputs(seed: int = 0) -> dict:
    streams_of = jax.random.split(jax.random.key(seed), 8)
    gas_state = bell_draw(streams_of[0], (5, NX, NY, NZ), 1.0, 6.0, ((1, 4), (2, 8)), jnp.float32)
    parcel_speed = bell_draw(streams_of[1], (N_GX, N_YZ, DEVICES, CAP, 3, PB), 1.0, 6.0, ((0, 4), (1, 8)), jnp.float32)
    parcel_mass = jnp.clip(jnp.exp(math.log(3.0) - 2.3025851 * jax.random.uniform(streams_of[2], (N_GX, N_YZ, DEVICES, CAP, PB), jnp.float32) ** shard_levels(streams_of[2], (N_GX, N_YZ, DEVICES, CAP, PB), ((0, 4), (1, 8)), -0.2, 0.2)), 0.3, 3.0)
    offsets = jnp.clip(1.0 * jax.random.uniform(streams_of[3], (N_GX, N_YZ, DEVICES, CAP, 3, PB), jnp.float32) ** shard_levels(streams_of[3], (N_GX, N_YZ, DEVICES, CAP, 3, PB), ((0, 4), (1, 8)), -0.2, 0.2), 0.0, 1.0)
    cell_base = draw_cell_base(jax.random.fold_in(streams_of[7], 71), 0)
    block_tile = with_ends(jax.random.randint(streams_of[5], (N_GX, N_YZ, DEVICES, CAP), 0, TILES_DEV), jax.random.fold_in(streams_of[5], 1), 0, TILES_DEV - 1).astype(jnp.int32)
    block_count = draw_block_count(jax.random.fold_in(streams_of[7], 71), 0)
    return dict(gas_state=gas_state, parcel_speed=parcel_speed, parcel_mass=parcel_mass, offsets=offsets, cell_base=cell_base, block_tile=block_tile, block_count=block_count)


DIFFUSION = 0.1
CELL_MASS = 4.0
DRAG_RATE = 0.5
EVAPORATION = 0.3
LATENT_HEAT = 2.0


def split_tiles(block):
    fields, extent_x, extent_y, extent_z = block.shape
    grid = block.reshape(fields, extent_x // TILE_X, TILE_X, extent_y // TILE_Y, TILE_Y, extent_z // TILE_Z, TILE_Z)
    grid = grid.transpose(1, 3, 5, 0, 2, 4, 6)
    return grid.reshape(-1, fields, TILE_X * TILE_Y * TILE_Z)


def join_tiles(tile_data, extent_x, extent_y, extent_z):
    fields = tile_data.shape[1]
    grid = tile_data.reshape(extent_x // TILE_X, extent_y // TILE_Y, extent_z // TILE_Z, fields, TILE_X, TILE_Y, TILE_Z)
    return grid.transpose(3, 0, 4, 1, 5, 2, 6).reshape(fields, extent_x, extent_y, extent_z)


def laplace(padded):
    framed = jnp.pad(padded, ((0, 0), (0, 0), (0, 0), (1, 1)))
    centre = framed[:, 1:-1, 1:-1, 1:-1]
    beside_all = framed[:, 2:, 1:-1, 1:-1] + framed[:, :-2, 1:-1, 1:-1]
    beside_all = beside_all + framed[:, 1:-1, 2:, 1:-1] + framed[:, 1:-1, :-2, 1:-1]
    beside_all = beside_all + framed[:, 1:-1, 1:-1, 2:] + framed[:, 1:-1, 1:-1, :-2]
    return beside_all - 6.0 * centre


def weights_along(fraction, base_cell, extent):
    positions = jnp.arange(extent, dtype=jnp.int32)
    lower_hit = (base_cell[..., None] == positions).astype(jnp.float32)
    upper_hit = (base_cell[..., None] + 1 == positions).astype(jnp.float32)
    return (1.0 - fraction)[..., None] * lower_hit + fraction[..., None] * upper_hit


def parcel_update(tile_data, velocity, shifts, cells, mass_old, live):
    along_x = weights_along(shifts[:, 0], cells[:, 0], TILE_X)
    along_y = weights_along(shifts[:, 1], cells[:, 1], TILE_Y)
    along_z = weights_along(shifts[:, 2], cells[:, 2], TILE_Z)
    stencil = along_x[:, :, :, None, None] * along_y[:, :, None, :, None] * along_z[:, :, None, None, :]
    stencil = stencil.reshape(mass_old.shape + (TILE_X * TILE_Y * TILE_Z,))
    sampled = jnp.einsum("scq,spq->scp", tile_data, stencil, precision=lax.Precision.HIGHEST)
    radius = jnp.cbrt(mass_old)
    factor = DRAG_RATE / (radius * radius)
    alive = live > 0.5
    moved = (velocity + factor[:, None, :] * sampled[:, 0:3]) / (1.0 + factor[:, None, :])
    velocity_new = jnp.where(alive[:, None, None], moved, velocity)
    evap_loss = EVAPORATION * jax.nn.softplus(sampled[:, 3] - sampled[:, 4]) / radius
    mass_new = jnp.where(alive[:, None], mass_old / (1.0 + evap_loss), mass_old)
    vapour = mass_old - mass_new
    momentum = mass_old[:, None, :] * (velocity - velocity_new) + vapour[:, None, :] * velocity_new
    source = jnp.concatenate([momentum, -LATENT_HEAT * vapour[:, None, :], vapour[:, None, :]], axis=1)
    source = source * live[:, None, None]
    deposit = jnp.einsum("scp,spq->scq", source, stencil, precision=lax.Precision.HIGHEST)
    return velocity_new, mass_new, deposit


def reference(gas_state, parcel_speed, parcel_mass, offsets, cell_base, block_tile, block_count):
    blocks = gas_state.reshape(5, N_GX, CX, N_YZ, CY, NZ).transpose(1, 3, 0, 2, 4, 5).reshape(DEVICES, 5, CX, CY, NZ)
    all_tiles = jax.vmap(split_tiles)(blocks)
    owners = jnp.arange(DEVICES, dtype=jnp.int32)[:, None]
    slot_total = DEVICES * CAP

    def per_source(packed):
        velocity, mass_old, shifts, cells, tile_index, counted = packed
        chosen = all_tiles[owners, tile_index]
        live = (jnp.arange(CAP, dtype=jnp.int32)[None, :] < counted[:, None]).astype(jnp.float32)
        velocity_new, mass_new, deposit = parcel_update(
            chosen.reshape((slot_total,) + chosen.shape[2:]),
            velocity.reshape((slot_total,) + velocity.shape[2:]),
            shifts.reshape((slot_total,) + shifts.shape[2:]),
            cells.reshape((slot_total,) + cells.shape[2:]),
            mass_old.reshape((slot_total,) + mass_old.shape[2:]),
            live.reshape(slot_total))
        return velocity_new.reshape(velocity.shape), mass_new.reshape(mass_old.shape), deposit.reshape(chosen.shape)

    block_index = block_tile.reshape(DEVICES, DEVICES, CAP)
    packed = (parcel_speed.reshape(DEVICES, DEVICES, CAP, 3, PB),
              parcel_mass.reshape(DEVICES, DEVICES, CAP, PB),
              offsets.reshape(DEVICES, DEVICES, CAP, 3, PB),
              cell_base.reshape(DEVICES, DEVICES, CAP, 3, PB),
              block_index,
              block_count.reshape(DEVICES, DEVICES))
    speed_out, mass_out, deposits = lax.map(per_source, packed)
    targets = owners[None, :, :] * TILES_DEV + block_index
    summed = jax.ops.segment_sum(deposits.reshape(-1, 5, TILE_X * TILE_Y * TILE_Z), targets.reshape(-1),
                                 num_segments=DEVICES * TILES_DEV)

    def join_owner(tile_data):
        return join_tiles(tile_data, CX, CY, NZ)

    source_blocks = jax.vmap(join_owner)(summed.reshape(DEVICES, TILES_DEV, 5, -1))
    source_field = source_blocks.reshape(N_GX, N_YZ, 5, CX, CY, NZ).transpose(2, 0, 3, 1, 4, 5).reshape(5, NX, NY, NZ)
    padded = jnp.pad(gas_state, ((0, 0), (1, 1), (1, 1), (0, 0)))
    gas_next = gas_state + DIFFUSION * laplace(padded) + source_field / CELL_MASS
    return gas_next, speed_out.reshape(parcel_speed.shape), mass_out.reshape(parcel_mass.shape)
```

```python
import functools

import jax
import jax.numpy as jnp
from jax import lax
from jax.experimental import pallas as pl
from jax.experimental.pallas import tpu as pltpu
from jax.sharding import PartitionSpec as P

TILE_X = 4
TILE_Y = 4
TILE_Z = 8
DIFFUSION = 0.1
CELL_MASS = 4.0
DRAG_RATE = 0.5
EVAPORATION = 0.3
LATENT_HEAT = 2.0

LANES = 128
SUB = 8
GRANULES = LANES // TILE_Z
FLOWS = 4
BOTH = ("gx", "yz")


def roll(x, shift, axis):
    size = x.shape[axis]
    shift = shift % size
    return pltpu.roll(x, shift, axis) if shift else x


def exchange(upper, lower):
    row = lax.broadcasted_iota(jnp.int32, (SUB, LANES), 0)
    column = lax.broadcasted_iota(jnp.int32, (SUB, LANES), 1) // TILE_Z
    right = (column & 8) != 0
    half = LANES // 2
    pair = [jnp.where(right, roll(lower, half, 1), upper), jnp.where(right, lower, roll(upper, half, 1))]
    for step in (4, 2, 1):
        row_bit = (row & step) != 0
        column_bit = (column & step) != 0
        same = row_bit == column_bit
        for place in range(2):
            x = pair[place]
            from_below = roll(roll(x, -step, 0), TILE_Z * step, 1)
            from_above = roll(roll(x, step, 0), -TILE_Z * step, 1)
            pair[place] = jnp.where(same, x, jnp.where(column_bit, from_below, from_above))
    return pair


def pack_kernel(speed, mass, offsets, cells, tile_ids, counts, message, *, rows):
    devices, capacity = speed.shape[:2]
    group = SUB * rows
    lane = lax.broadcasted_iota(jnp.int32, (1, capacity), 1)

    def per_group(g, carry):
        part = message.at[pl.ds(pl.multiple_of(g * group, SUB), group)]
        for i in range(SUB):
            d = g * SUB + i
            base = i * rows
            for k in range(capacity):
                part[base + 3 * k : base + 3 * k + 3, :] = speed[d, k]
                part[base + 12 + 3 * k : base + 15 + 3 * k, :] = offsets[d, k]
                part[base + 24 + 3 * k : base + 27 + 3 * k, :] = cells[d, k].astype(jnp.float32)
            part[base + 36 : base + 40, :] = mass[d]
            ids = jnp.where(lane < counts[d], tile_ids[pl.ds(d, 1), :], -1)
            part[base + 40 : base + 41, 0:capacity] = ids.astype(jnp.float32)
        return carry

    lax.fori_loop(0, devices // SUB, per_group, 0)


def table_kernel(gas, table, face_x0, face_x1, face_y0, face_y1):
    fields, extent_x, extent_y, extent_z = gas.shape
    across_y = extent_y // TILE_Y
    across_z = extent_z // TILE_Z
    face_x0[...] = gas[:, 0]
    face_x1[...] = gas[:, extent_x - 1]
    face_y0[...] = gas[:, :, 0, :]
    face_y1[...] = gas[:, :, extent_y - 1, :]

    def per_a(a, carry):
        for f in range(FLOWS):
            for b in range(across_y):
                for h in range(extent_z // LANES):
                    lanes = slice(h * LANES, (h + 1) * LANES)
                    rows = slice(b * TILE_Y, (b + 1) * TILE_Y)
                    parts = []
                    for u in range(TILE_X):
                        piece = gas[f, a * TILE_X + u, rows, lanes]
                        if f == 3:
                            piece = piece - gas[4, a * TILE_X + u, rows, lanes]
                        parts.append(piece)
                    pair = exchange(jnp.concatenate(parts[:2], 0), jnp.concatenate(parts[2:], 0))
                    start = pl.multiple_of((a * across_y + b) * across_z + h * GRANULES, SUB)
                    table[f, pl.ds(start, SUB), :] = pair[0]
                    table[f, pl.ds(start + SUB, SUB), :] = pair[1]
        return carry

    lax.fori_loop(0, extent_x // TILE_X, per_a, 0)


def update_kernel(message, table, result, source, ids_out, ids_vmem, ids_smem, products, sem, *, rows, capacity):
    devices = message.shape[0] // rows
    group = SUB * rows
    for g in range(devices // SUB):
        ids_vmem[g * SUB : (g + 1) * SUB, :] = message[pl.ds(g * group + 40, SUB, stride=rows), :].astype(jnp.int32)
    ids_out[...] = ids_vmem[...]
    copy = pltpu.make_async_copy(ids_vmem, ids_smem, sem)
    copy.start()
    copy.wait()
    corner = lax.broadcasted_iota(jnp.int32, (SUB, LANES), 0)
    high = [(corner & bit) != 0 for bit in (4, 2, 1)]
    least = [jnp.where(h, 0.0, 1.0) for h in high]
    slope = [jnp.where(h, 1.0, -1.0) for h in high]
    shift = (
        jnp.where(high[0], TILE_Y * TILE_Z, 0) + jnp.where(high[1], TILE_Z, 0) + jnp.where(high[2], 1, 0)
    )
    row = corner

    def per_group(g, carry):
        part = message.at[pl.ds(pl.multiple_of(g * group, SUB), group)]
        for step in range(SUB // 2):
            alive = jnp.zeros((SUB, LANES), jnp.int32)
            for j in range(2 * capacity):
                i, k = 2 * step + j // capacity, j % capacity
                base = i * rows
                tile = ids_smem[g * SUB + i, k]
                alive = jnp.where(row == j, tile, alive)
                safe = jnp.maximum(tile, 0)
                weight = None
                for dim in range(3):
                    fraction = part[base + 12 + 3 * k + dim : base + 13 + 3 * k + dim, :]
                    along = least[dim] + slope[dim] * fraction
                    weight = along if weight is None else weight * along
                cell = part[base + 24 + 3 * k : base + 27 + 3 * k, :].astype(jnp.int32)
                first = (cell[0:1] * TILE_Y + cell[1:2]) * TILE_Z + cell[2:3]
                index = first + shift
                for f in range(FLOWS):
                    held = jnp.broadcast_to(table[f, pl.ds(safe, 1), :], (SUB, LANES))
                    found = jnp.take_along_axis(held, index, axis=1, mode="promise_in_bounds")
                    products[(f * SUB + j) * SUB : (f * SUB + j + 1) * SUB, :] = found * weight
            live = alive >= 0
            sampled = []
            for f in range(FLOWS):
                total = products[pl.ds(f * SUB * SUB, SUB, stride=SUB), :]
                for c in range(1, SUB):
                    total = total + products[pl.ds(f * SUB * SUB + c, SUB, stride=SUB), :]
                sampled.append(total)

            def both(offset, stride):
                return jnp.concatenate(
                    [
                        part[pl.ds((2 * step + n) * rows + offset, capacity, stride=stride), :]
                        for n in range(2)
                    ],
                    axis=0,
                )

            mass_old = both(36, 1)
            radius = jnp.exp(jnp.log(mass_old) * (1.0 / 3.0))
            factor = DRAG_RATE / (radius * radius)
            share = 1.0 / (1.0 + factor)
            gap = sampled[3]
            soft = jnp.maximum(gap, 0.0) + jnp.log(1.0 + jnp.exp(-jnp.abs(gap)))
            mass_new = jnp.where(live, mass_old / (1.0 + EVAPORATION * soft / radius), mass_old)
            vapour = mass_old - mass_new
            fields, sources = [], []
            for f in range(3):
                velocity = both(f, 3)
                moved = jnp.where(live, (velocity + factor * sampled[f]) * share, velocity)
                fields.append(moved)
                sources.append(mass_old * (velocity - moved) + vapour * moved)
            fields.append(mass_new)
            sources.append(vapour)
            for dim in range(3):
                sources.append(both(12 + dim, 3) + both(24 + dim, 3))
            first_block = (g * SUB + 2 * step) * capacity
            out = result.at[pl.ds(pl.multiple_of(first_block * FLOWS, SUB), SUB * FLOWS)]
            for f in range(FLOWS):
                out[pl.ds(f, SUB, stride=FLOWS), :] = fields[f]
            out = source.at[pl.ds(pl.multiple_of(first_block * SUB, SUB), SUB * SUB)]
            for f in range(7):
                out[pl.ds(f, SUB, stride=SUB), :] = sources[f]
        return carry

    lax.fori_loop(0, devices // SUB, per_group, 0)


def tent(position, cell):
    return jnp.maximum(0.0, 1.0 - jnp.abs(position - cell))


def deposit_kernel(ids, source, gas, from_x0, from_x1, from_y0, from_y1, gas_next, total, *, capacity):
    fields, extent_x, extent_y, extent_z = gas.shape
    across_y = extent_y // TILE_Y
    across_z = extent_z // TILE_Z
    blocks = source.shape[0] // SUB
    total[...] = jnp.zeros(total.shape, total.dtype)
    row = lax.broadcasted_iota(jnp.int32, (SUB, LANES), 0)
    along_z = row.astype(jnp.float32)
    along_y = (row % TILE_Y).astype(jnp.float32)
    along_x = (row // TILE_Y).astype(jnp.float32)

    def one(n):
        tile = jnp.maximum(ids[n // capacity, n % capacity], 0)
        held = source[pl.ds(pl.multiple_of(n * SUB, SUB), SUB), :]
        given = held[0:FLOWS]
        coarse = given.astype(jnp.bfloat16).astype(jnp.float32)
        left = jnp.concatenate([given, given - coarse], axis=0).astype(jnp.bfloat16)
        x, y, z = held[4:5], held[5:6], held[6:7]
        weight_z = tent(z, along_z)
        weight_y = tent(y, along_y)
        planes = []
        for part in range(2):
            weight_xy = tent(x, along_x + 2.0 * part) * weight_y
            for i in range(SUB):
                planes.append(weight_xy[i : i + 1] * weight_z)
        stencil = jnp.concatenate(planes, axis=0)
        high = stencil.astype(jnp.bfloat16)
        low = (stencil - high.astype(jnp.float32)).astype(jnp.bfloat16)
        right = jnp.concatenate([high, low], axis=0)
        sums = lax.dot_general(left, right, (((1,), (1,)), ((), ())), preferred_element_type=jnp.float32)
        return pl.multiple_of(tile * SUB, SUB), sums[:, :LANES] + sums[:, LANES:]

    unroll = 4

    def per_step(step, carry):
        made = [one(step * unroll + n) for n in range(unroll)]
        for start, sums in made:
            total[pl.ds(start, SUB), :] += sums
        return carry

    lax.fori_loop(0, blocks // unroll, per_step, 0)

    last_z = extent_z - 1
    lane = lax.broadcasted_iota(jnp.int32, (extent_y, extent_z), 1)
    line = lax.broadcasted_iota(jnp.int32, (extent_y, extent_z), 0)

    def per_field(f, carry):
        for x in range(extent_x):
            centre = gas[f, x]
            before = from_x0[f] if x == 0 else gas[f, x - 1]
            after = from_x1[f] if x == extent_x - 1 else gas[f, x + 1]
            beside = before + after
            beside += jnp.where(line == 0, from_y0[f, x : x + 1, :], roll(centre, 1, 0))
            beside += jnp.where(line == extent_y - 1, from_y1[f, x : x + 1, :], roll(centre, -1, 0))
            beside += jnp.where(lane == 0, 0.0, roll(centre, 1, 1))
            beside += jnp.where(lane == last_z, 0.0, roll(centre, -1, 1))
            gas_next[f, x] = centre + DIFFUSION * (beside - 6.0 * centre)
        return carry

    lax.fori_loop(0, fields, per_field, 0)

    def per_a(a, carry):
        for f in range(FLOWS):
            for b in range(across_y):
                for h in range(extent_z // LANES):
                    start = ((a * across_y + b) * across_z + h * GRANULES) * SUB
                    part = total.at[pl.ds(pl.multiple_of(start, SUB), GRANULES * SUB)]
                    pair = [
                        part[pl.ds(n * SUB * SUB + f, SUB, stride=SUB), :]
                        + part[pl.ds(n * SUB * SUB + f + FLOWS, SUB, stride=SUB), :]
                        for n in range(2)
                    ]
                    pair = exchange(*pair)
                    lanes = slice(h * LANES, (h + 1) * LANES)
                    lines = slice(b * TILE_Y, (b + 1) * TILE_Y)
                    for u in range(TILE_X):
                        piece = pair[u // 2][(u % 2) * TILE_Y : (u % 2 + 1) * TILE_Y]
                        piece = piece * (1.0 / CELL_MASS)
                        x = a * TILE_X + u
                        if f < 3:
                            gas_next[f, x, lines, lanes] += piece
                        else:
                            gas_next[3, x, lines, lanes] += -LATENT_HEAT * piece
                            gas_next[4, x, lines, lanes] += piece
        return carry

    lax.fori_loop(0, extent_x // TILE_X, per_a, 0)


def call(kernel, name, out_shape, in_specs=None, scratch=(), flops=0, moved=0):
    extra = {} if in_specs is None else {"in_specs": in_specs}
    return pl.pallas_call(
        kernel,
        out_shape=out_shape,
        scratch_shapes=scratch,
        name=name,
        cost_estimate=pl.CostEstimate(flops=flops, bytes_accessed=moved, transcendentals=0),
        compiler_params=pltpu.CompilerParams(vmem_limit_bytes=32 * 1024 * 1024),
        **extra,
    )


def vmem():
    return pl.BlockSpec(memory_space=pltpu.VMEM)


def smem():
    return pl.BlockSpec(memory_space=pltpu.SMEM)


def shards(gas_state, parcel_speed, parcel_mass, offsets, cell_base, block_tile, block_count):
    fields, extent_x, extent_y, extent_z = gas_state.shape
    devices, capacity = block_tile.shape[2:]
    rows = 10 * capacity + 1
    tiles = (extent_x // TILE_X) * (extent_y // TILE_Y) * (extent_z // TILE_Z)
    f32 = jnp.float32

    def shape(*dims, dtype=f32):
        return jax.ShapeDtypeStruct(dims, dtype)

    message = call(
        functools.partial(pack_kernel, rows=rows),
        "pack",
        shape(devices * rows, LANES),
        [vmem()] * 5 + [smem()],
    )(parcel_speed[0, 0], parcel_mass[0, 0], offsets[0, 0], cell_base[0, 0], block_tile[0, 0], block_count[0, 0])
    message = lax.all_to_all(message.reshape(devices, rows, 1, LANES), BOTH, split_axis=0, concat_axis=0, tiled=True)
    message = message.reshape(devices * rows, LANES)

    face = shape(fields, extent_x, extent_z)
    table, face_x0, face_x1, face_y0, face_y1 = call(
        table_kernel,
        "table",
        (shape(FLOWS, tiles, LANES), shape(fields, extent_y, extent_z), shape(fields, extent_y, extent_z), face, face),
        flops=10**7,
    )(gas_state)

    def shifted(value, axis, step):
        count = lax.axis_size(axis)
        pairs = [(i, i + step) for i in range(count) if 0 <= i + step < count]
        return lax.ppermute(value, axis, pairs)

    from_x0 = shifted(face_x1, "gx", 1)
    from_x1 = shifted(face_x0, "gx", -1)
    from_y0 = shifted(face_y1, "yz", 1)
    from_y1 = shifted(face_y0, "yz", -1)

    blocks = devices * capacity
    result, source, ids = call(
        functools.partial(update_kernel, rows=rows, capacity=capacity),
        "update",
        (shape(blocks * FLOWS, LANES), shape(blocks * SUB, LANES), shape(devices, LANES, dtype=jnp.int32)),
        scratch=[
            pltpu.VMEM((devices, LANES), jnp.int32),
            pltpu.SMEM((devices, LANES), jnp.int32),
            pltpu.VMEM((FLOWS * SUB * SUB, LANES), f32),
            pltpu.SemaphoreType.DMA(()),
        ],
        flops=10**7,
    )(message, table)
    result = lax.all_to_all(
        result.reshape(devices, capacity * FLOWS, LANES), BOTH, split_axis=0, concat_axis=0, tiled=True
    )
    gas_next = call(
        functools.partial(deposit_kernel, capacity=capacity),
        "deposit",
        shape(*gas_state.shape),
        [smem()] + [vmem()] * 6,
        scratch=[pltpu.VMEM((tiles * SUB, LANES), f32)],
        flops=3 * 10**7,
    )(ids, source, gas_state, from_x0, from_x1, from_y0, from_y1)
    result = result.reshape(devices, capacity, FLOWS, LANES)
    return gas_next, result[:, :, :3].reshape(parcel_speed.shape), result[:, :, 3].reshape(parcel_mass.shape)


def solution(mesh):
    in_specs = (
        P(None, "gx", "yz", None),
        P("gx", "yz", None, None, None, None),
        P("gx", "yz", None, None, None),
        P("gx", "yz", None, None, None, None),
        P("gx", "yz", None, None, None, None),
        P("gx", "yz", None, None),
        P("gx", "yz", None),
    )
    out_specs = (
        P(None, "gx", "yz", None),
        P("gx", "yz", None, None, None, None),
        P("gx", "yz", None, None, None),
    )
    return jax.shard_map(shards, mesh=mesh, in_specs=in_specs, out_specs=out_specs, check_vma=False)
```

```python
import functools

import jax
import jax.numpy as jnp
from jax import lax
from jax.experimental import pallas as pl
from jax.experimental.pallas import tpu as pltpu
from jax.sharding import PartitionSpec as P

TILE_X = 4
TILE_Y = 4
TILE_Z = 8
DIFFUSION = 0.1
CELL_MASS = 4.0
DRAG_RATE = 0.5
EVAPORATION = 0.3
LATENT_HEAT = 2.0

LANES = 128
SUB = 8
GRANULES = LANES // TILE_Z
FLOWS = 4
BOTH = ("gx", "yz")


def roll(x, shift, axis):
    shift = shift % x.shape[axis]
    return pltpu.roll(x, shift, axis) if shift else x


def pick(x, rows):
    return jnp.take_along_axis(x, rows, axis=0, mode="promise_in_bounds")


def exchange(upper, lower):
    row = lax.broadcasted_iota(jnp.int32, (SUB, LANES), 0)
    granule = lax.broadcasted_iota(jnp.int32, (SUB, LANES), 1) // TILE_Z
    half = LANES // 2
    turned = [
        pltpu.roll(x, shift, 1, stride=TILE_Z, stride_axis=0) for x, shift in ((upper, 0), (lower, half))
    ]
    back = SUB - 1 - row
    pair = []
    for part in range(2):
        wanted = (granule - back - SUB * part) % GRANULES
        mixed = jnp.where(wanted < SUB, pick(turned[0], wanted % SUB), pick(turned[1], wanted % SUB))
        shift = (-TILE_Z * (SUB - 1) - half * part) % LANES
        pair.append(pick(pltpu.roll(mixed, shift, 1, stride=TILE_Z, stride_axis=0), back))
    return pair


def pack_kernel(speed, mass, offsets, cells, tile_ids, counts, message, *, rows, capacity):
    group = SUB * rows
    vector = 3 * capacity
    owners = tile_ids.shape[1]
    slot = lax.broadcasted_iota(jnp.int32, tile_ids.shape, 0)
    ids = jnp.where(slot < counts[...], tile_ids[...], -1).astype(jnp.float32)
    ids = jnp.concatenate([ids, jnp.zeros((LANES - capacity, owners), jnp.float32)], axis=0).T

    for g in range(owners // SUB):
        for i in range(SUB):
            d = g * SUB + i
            base = d * rows
            message[base : base + vector, :] = speed[d * vector : (d + 1) * vector, :]
            message[base + vector : base + 2 * vector, :] = offsets[d * vector : (d + 1) * vector, :]
            message[base + 2 * vector : base + 3 * vector, :] = cells[d * vector : (d + 1) * vector, :].astype(jnp.float32)
            message[base + 3 * vector : base + 3 * vector + capacity, :] = mass[d * capacity : (d + 1) * capacity, :]
            message[base + rows - 1 : base + rows, :] = ids[d : d + 1, :]


def table_kernel(gas, table, face_x0, face_x1, face_y0, face_y1):
    fields, extent_x, extent_y, extent_z = gas.shape
    across_y = extent_y // TILE_Y
    across_z = extent_z // TILE_Z
    face_x0[...] = gas[:, 0]
    face_x1[...] = gas[:, extent_x - 1]
    face_y0[...] = gas[:, :, 0, :]
    face_y1[...] = gas[:, :, extent_y - 1, :]

    def per_a(a, carry):
        for f in range(FLOWS):
            for b in range(across_y):
                for h in range(extent_z // LANES):
                    lanes = slice(h * LANES, (h + 1) * LANES)
                    rows = slice(b * TILE_Y, (b + 1) * TILE_Y)
                    parts = []
                    for u in range(TILE_X):
                        piece = gas[f, a * TILE_X + u, rows, lanes]
                        if f == 3:
                            piece = piece - gas[4, a * TILE_X + u, rows, lanes]
                        parts.append(piece)
                    pair = exchange(jnp.concatenate(parts[:2], 0), jnp.concatenate(parts[2:], 0))
                    start = pl.multiple_of((a * across_y + b) * across_z + h * GRANULES, SUB)
                    table[f, pl.ds(start, SUB), :] = pair[0]
                    table[f, pl.ds(start + SUB, SUB), :] = pair[1]
        return carry

    lax.fori_loop(0, extent_x // TILE_X, per_a, 0)


def update_kernel(message, table, result, source, ids_out, ids_vmem, ids_smem, products, sem, *, rows, capacity):
    devices = message.shape[0] // rows
    group = SUB * rows
    for g in range(devices // SUB):
        ids_vmem[g * SUB : (g + 1) * SUB, :] = message[pl.ds(g * group + rows - 1, SUB, stride=rows), :].astype(jnp.int32)
    ids_out[...] = ids_vmem[...]
    copy = pltpu.make_async_copy(ids_vmem, ids_smem, sem)
    copy.start()
    copy.wait()
    corner = lax.broadcasted_iota(jnp.int32, (SUB, LANES), 0)
    high = [(corner & bit) != 0 for bit in (4, 2, 1)]
    least = [jnp.where(h, 0.0, 1.0) for h in high]
    slope = [jnp.where(h, 1.0, -1.0) for h in high]
    shift = (
        jnp.where(high[0], TILE_Y * TILE_Z, 0) + jnp.where(high[1], TILE_Z, 0) + jnp.where(high[2], 1, 0)
    )
    row = corner

    def per_group(g, carry):
        part = message.at[pl.ds(pl.multiple_of(g * group, SUB), group)]
        for step in range(SUB // 2):
            alive = jnp.zeros((SUB, LANES), jnp.int32)
            for j in range(2 * capacity):
                i, k = 2 * step + j // capacity, j % capacity
                base = i * rows
                tile = ids_smem[g * SUB + i, k]
                alive = jnp.where(row == j, tile, alive)
                safe = jnp.maximum(tile, 0)
                weight = None
                for dim in range(3):
                    start = base + (3 + dim) * capacity + k
                    fraction = part[start : start + 1, :]
                    along = least[dim] + slope[dim] * fraction
                    weight = along if weight is None else weight * along
                cell = [part[base + (6 + dim) * capacity + k, :][None] for dim in range(3)]
                first = (cell[0] * TILE_Y + cell[1]) * TILE_Z + cell[2]
                index = first.astype(jnp.int32) + shift
                for f in range(FLOWS):
                    held = jnp.broadcast_to(table[f, pl.ds(safe, 1), :], (SUB, LANES))
                    found = jnp.take_along_axis(held, index, axis=1, mode="promise_in_bounds")
                    products[(f * SUB + j) * SUB : (f * SUB + j + 1) * SUB, :] = found * weight
            live = alive >= 0
            sampled = []
            for f in range(FLOWS):
                total = products[pl.ds(f * SUB * SUB, SUB, stride=SUB), :]
                for c in range(1, SUB):
                    total = total + products[pl.ds(f * SUB * SUB + c, SUB, stride=SUB), :]
                sampled.append(total)

            def both(field):
                starts = [(2 * step + n) * rows + field * capacity for n in range(2)]
                return jnp.concatenate([part[start : start + capacity, :] for start in starts], axis=0)

            mass_old = both(9)
            radius = jnp.exp(jnp.log(mass_old) * (1.0 / 3.0))
            factor = DRAG_RATE / (radius * radius)
            share = 1.0 / (1.0 + factor)
            gap = sampled[3]
            soft = jnp.maximum(gap, 0.0) + jnp.log(1.0 + jnp.exp(-jnp.abs(gap)))
            mass_new = jnp.where(live, mass_old / (1.0 + EVAPORATION * soft / radius), mass_old)
            vapour = mass_old - mass_new
            fields, sources = [], []
            for f in range(3):
                velocity = both(f)
                moved = jnp.where(live, (velocity + factor * sampled[f]) * share, velocity)
                fields.append(moved)
                sources.append(mass_old * (velocity - moved) + vapour * moved)
            fields.append(mass_new)
            sources.append(vapour)
            for dim in range(3):
                sources.append(both(3 + dim) + both(6 + dim))
            first_block = (g * SUB + 2 * step) * capacity
            out = result.at[pl.ds(pl.multiple_of(first_block * FLOWS, SUB), SUB * FLOWS)]
            for n in range(2):
                for f in range(FLOWS):
                    start = (n * FLOWS + f) * capacity
                    out[start : start + capacity, :] = fields[f][n * capacity : (n + 1) * capacity]
            out = source.at[pl.ds(pl.multiple_of(first_block * SUB, SUB), SUB * SUB)]
            for f in range(7):
                out[pl.ds(f, SUB, stride=SUB), :] = sources[f]
        return carry

    lax.fori_loop(0, devices // SUB, per_group, 0)


def tent(position, cell):
    return jnp.maximum(0.0, 1.0 - jnp.abs(position - cell))


def diffuse_kernel(gas, from_x0, from_x1, from_y0, from_y1, diffused):
    fields, extent_x, extent_y, extent_z = gas.shape
    lane = lax.broadcasted_iota(jnp.int32, (extent_y, extent_z), 1)
    line = lax.broadcasted_iota(jnp.int32, (extent_y, extent_z), 0)

    def per_field(f, carry):
        for x in range(extent_x):
            centre = gas[f, x]
            before = from_x0[f] if x == 0 else gas[f, x - 1]
            after = from_x1[f] if x == extent_x - 1 else gas[f, x + 1]
            beside = before + after
            beside += jnp.where(line == 0, from_y0[f, x : x + 1, :], roll(centre, 1, 0))
            beside += jnp.where(line == extent_y - 1, from_y1[f, x : x + 1, :], roll(centre, -1, 0))
            beside += jnp.where(lane == 0, 0.0, roll(centre, 1, 1))
            beside += jnp.where(lane == extent_z - 1, 0.0, roll(centre, -1, 1))
            diffused[f, x] = centre + DIFFUSION * (beside - 6.0 * centre)
        return carry

    lax.fori_loop(0, fields, per_field, 0)


def deposit_kernel(ids_vmem, source, diffused, gas_next, total, ids, sem, *, capacity):
    fields, extent_x, extent_y, extent_z = diffused.shape
    across_y = extent_y // TILE_Y
    across_z = extent_z // TILE_Z
    blocks = source.shape[0] // SUB
    copy = pltpu.make_async_copy(ids_vmem, ids, sem)
    copy.start()
    total[...] = jnp.zeros(total.shape, total.dtype)
    row = lax.broadcasted_iota(jnp.int32, (SUB, LANES), 0)
    along_z = row.astype(jnp.float32)
    along_y = (row % TILE_Y).astype(jnp.float32)
    along_x = (row // TILE_Y).astype(jnp.float32)
    copy.wait()

    def one(n):
        tile = jnp.maximum(ids[n // capacity, n % capacity], 0)
        held = source[pl.ds(pl.multiple_of(n * SUB, SUB), SUB), :]
        given = held[0:FLOWS]
        coarse = given.astype(jnp.bfloat16).astype(jnp.float32)
        left = jnp.concatenate([given, given - coarse], axis=0).astype(jnp.bfloat16)
        x, y, z = held[4:5], held[5:6], held[6:7]
        weight_z = tent(z, along_z)
        weight_y = tent(y, along_y)
        planes = []
        for part in range(2):
            weight_xy = tent(x, along_x + 2.0 * part) * weight_y
            for i in range(SUB):
                planes.append(weight_xy[i : i + 1] * weight_z)
        stencil = jnp.concatenate(planes, axis=0)
        high = stencil.astype(jnp.bfloat16)
        low = (stencil - high.astype(jnp.float32)).astype(jnp.bfloat16)
        right = jnp.concatenate([high, low], axis=0)
        sums = lax.dot_general(left, right, (((1,), (1,)), ((), ())), preferred_element_type=jnp.float32)
        return pl.multiple_of(tile * SUB, SUB), sums[:, :LANES] + sums[:, LANES:]

    unroll = 4

    def per_step(step, carry):
        made = [one(step * unroll + n) for n in range(unroll)]
        for start, sums in made:
            total[pl.ds(start, SUB), :] += sums
        return carry

    lax.fori_loop(0, blocks // unroll, per_step, 0)

    def per_a(a, carry):
        for b in range(across_y):
            for h in range(extent_z // LANES):
                start = ((a * across_y + b) * across_z + h * GRANULES) * SUB
                part = total.at[pl.ds(pl.multiple_of(start, SUB), GRANULES * SUB)]
                lanes = slice(h * LANES, (h + 1) * LANES)
                lines = slice(b * TILE_Y, (b + 1) * TILE_Y)
                for f in range(FLOWS):
                    pair = [
                        part[pl.ds(n * SUB * SUB + f, SUB, stride=SUB), :]
                        + part[pl.ds(n * SUB * SUB + f + FLOWS, SUB, stride=SUB), :]
                        for n in range(2)
                    ]
                    pair = [x * (1.0 / CELL_MASS) for x in exchange(*pair)]
                    for u in range(TILE_X):
                        piece = pair[u // 2][(u % 2) * TILE_Y : (u % 2 + 1) * TILE_Y]
                        x = a * TILE_X + u
                        if f < 3:
                            gas_next[f, x, lines, lanes] = diffused[f, x, lines, lanes] + piece
                        else:
                            gas_next[3, x, lines, lanes] = diffused[3, x, lines, lanes] - LATENT_HEAT * piece
                            gas_next[4, x, lines, lanes] = diffused[4, x, lines, lanes] + piece
        return carry

    lax.fori_loop(0, extent_x // TILE_X, per_a, 0)


def call(kernel, name, out_shape, scratch=(), flops=0, moved=0):
    return pl.pallas_call(
        kernel,
        out_shape=out_shape,
        scratch_shapes=scratch,
        name=name,
        cost_estimate=pl.CostEstimate(flops=flops, bytes_accessed=moved, transcendentals=0),
        compiler_params=pltpu.CompilerParams(vmem_limit_bytes=32 * 1024 * 1024),
    )


def shards(gas_state, parcel_speed, parcel_mass, offsets, cell_base, block_tile, block_count):
    fields, extent_x, extent_y, extent_z = gas_state.shape
    devices, capacity = block_tile.shape[2:]
    rows = 10 * capacity + 1
    tiles = (extent_x // TILE_X) * (extent_y // TILE_Y) * (extent_z // TILE_Z)
    f32 = jnp.float32

    def shape(*dims, dtype=f32):
        return jax.ShapeDtypeStruct(dims, dtype)

    def by_component(value):
        return value[0, 0].transpose(0, 2, 1, 3).reshape(devices * 3 * capacity, LANES)

    message = call(
        functools.partial(pack_kernel, rows=rows, capacity=capacity),
        "pack",
        shape(devices * rows, LANES),
    )(
        by_component(parcel_speed),
        parcel_mass.reshape(devices * capacity, LANES),
        by_component(offsets),
        by_component(cell_base),
        block_tile[0, 0].T,
        block_count[0],
    )
    message = lax.all_to_all(message.reshape(devices, rows, 1, LANES), BOTH, split_axis=0, concat_axis=0, tiled=True)
    message = message.reshape(devices * rows, LANES)

    face = shape(fields, extent_x, extent_z)
    table, face_x0, face_x1, face_y0, face_y1 = call(
        table_kernel,
        "table",
        (shape(FLOWS, tiles, LANES), shape(fields, extent_y, extent_z), shape(fields, extent_y, extent_z), face, face),
        flops=10**7,
    )(gas_state)

    def shifted(value, axis, step):
        count = lax.axis_size(axis)
        pairs = [(i, i + step) for i in range(count) if 0 <= i + step < count]
        return lax.ppermute(value, axis, pairs)

    diffused = call(diffuse_kernel, "diffuse", shape(*gas_state.shape), flops=10**7)(
        gas_state,
        shifted(face_x1, "gx", 1),
        shifted(face_x0, "gx", -1),
        shifted(face_y1, "yz", 1),
        shifted(face_y0, "yz", -1),
    )
    message, table, diffused = lax.optimization_barrier((message, table, diffused))

    blocks = devices * capacity
    result, source, ids = call(
        functools.partial(update_kernel, rows=rows, capacity=capacity),
        "update",
        (shape(blocks * FLOWS, LANES), shape(blocks * SUB, LANES), shape(devices, LANES, dtype=jnp.int32)),
        scratch=[
            pltpu.VMEM((devices, LANES), jnp.int32),
            pltpu.SMEM((devices, LANES), jnp.int32),
            pltpu.VMEM((FLOWS * SUB * SUB, LANES), f32),
            pltpu.SemaphoreType.DMA(()),
        ],
        flops=10**7,
    )(message, table)
    result = lax.all_to_all(
        result.reshape(devices, capacity * FLOWS, LANES), BOTH, split_axis=0, concat_axis=0, tiled=True
    )
    gas_next = call(
        functools.partial(deposit_kernel, capacity=capacity),
        "deposit",
        shape(*gas_state.shape),
        scratch=[
            pltpu.VMEM((tiles * SUB, LANES), f32),
            pltpu.SMEM((devices, LANES), jnp.int32),
            pltpu.SemaphoreType.DMA(()),
        ],
        flops=3 * 10**7,
    )(ids, source, diffused)
    speed_next = result[:, : 3 * capacity].reshape(devices, 3, capacity, LANES).transpose(0, 2, 1, 3)
    mass_next = result[:, 3 * capacity :]
    return gas_next, speed_next.reshape(parcel_speed.shape), mass_next.reshape(parcel_mass.shape)


def solution(mesh):
    in_specs = (
        P(None, "gx", "yz", None),
        P("gx", "yz", None, None, None, None),
        P("gx", "yz", None, None, None),
        P("gx", "yz", None, None, None, None),
        P("gx", "yz", None, None, None, None),
        P("gx", "yz", None, None),
        P("gx", "yz", None),
    )
    out_specs = (
        P(None, "gx", "yz", None),
        P("gx", "yz", None, None, None, None),
        P("gx", "yz", None, None, None),
    )
    return jax.shard_map(shards, mesh=mesh, in_specs=in_specs, out_specs=out_specs, check_vma=False)
```

```python
import functools

import jax
import jax.numpy as jnp
from jax import lax
from jax.experimental import pallas as pl
from jax.experimental.pallas import tpu as pltpu
from jax.sharding import PartitionSpec as P

TILE_X = 4
TILE_Y = 4
TILE_Z = 8
DIFFUSION = 0.1
CELL_MASS = 4.0
DRAG_RATE = 0.5
EVAPORATION = 0.3
LATENT_HEAT = 2.0

LANES = 128
SUB = 8
GRANULES = LANES // TILE_Z
FLOWS = 4
BOTH = ("gx", "yz")


def roll(x, shift, axis):
    shift = shift % x.shape[axis]
    return pltpu.roll(x, shift, axis) if shift else x


def pick(x, rows):
    return jnp.take_along_axis(x, rows, axis=0, mode="promise_in_bounds")


def exchange(upper, lower):
    row = lax.broadcasted_iota(jnp.int32, (SUB, LANES), 0)
    granule = lax.broadcasted_iota(jnp.int32, (SUB, LANES), 1) // TILE_Z
    half = LANES // 2
    turned = [
        pltpu.roll(x, shift, 1, stride=TILE_Z, stride_axis=0) for x, shift in ((upper, 0), (lower, half))
    ]
    back = SUB - 1 - row
    pair = []
    for part in range(2):
        wanted = (granule - back - SUB * part) % GRANULES
        mixed = jnp.where(wanted < SUB, pick(turned[0], wanted % SUB), pick(turned[1], wanted % SUB))
        shift = (-TILE_Z * (SUB - 1) - half * part) % LANES
        pair.append(pick(pltpu.roll(mixed, shift, 1, stride=TILE_Z, stride_axis=0), back))
    return pair


def pack_kernel(
    speed, mass, offsets, cells, tile_ids, counts, message,
    speed_v, mass_v, offsets_v, cells_v, tile_ids_v, counts_v, ids_v, message_v, sems, *, rows, capacity
):
    owners = tile_ids.shape[1]
    vector = 3 * capacity
    sources = ((speed, speed_v, vector), (offsets, offsets_v, vector), (cells, cells_v, vector), (mass, mass_v, capacity))
    parts = 2
    each = owners // parts
    small = [
        pltpu.make_async_copy(tile_ids, tile_ids_v, sems.at[0]),
        pltpu.make_async_copy(counts, counts_v, sems.at[1]),
    ]
    taken = []
    for copy in small:
        copy.start()
    for part in range(parts):
        taken.append([])
        for n, (source, held, count) in enumerate(sources):
            place = pl.ds(part * each * count, each * count)
            copy = pltpu.make_async_copy(source.at[place], held.at[place], sems.at[2 + part * 4 + n])
            copy.start()
            taken[-1].append(copy)
    for copy in small:
        copy.wait()
    slot = lax.broadcasted_iota(jnp.int32, tile_ids_v.shape, 0)
    ids = jnp.where(slot < counts_v[...], tile_ids_v[...], -1).astype(jnp.float32)
    ids_v[...] = jnp.concatenate([ids, jnp.zeros((LANES - capacity, owners), jnp.float32)], axis=0).T

    def per_group(g, carry):
        def at(held, count):
            return held.at[pl.ds(pl.multiple_of(g * SUB * count, SUB), SUB * count)]

        out = at(message_v, rows)
        speed_g, offsets_g, cells_g, mass_g = (at(held, count) for _, held, count in sources)
        ids_g = at(ids_v, 1)
        for i in range(SUB):
            base = i * rows
            place = slice(i * vector, (i + 1) * vector)
            out[base : base + vector, :] = speed_g[place, :]
            out[base + vector : base + 2 * vector, :] = offsets_g[place, :]
            out[base + 2 * vector : base + 3 * vector, :] = cells_g[place, :].astype(jnp.float32)
            out[base + 3 * vector : base + 3 * vector + capacity, :] = mass_g[i * capacity : (i + 1) * capacity, :]
            out[base + rows - 1 : base + rows, :] = ids_g[i : i + 1, :]
        return carry

    sent = []
    for part in range(parts):
        for copy in taken[part]:
            copy.wait()
        lax.fori_loop(part * each // SUB, (part + 1) * each // SUB, per_group, 0)
        place = pl.ds(part * each * rows, each * rows)
        copy = pltpu.make_async_copy(message_v.at[place], message.at[place], sems.at[2 + parts * 4 + part])
        copy.start()
        sent.append(copy)
    for copy in sent:
        copy.wait()


def table_kernel(gas, table_hbm, face_x0, face_x1, face_y0, face_y1, table, sem):
    fields, extent_x, extent_y, extent_z = gas.shape
    across_y = extent_y // TILE_Y
    across_z = extent_z // TILE_Z
    face_x0[...] = gas[:, 0]
    face_x1[...] = gas[:, extent_x - 1]
    face_y0[...] = gas[:, :, 0, :]
    face_y1[...] = gas[:, :, extent_y - 1, :]

    def per_a(a, carry):
        for f in range(FLOWS):
            for b in range(across_y):
                for h in range(extent_z // LANES):
                    lanes = slice(h * LANES, (h + 1) * LANES)
                    rows = slice(b * TILE_Y, (b + 1) * TILE_Y)
                    parts = []
                    for u in range(TILE_X):
                        piece = gas[f, a * TILE_X + u, rows, lanes]
                        if f == 3:
                            piece = piece - gas[4, a * TILE_X + u, rows, lanes]
                        parts.append(piece)
                    pair = exchange(jnp.concatenate(parts[:2], 0), jnp.concatenate(parts[2:], 0))
                    start = pl.multiple_of((a * across_y + b) * across_z + h * GRANULES, SUB)
                    table[f, pl.ds(start, SUB), :] = pair[0]
                    table[f, pl.ds(start + SUB, SUB), :] = pair[1]
        return carry

    lax.fori_loop(0, extent_x // TILE_X, per_a, 0)
    copy = pltpu.make_async_copy(table, table_hbm, sem)
    copy.start()
    copy.wait()


def update_kernel(
    message, table_hbm, result_hbm, source, ids_vmem, ids_smem, products, table, result, sems, *, rows, capacity
):
    devices = message.shape[0] // rows
    group = SUB * rows
    fetch = pltpu.make_async_copy(table_hbm, table, sems.at[0])
    fetch.start()
    for g in range(devices // SUB):
        ids_vmem[g * SUB : (g + 1) * SUB, :] = message[pl.ds(g * group + rows - 1, SUB, stride=rows), :].astype(jnp.int32)
    copy = pltpu.make_async_copy(ids_vmem, ids_smem, sems.at[1])
    copy.start()
    corner = lax.broadcasted_iota(jnp.int32, (SUB, LANES), 0)
    high = [(corner & bit) != 0 for bit in (4, 2, 1)]
    least = [jnp.where(h, 0.0, 1.0) for h in high]
    slope = [jnp.where(h, 1.0, -1.0) for h in high]
    shift = (
        jnp.where(high[0], TILE_Y * TILE_Z, 0) + jnp.where(high[1], TILE_Z, 0) + jnp.where(high[2], 1, 0)
    )
    row = corner
    copy.wait()
    fetch.wait()

    def returned(g):
        place = pl.ds(pl.multiple_of(g * SUB * capacity * FLOWS, SUB), SUB * capacity * FLOWS)
        return pltpu.make_async_copy(result.at[place], result_hbm.at[place], sems.at[2 + g])

    def per_group(g, carry):
        part = message.at[pl.ds(pl.multiple_of(g * group, SUB), group)]
        for step in range(SUB // 2):
            alive = jnp.zeros((SUB, LANES), jnp.int32)
            for j in range(2 * capacity):
                i, k = 2 * step + j // capacity, j % capacity
                base = i * rows
                tile = ids_smem[g * SUB + i, k]
                alive = jnp.where(row == j, tile, alive)
                safe = jnp.maximum(tile, 0)
                weight = None
                for dim in range(3):
                    start = base + (3 + dim) * capacity + k
                    fraction = part[start : start + 1, :]
                    along = least[dim] + slope[dim] * fraction
                    weight = along if weight is None else weight * along
                starts = [base + (6 + dim) * capacity + k for dim in range(3)]
                cell = [part[start : start + 1, :] for start in starts]
                first = (cell[0] * TILE_Y + cell[1]) * TILE_Z + cell[2]
                index = first.astype(jnp.int32) + shift
                for f in range(FLOWS):
                    held = jnp.broadcast_to(table[f, pl.ds(safe, 1), :], (SUB, LANES))
                    found = jnp.take_along_axis(held, index, axis=1, mode="promise_in_bounds")
                    products[(f * SUB + j) * SUB : (f * SUB + j + 1) * SUB, :] = found * weight
            live = alive >= 0
            sampled = []
            for f in range(FLOWS):
                total = products[pl.ds(f * SUB * SUB, SUB, stride=SUB), :]
                for c in range(1, SUB):
                    total = total + products[pl.ds(f * SUB * SUB + c, SUB, stride=SUB), :]
                sampled.append(total)

            def both(field):
                starts = [(2 * step + n) * rows + field * capacity for n in range(2)]
                return jnp.concatenate([part[start : start + capacity, :] for start in starts], axis=0)

            mass_old = both(9)
            radius = jnp.exp(jnp.log(mass_old) * (1.0 / 3.0))
            factor = DRAG_RATE / (radius * radius)
            share = 1.0 / (1.0 + factor)
            gap = sampled[3]
            soft = jnp.maximum(gap, 0.0) + jnp.log(1.0 + jnp.exp(-jnp.abs(gap)))
            mass_new = jnp.where(live, mass_old / (1.0 + EVAPORATION * soft / radius), mass_old)
            vapour = mass_old - mass_new
            fields, sources = [], []
            for f in range(3):
                velocity = both(f)
                moved = jnp.where(live, (velocity + factor * sampled[f]) * share, velocity)
                fields.append(moved)
                sources.append(mass_old * (velocity - moved) + vapour * moved)
            fields.append(mass_new)
            sources.append(vapour)
            for dim in range(3):
                sources.append(both(3 + dim) + both(6 + dim))
            first_block = (g * SUB + 2 * step) * capacity
            out = result.at[pl.ds(pl.multiple_of(first_block * FLOWS, SUB), SUB * FLOWS)]
            for n in range(2):
                for f in range(FLOWS):
                    start = (n * FLOWS + f) * capacity
                    out[start : start + capacity, :] = fields[f][n * capacity : (n + 1) * capacity]
            out = source.at[pl.ds(pl.multiple_of(first_block * SUB, SUB), SUB * SUB)]
            for f in range(7):
                out[pl.ds(f, SUB, stride=SUB), :] = sources[f]
        returned(g).start()
        return carry

    lax.fori_loop(0, devices // SUB, per_group, 0)
    for g in range(devices // SUB):
        returned(g).wait()


def tent(position, cell):
    return jnp.maximum(0.0, 1.0 - jnp.abs(position - cell))


def diffuse_kernel(gas, from_x0, from_x1, from_y0, from_y1, diffused):
    fields, extent_x, extent_y, extent_z = gas.shape
    lane = lax.broadcasted_iota(jnp.int32, (extent_y, extent_z), 1)
    line = lax.broadcasted_iota(jnp.int32, (extent_y, extent_z), 0)

    def per_field(f, carry):
        for x in range(extent_x):
            centre = gas[f, x]
            before = from_x0[f] if x == 0 else gas[f, x - 1]
            after = from_x1[f] if x == extent_x - 1 else gas[f, x + 1]
            beside = before + after
            beside += jnp.where(line == 0, from_y0[f, x : x + 1, :], roll(centre, 1, 0))
            beside += jnp.where(line == extent_y - 1, from_y1[f, x : x + 1, :], roll(centre, -1, 0))
            beside += jnp.where(lane == 0, 0.0, roll(centre, 1, 1))
            beside += jnp.where(lane == extent_z - 1, 0.0, roll(centre, -1, 1))
            diffused[f, x] = centre + DIFFUSION * (beside - 6.0 * centre)
        return carry

    lax.fori_loop(0, fields, per_field, 0)


def deposit_kernel(ids_vmem, source, diffused, gas_next, total, ids, sem, *, capacity):
    fields, extent_x, extent_y, extent_z = diffused.shape
    across_y = extent_y // TILE_Y
    across_z = extent_z // TILE_Z
    blocks = source.shape[0] // SUB
    copy = pltpu.make_async_copy(ids_vmem, ids, sem)
    copy.start()
    total[...] = jnp.zeros(total.shape, total.dtype)
    row = lax.broadcasted_iota(jnp.int32, (SUB, LANES), 0)
    along_z = row.astype(jnp.float32)
    along_y = (row % TILE_Y).astype(jnp.float32)
    along_x = (row // TILE_Y).astype(jnp.float32)
    copy.wait()

    def one(n):
        tile = jnp.maximum(ids[n // capacity, n % capacity], 0)
        held = source[pl.ds(pl.multiple_of(n * SUB, SUB), SUB), :]
        given = held[0:FLOWS]
        coarse = given.astype(jnp.bfloat16).astype(jnp.float32)
        left = jnp.concatenate([given, given - coarse], axis=0).astype(jnp.bfloat16)
        x, y, z = held[4:5], held[5:6], held[6:7]
        weight_z = tent(z, along_z)
        weight_y = tent(y, along_y)
        planes = []
        for part in range(2):
            weight_xy = tent(x, along_x + 2.0 * part) * weight_y
            for i in range(SUB):
                planes.append(weight_xy[i : i + 1] * weight_z)
        stencil = jnp.concatenate(planes, axis=0)
        high = stencil.astype(jnp.bfloat16)
        low = (stencil - high.astype(jnp.float32)).astype(jnp.bfloat16)
        right = jnp.concatenate([high, low], axis=0)
        sums = lax.dot_general(left, right, (((1,), (1,)), ((), ())), preferred_element_type=jnp.float32)
        return pl.multiple_of(tile * SUB, SUB), sums[:, :LANES] + sums[:, LANES:]

    unroll = 4

    def per_step(step, carry):
        made = [one(step * unroll + n) for n in range(unroll)]
        for start, sums in made:
            total[pl.ds(start, SUB), :] += sums
        return carry

    lax.fori_loop(0, blocks // unroll, per_step, 0)

    def per_a(a, carry):
        for b in range(across_y):
            for h in range(extent_z // LANES):
                start = ((a * across_y + b) * across_z + h * GRANULES) * SUB
                part = total.at[pl.ds(pl.multiple_of(start, SUB), GRANULES * SUB)]
                lanes = slice(h * LANES, (h + 1) * LANES)
                lines = slice(b * TILE_Y, (b + 1) * TILE_Y)
                for f in range(FLOWS):
                    pair = [
                        part[pl.ds(n * SUB * SUB + f, SUB, stride=SUB), :]
                        + part[pl.ds(n * SUB * SUB + f + FLOWS, SUB, stride=SUB), :]
                        for n in range(2)
                    ]
                    pair = [x * (1.0 / CELL_MASS) for x in exchange(*pair)]
                    for u in range(TILE_X):
                        piece = pair[u // 2][(u % 2) * TILE_Y : (u % 2 + 1) * TILE_Y]
                        x = a * TILE_X + u
                        if f < 3:
                            gas_next[f, x, lines, lanes] = diffused[f, x, lines, lanes] + piece
                        else:
                            gas_next[3, x, lines, lanes] = diffused[3, x, lines, lanes] - LATENT_HEAT * piece
                            gas_next[4, x, lines, lanes] = diffused[4, x, lines, lanes] + piece
        return carry

    lax.fori_loop(0, extent_x // TILE_X, per_a, 0)


def unpack_kernel(result, speed, mass, sems):
    vector = speed.shape[1]
    copies = [
        pltpu.make_async_copy(result.at[:, :vector], speed, sems.at[0]),
        pltpu.make_async_copy(result.at[:, vector:], mass, sems.at[1]),
    ]
    for copy in copies:
        copy.start()
    for copy in copies:
        copy.wait()


def specs(spaces):
    return [pl.BlockSpec(memory_space=space) for space in spaces]


def call(kernel, name, out_shape, scratch=(), flops=0, moved=0, ins=None, outs=None):
    extra = {}
    if ins is not None:
        extra["in_specs"] = specs(ins)
    if outs is not None:
        extra["out_specs"] = specs(outs) if len(outs) > 1 else specs(outs)[0]
        if pltpu.HBM in outs:
            shapes = out_shape if len(outs) > 1 else (out_shape,)
            shapes = [pltpu.HBM(o.shape, o.dtype) if space == pltpu.HBM else o for o, space in zip(shapes, outs)]
            out_shape = shapes if len(outs) > 1 else shapes[0]
    called = pl.pallas_call(
        kernel,
        out_shape=out_shape,
        scratch_shapes=scratch,
        name=name,
        cost_estimate=pl.CostEstimate(flops=flops, bytes_accessed=moved, transcendentals=0),
        compiler_params=pltpu.CompilerParams(vmem_limit_bytes=32 * 1024 * 1024),
        **extra,
    )

    def with_spaces(*values):
        if ins is not None:
            values = [
                pltpu.with_memory_space_constraint(v, space) if space == pltpu.HBM else v
                for v, space in zip(values, ins)
            ]
        return called(*values)

    return with_spaces


def shards(gas_state, parcel_speed, parcel_mass, offsets, cell_base, block_tile, block_count):
    fields, extent_x, extent_y, extent_z = gas_state.shape
    devices, capacity = block_tile.shape[2:]
    rows = 10 * capacity + 1
    tiles = (extent_x // TILE_X) * (extent_y // TILE_Y) * (extent_z // TILE_Z)
    f32 = jnp.float32

    def shape(*dims, dtype=f32):
        return jax.ShapeDtypeStruct(dims, dtype)

    def by_component(value):
        return value[0, 0].transpose(0, 2, 1, 3).reshape(devices * 3 * capacity, LANES)

    vector = 3 * capacity
    blocks = devices * capacity
    i32 = jnp.int32
    hbm, vmem = pltpu.HBM, pltpu.VMEM
    dma = pltpu.SemaphoreType.DMA
    message = call(
        functools.partial(pack_kernel, rows=rows, capacity=capacity),
        "pack",
        shape(devices * rows, LANES),
        scratch=[
            vmem((devices * vector, LANES), f32),
            vmem((blocks, LANES), f32),
            vmem((devices * vector, LANES), f32),
            vmem((devices * vector, LANES), i32),
            vmem((capacity, devices), i32),
            vmem((1, devices), i32),
            vmem((devices, LANES), f32),
            vmem((devices * rows, LANES), f32),
            dma((12,)),
        ],
        ins=[hbm] * 6,
        outs=[hbm],
    )(
        by_component(parcel_speed),
        parcel_mass.reshape(blocks, LANES),
        by_component(offsets),
        by_component(cell_base),
        block_tile[0, 0].T,
        block_count[0],
    )
    message = lax.all_to_all(message.reshape(devices, rows, 1, LANES), BOTH, split_axis=0, concat_axis=0, tiled=True)
    message = message.reshape(devices * rows, LANES)

    face = shape(fields, extent_x, extent_z)
    table, face_x0, face_x1, face_y0, face_y1 = call(
        table_kernel,
        "table",
        (shape(FLOWS, tiles, LANES), shape(fields, extent_y, extent_z), shape(fields, extent_y, extent_z), face, face),
        scratch=[vmem((FLOWS, tiles, LANES), f32), dma(())],
        flops=10**7,
        ins=[vmem],
        outs=[hbm] + [vmem] * 4,
    )(gas_state)

    def shifted(value, axis, step):
        count = lax.axis_size(axis)
        pairs = [(i, i + step) for i in range(count) if 0 <= i + step < count]
        return lax.ppermute(value, axis, pairs)

    diffused = call(diffuse_kernel, "diffuse", shape(*gas_state.shape), flops=10**7)(
        gas_state,
        shifted(face_x1, "gx", 1),
        shifted(face_x0, "gx", -1),
        shifted(face_y1, "yz", 1),
        shifted(face_y0, "yz", -1),
    )
    message, table, diffused = lax.optimization_barrier((message, table, diffused))

    result, source, ids = call(
        functools.partial(update_kernel, rows=rows, capacity=capacity),
        "update",
        (shape(blocks * FLOWS, LANES), shape(blocks * SUB, LANES), shape(devices, LANES, dtype=i32)),
        scratch=[
            pltpu.SMEM((devices, LANES), i32),
            vmem((FLOWS * SUB * SUB, LANES), f32),
            vmem((FLOWS, tiles, LANES), f32),
            vmem((blocks * FLOWS, LANES), f32),
            dma((2 + devices // SUB,)),
        ],
        flops=10**7,
        ins=[vmem, hbm],
        outs=[hbm, vmem, vmem],
    )(message, table)
    result = lax.all_to_all(
        result.reshape(devices, capacity * FLOWS, 1, LANES), BOTH, split_axis=0, concat_axis=0, tiled=True
    )
    gas_next = call(
        functools.partial(deposit_kernel, capacity=capacity),
        "deposit",
        shape(*gas_state.shape),
        scratch=[vmem((tiles * SUB, LANES), f32), pltpu.SMEM((devices, LANES), i32), dma(())],
        flops=3 * 10**7,
    )(ids, source, diffused)
    speed_next, mass_next = call(
        unpack_kernel,
        "unpack",
        (shape(devices, vector, 1, LANES), shape(devices, capacity, 1, LANES)),
        scratch=[dma((2,))],
        ins=[vmem],
        outs=[hbm, hbm],
    )(result)
    speed_next = speed_next.reshape(devices, 3, capacity, LANES).transpose(0, 2, 1, 3)
    return gas_next, speed_next.reshape(parcel_speed.shape), mass_next.reshape(parcel_mass.shape)


def solution(mesh):
    in_specs = (
        P(None, "gx", "yz", None),
        P("gx", "yz", None, None, None, None),
        P("gx", "yz", None, None, None),
        P("gx", "yz", None, None, None, None),
        P("gx", "yz", None, None, None, None),
        P("gx", "yz", None, None),
        P("gx", "yz", None),
    )
    out_specs = (
        P(None, "gx", "yz", None),
        P("gx", "yz", None, None, None, None),
        P("gx", "yz", None, None, None),
    )
    return jax.shard_map(shards, mesh=mesh, in_specs=in_specs, out_specs=out_specs, check_vma=False)
```

```python
import functools

import jax
import jax.numpy as jnp
from jax import lax
from jax.experimental import pallas as pl
from jax.experimental.pallas import tpu as pltpu
from jax.sharding import PartitionSpec as P


TILE_X = 4
TILE_Y = 4
TILE_Z = 8
DIFFUSION = 0.1
CELL_MASS = 4.0
DRAG_RATE = 0.5
EVAPORATION = 0.3
LATENT_HEAT = 2.0

LANES = 128
SUB = 8
GRANULES = LANES // TILE_Z
FLOWS = 4
BOTH = ("gx", "yz")


def roll(x, shift, axis):
    shift = shift % x.shape[axis]
    return pltpu.roll(x, shift, axis) if shift else x


def pick(x, rows):
    return jnp.take_along_axis(x, rows, axis=0, mode="promise_in_bounds")


def exchange(upper, lower):
    row = lax.broadcasted_iota(jnp.int32, (SUB, LANES), 0)
    granule = lax.broadcasted_iota(jnp.int32, (SUB, LANES), 1) // TILE_Z
    half = LANES // 2
    turned = [
        pltpu.roll(x, shift, 1, stride=TILE_Z, stride_axis=0) for x, shift in ((upper, 0), (lower, half))
    ]
    back = SUB - 1 - row
    pair = []
    for part in range(2):
        wanted = (granule - back - SUB * part) % GRANULES
        mixed = jnp.where(wanted < SUB, pick(turned[0], wanted % SUB), pick(turned[1], wanted % SUB))
        shift = (-TILE_Z * (SUB - 1) - half * part) % LANES
        pair.append(pick(pltpu.roll(mixed, shift, 1, stride=TILE_Z, stride_axis=0), back))
    return pair


def pack_kernel(
    speed, mass, offsets, cells, tile_ids, counts, message,
    speed_v, mass_v, offsets_v, cells_v, tile_ids_v, counts_v, ids_v, message_v, sems, *, rows, capacity
):
    owners = tile_ids.shape[1]
    vector = 3 * capacity
    sources = ((speed, speed_v, vector), (offsets, offsets_v, vector), (cells, cells_v, vector), (mass, mass_v, capacity))
    parts = 2
    each = owners // parts
    small = [
        pltpu.make_async_copy(tile_ids, tile_ids_v, sems.at[0]),
        pltpu.make_async_copy(counts, counts_v, sems.at[1]),
    ]
    taken = []
    for copy in small:
        copy.start()
    for part in range(parts):
        taken.append([])
        for n, (source, held, count) in enumerate(sources):
            place = pl.ds(part * each * count, each * count)
            copy = pltpu.make_async_copy(source.at[place], held.at[place], sems.at[2 + part * 4 + n])
            copy.start()
            taken[-1].append(copy)
    for copy in small:
        copy.wait()
    slot = lax.broadcasted_iota(jnp.int32, tile_ids_v.shape, 0)
    ids = jnp.where(slot < counts_v[...], tile_ids_v[...], -1).astype(jnp.float32)
    ids_v[...] = jnp.concatenate([ids, jnp.zeros((LANES - capacity, owners), jnp.float32)], axis=0).T

    def per_group(g, carry):
        def at(held, count):
            return held.at[pl.ds(pl.multiple_of(g * SUB * count, SUB), SUB * count)]

        out = at(message_v, rows)
        speed_g, offsets_g, cells_g, mass_g = (at(held, count) for _, held, count in sources)
        ids_g = at(ids_v, 1)
        for i in range(SUB):
            base = i * rows
            place = slice(i * vector, (i + 1) * vector)
            out[base : base + vector, :] = speed_g[place, :]
            out[base + vector : base + 2 * vector, :] = offsets_g[place, :]
            out[base + 2 * vector : base + 3 * vector, :] = cells_g[place, :].astype(jnp.float32)
            out[base + 3 * vector : base + 3 * vector + capacity, :] = mass_g[i * capacity : (i + 1) * capacity, :]
            out[base + rows - 1 : base + rows, :] = ids_g[i : i + 1, :]
        return carry

    sent = []
    for part in range(parts):
        for copy in taken[part]:
            copy.wait()
        lax.fori_loop(part * each // SUB, (part + 1) * each // SUB, per_group, 0)
        place = pl.ds(part * each * rows, each * rows)
        copy = pltpu.make_async_copy(message_v.at[place], message.at[place], sems.at[2 + parts * 4 + part])
        copy.start()
        sent.append(copy)
    for copy in sent:
        copy.wait()


def faces_kernel(gas_hbm, face_x0, face_x1, face_y0, face_y1, gas, sem):
    extent_x, extent_y = gas_hbm.shape[1:3]
    copy = pltpu.make_async_copy(gas_hbm, gas, sem)
    copy.start()
    copy.wait()
    face_x0[...] = gas[:, 0]
    face_x1[...] = gas[:, extent_x - 1]
    face_y0[...] = gas[:, :, 0, :]
    face_y1[...] = gas[:, :, extent_y - 1, :]


def local_kernel(gas_hbm, table, diffused_hbm, gas, diffused, sems):
    fields, extent_x, extent_y, extent_z = gas.shape
    across_y = extent_y // TILE_Y
    across_z = extent_z // TILE_Z
    lane = lax.broadcasted_iota(jnp.int32, (extent_y, extent_z), 1)
    line = lax.broadcasted_iota(jnp.int32, (extent_y, extent_z), 0)
    copy = pltpu.make_async_copy(gas_hbm, gas, sems.at[fields])
    copy.start()
    copy.wait()

    def sent(f):
        return pltpu.make_async_copy(diffused.at[f], diffused_hbm.at[f], sems.at[f])

    def per_field(f, carry):
        for x in range(extent_x):
            centre = gas[f, x]
            beside = jnp.where(line == 0, 0.0, roll(centre, 1, 0))
            beside += jnp.where(line == extent_y - 1, 0.0, roll(centre, -1, 0))
            beside += jnp.where(lane == 0, 0.0, roll(centre, 1, 1))
            beside += jnp.where(lane == extent_z - 1, 0.0, roll(centre, -1, 1))
            if x > 0:
                beside += gas[f, x - 1]
            if x < extent_x - 1:
                beside += gas[f, x + 1]
            diffused[f, x * extent_y : (x + 1) * extent_y, :] = centre + DIFFUSION * (beside - 6.0 * centre)
        sent(f).start()
        return carry

    lax.fori_loop(0, fields, per_field, 0)

    def per_a(a, carry):
        for f in range(FLOWS):
            for b in range(across_y):
                for h in range(extent_z // LANES):
                    lanes = slice(h * LANES, (h + 1) * LANES)
                    rows = slice(b * TILE_Y, (b + 1) * TILE_Y)
                    parts = []
                    for u in range(TILE_X):
                        piece = gas[f, a * TILE_X + u, rows, lanes]
                        if f == 3:
                            piece = piece - gas[4, a * TILE_X + u, rows, lanes]
                        parts.append(piece)
                    pair = exchange(jnp.concatenate(parts[:2], 0), jnp.concatenate(parts[2:], 0))
                    start = pl.multiple_of((a * across_y + b) * across_z + h * GRANULES, SUB)
                    table[f, pl.ds(start, SUB), :] = pair[0]
                    table[f, pl.ds(start + SUB, SUB), :] = pair[1]
        return carry

    lax.fori_loop(0, extent_x // TILE_X, per_a, 0)
    for f in range(fields):
        sent(f).wait()


def update_kernel(
    message, table, result_hbm, source, ids_vmem, ids_smem, products, result, sems, *, rows, capacity
):
    devices = message.shape[0] // rows
    group = SUB * rows
    for g in range(devices // SUB):
        ids_vmem[g * SUB : (g + 1) * SUB, :] = message[pl.ds(g * group + rows - 1, SUB, stride=rows), :].astype(jnp.int32)
    copy = pltpu.make_async_copy(ids_vmem, ids_smem, sems.at[0])
    copy.start()
    corner = lax.broadcasted_iota(jnp.int32, (SUB, LANES), 0)
    high = [(corner & bit) != 0 for bit in (4, 2, 1)]
    least = [jnp.where(h, 0.0, 1.0) for h in high]
    slope = [jnp.where(h, 1.0, -1.0) for h in high]
    shift = (
        jnp.where(high[0], TILE_Y * TILE_Z, 0) + jnp.where(high[1], TILE_Z, 0) + jnp.where(high[2], 1, 0)
    )
    row = corner
    copy.wait()

    def returned(g):
        place = pl.ds(pl.multiple_of(g * SUB * capacity * FLOWS, SUB), SUB * capacity * FLOWS)
        return pltpu.make_async_copy(result.at[place], result_hbm.at[place], sems.at[1 + g])

    def per_group(g, carry):
        part = message.at[pl.ds(pl.multiple_of(g * group, SUB), group)]
        for step in range(SUB // 2):
            alive = jnp.zeros((SUB, LANES), jnp.int32)
            for j in range(2 * capacity):
                i, k = 2 * step + j // capacity, j % capacity
                base = i * rows
                tile = ids_smem[g * SUB + i, k]
                alive = jnp.where(row == j, tile, alive)
                safe = jnp.maximum(tile, 0)
                weight = None
                for dim in range(3):
                    start = base + (3 + dim) * capacity + k
                    fraction = part[start : start + 1, :]
                    along = least[dim] + slope[dim] * fraction
                    weight = along if weight is None else weight * along
                starts = [base + (6 + dim) * capacity + k for dim in range(3)]
                cell = [part[start : start + 1, :] for start in starts]
                first = (cell[0] * TILE_Y + cell[1]) * TILE_Z + cell[2]
                index = first.astype(jnp.int32) + shift
                for f in range(FLOWS):
                    held = jnp.broadcast_to(table[f, pl.ds(safe, 1), :], (SUB, LANES))
                    found = jnp.take_along_axis(held, index, axis=1, mode="promise_in_bounds")
                    products[(f * SUB + j) * SUB : (f * SUB + j + 1) * SUB, :] = found * weight
            live = alive >= 0
            sampled = []
            for f in range(FLOWS):
                total = products[pl.ds(f * SUB * SUB, SUB, stride=SUB), :]
                for c in range(1, SUB):
                    total = total + products[pl.ds(f * SUB * SUB + c, SUB, stride=SUB), :]
                sampled.append(total)

            def both(field):
                starts = [(2 * step + n) * rows + field * capacity for n in range(2)]
                return jnp.concatenate([part[start : start + capacity, :] for start in starts], axis=0)

            mass_old = both(9)
            radius = jnp.exp(jnp.log(mass_old) * (1.0 / 3.0))
            factor = DRAG_RATE / (radius * radius)
            share = 1.0 / (1.0 + factor)
            gap = sampled[3]
            soft = jnp.maximum(gap, 0.0) + jnp.log(1.0 + jnp.exp(-jnp.abs(gap)))
            mass_new = jnp.where(live, mass_old / (1.0 + EVAPORATION * soft / radius), mass_old)
            vapour = mass_old - mass_new
            fields, sources = [], []
            for f in range(3):
                velocity = both(f)
                moved = jnp.where(live, (velocity + factor * sampled[f]) * share, velocity)
                fields.append(moved)
                sources.append(mass_old * (velocity - moved) + vapour * moved)
            fields.append(mass_new)
            sources.append(vapour)
            for dim in range(3):
                sources.append(both(3 + dim) + both(6 + dim))
            first_block = (g * SUB + 2 * step) * capacity
            out = result.at[pl.ds(pl.multiple_of(first_block * FLOWS, SUB), SUB * FLOWS)]
            for n in range(2):
                for f in range(FLOWS):
                    start = (n * FLOWS + f) * capacity
                    out[start : start + capacity, :] = fields[f][n * capacity : (n + 1) * capacity]
            out = source.at[pl.ds(pl.multiple_of(first_block * SUB, SUB), SUB * SUB)]
            for f in range(7):
                out[pl.ds(f, SUB, stride=SUB), :] = sources[f]
        returned(g).start()
        return carry

    lax.fori_loop(0, devices // SUB, per_group, 0)
    for g in range(devices // SUB):
        returned(g).wait()


def tent(position, cell):
    return jnp.maximum(0.0, 1.0 - jnp.abs(position - cell))


def deposit_kernel(
    ids_vmem, source, diffused, from_x0, from_x1, from_y0, from_y1, gas_next, total, ids, work, sems, *, capacity
):
    fields, extent_x, extent_z = from_y0.shape
    extent_y = from_x0.shape[1]
    across_y = extent_y // TILE_Y
    across_z = extent_z // TILE_Z
    blocks = source.shape[0] // SUB
    copy = pltpu.make_async_copy(ids_vmem, ids, sems.at[0])
    copy.start()
    fetch = pltpu.make_async_copy(diffused, work, sems.at[1])
    fetch.start()
    total[...] = jnp.zeros(total.shape, total.dtype)
    row = lax.broadcasted_iota(jnp.int32, (SUB, LANES), 0)
    along_z = row.astype(jnp.float32)
    along_y = (row % TILE_Y).astype(jnp.float32)
    along_x = (row // TILE_Y).astype(jnp.float32)
    copy.wait()

    def one(n):
        tile = jnp.maximum(ids[n // capacity, n % capacity], 0)
        held = source[pl.ds(pl.multiple_of(n * SUB, SUB), SUB), :]
        given = held[0:FLOWS]
        coarse = given.astype(jnp.bfloat16).astype(jnp.float32)
        left = jnp.concatenate([given, given - coarse], axis=0).astype(jnp.bfloat16)
        x, y, z = held[4:5], held[5:6], held[6:7]
        weight_z = tent(z, along_z)
        weight_y = tent(y, along_y)
        planes = []
        for part in range(2):
            weight_xy = tent(x, along_x + 2.0 * part) * weight_y
            for i in range(SUB):
                planes.append(weight_xy[i : i + 1] * weight_z)
        stencil = jnp.concatenate(planes, axis=0)
        high = stencil.astype(jnp.bfloat16)
        low = (stencil - high.astype(jnp.float32)).astype(jnp.bfloat16)
        right = jnp.concatenate([high, low], axis=0)
        sums = lax.dot_general(left, right, (((1,), (1,)), ((), ())), preferred_element_type=jnp.float32)
        return pl.multiple_of(tile * SUB, SUB), sums[:, :LANES] + sums[:, LANES:]

    unroll = 16

    def per_step(step, carry):
        made = [one(step * unroll + n) for n in range(unroll)]
        for start, sums in made:
            total[pl.ds(start, SUB), :] += sums
        return carry

    lax.fori_loop(0, blocks // unroll, per_step, 0)

    fetch.wait()
    last_x = (extent_x - 1) * extent_y
    for f in range(fields):
        work[f, 0:extent_y, :] += DIFFUSION * from_x0[f]
        work[f, last_x : last_x + extent_y, :] += DIFFUSION * from_x1[f]
        for h in range(extent_z // LANES):
            lanes = slice(h * LANES, (h + 1) * LANES)
            for line, face in ((0, from_y0), (extent_y - 1, from_y1)):
                for x in range(extent_x):
                    spot = x * extent_y + line
                    work[f, spot : spot + 1, lanes] += DIFFUSION * face[f, x : x + 1, lanes]

    def sent(a):
        place = pl.ds(pl.multiple_of(a * TILE_X * extent_y, SUB), TILE_X * extent_y)
        return pltpu.make_async_copy(work.at[:, place], gas_next.at[:, place], sems.at[2 + a])

    def per_a(a, carry):
        held = work.at[:, pl.ds(pl.multiple_of(a * TILE_X * extent_y, SUB), TILE_X * extent_y)]
        for b in range(across_y):
            for h in range(extent_z // LANES):
                start = ((a * across_y + b) * across_z + h * GRANULES) * SUB
                part = total.at[pl.ds(pl.multiple_of(start, SUB), GRANULES * SUB)]
                lanes = slice(h * LANES, (h + 1) * LANES)
                for f in range(FLOWS):
                    pair = [
                        part[pl.ds(n * SUB * SUB + f, SUB, stride=SUB), :]
                        + part[pl.ds(n * SUB * SUB + f + FLOWS, SUB, stride=SUB), :]
                        for n in range(2)
                    ]
                    pair = [x * (1.0 / CELL_MASS) for x in exchange(*pair)]
                    for u in range(TILE_X):
                        piece = pair[u // 2][(u % 2) * TILE_Y : (u % 2 + 1) * TILE_Y]
                        spot = u * extent_y + b * TILE_Y
                        lines = slice(spot, spot + TILE_Y)
                        if f < 3:
                            held[f, lines, lanes] += piece
                        else:
                            held[3, lines, lanes] -= LATENT_HEAT * piece
                            held[4, lines, lanes] += piece
        sent(a).start()
        return carry

    lax.fori_loop(0, extent_x // TILE_X, per_a, 0)
    for a in range(extent_x // TILE_X):
        sent(a).wait()


def unpack_kernel(result, speed, mass, sems):
    vector = speed.shape[1]
    copies = [
        pltpu.make_async_copy(result.at[:, :vector], speed, sems.at[0]),
        pltpu.make_async_copy(result.at[:, vector:], mass, sems.at[1]),
    ]
    for copy in copies:
        copy.start()
    for copy in copies:
        copy.wait()


def specs(spaces):
    return [pl.BlockSpec(memory_space=space) for space in spaces]


def call(kernel, out_shape, scratch=(), flops=0, moved=0, ins=None, outs=None):
    extra = {}
    if ins is not None:
        extra["in_specs"] = specs(ins)
    if outs is not None:
        extra["out_specs"] = specs(outs) if len(outs) > 1 else specs(outs)[0]
        if pltpu.HBM in outs:
            shapes = out_shape if len(outs) > 1 else (out_shape,)
            shapes = [pltpu.HBM(o.shape, o.dtype) if space == pltpu.HBM else o for o, space in zip(shapes, outs)]
            out_shape = shapes if len(outs) > 1 else shapes[0]
    called = pl.pallas_call(
        kernel,
        out_shape=out_shape,
        scratch_shapes=scratch,
        cost_estimate=pl.CostEstimate(flops=flops, bytes_accessed=moved, transcendentals=0),
        compiler_params=pltpu.CompilerParams(vmem_limit_bytes=32 * 1024 * 1024),
        **extra,
    )

    def with_spaces(*values):
        if ins is not None:
            values = [
                pltpu.with_memory_space_constraint(v, space) if space == pltpu.HBM else v
                for v, space in zip(values, ins)
            ]
        return called(*values)

    return with_spaces


def step(gas_state, parcel_speed, parcel_mass, offsets, cell_base, block_tile, block_count):
    fields, extent_x, extent_y, extent_z = gas_state.shape
    devices, capacity = block_tile.shape[2:]
    rows = 10 * capacity + 1
    tiles = (extent_x // TILE_X) * (extent_y // TILE_Y) * (extent_z // TILE_Z)
    f32 = jnp.float32

    def shape(*dims, dtype=f32):
        return jax.ShapeDtypeStruct(dims, dtype)

    def by_component(value):
        return value[0, 0].transpose(0, 2, 1, 3).reshape(devices * 3 * capacity, LANES)

    vector = 3 * capacity
    blocks = devices * capacity
    i32 = jnp.int32
    hbm, vmem = pltpu.HBM, pltpu.VMEM
    dma = pltpu.SemaphoreType.DMA
    message = call(
        functools.partial(pack_kernel, rows=rows, capacity=capacity),
        shape(devices * rows, LANES),
        scratch=[
            vmem((devices * vector, LANES), f32),
            vmem((blocks, LANES), f32),
            vmem((devices * vector, LANES), f32),
            vmem((devices * vector, LANES), i32),
            vmem((capacity, devices), i32),
            vmem((1, devices), i32),
            vmem((devices, LANES), f32),
            vmem((devices * rows, LANES), f32),
            dma((12,)),
        ],
        ins=[hbm] * 6,
        outs=[hbm],
    )(
        by_component(parcel_speed),
        parcel_mass.reshape(blocks, LANES),
        by_component(offsets),
        by_component(cell_base),
        block_tile[0, 0].T,
        block_count[0],
    )
    message = lax.all_to_all(message.reshape(devices, rows, 1, LANES), BOTH, split_axis=0, concat_axis=0, tiled=True)
    message = message.reshape(devices * rows, LANES)

    face = shape(fields, extent_x, extent_z)
    side = shape(fields, extent_y, extent_z)
    whole = vmem(gas_state.shape, f32)
    flat = (fields, extent_x * extent_y, extent_z)
    face_x0, face_x1, face_y0, face_y1 = call(
        faces_kernel, (side, side, face, face), scratch=[whole, dma(())], ins=[hbm], outs=[vmem] * 4
    )(gas_state)

    def shifted(value, axis, step):
        count = lax.axis_size(axis)
        pairs = [(i, i + step) for i in range(count) if 0 <= i + step < count]
        return lax.ppermute(value, axis, pairs)

    halo = (
        shifted(face_x1, "gx", 1), shifted(face_x0, "gx", -1), shifted(face_y1, "yz", 1), shifted(face_y0, "yz", -1)
    )
    table, diffused = call(
        local_kernel,
        (shape(FLOWS, tiles, LANES), shape(*flat)),
        scratch=[whole, vmem(flat, f32), dma((fields + 1,))],
        flops=10**7,
        ins=[hbm],
        outs=[vmem, hbm],
    )(gas_state)
    message, table, diffused = lax.optimization_barrier((message, table, diffused))

    result, source, ids = call(
        functools.partial(update_kernel, rows=rows, capacity=capacity),
        (shape(blocks * FLOWS, LANES), shape(blocks * SUB, LANES), shape(devices, LANES, dtype=i32)),
        scratch=[
            pltpu.SMEM((devices, LANES), i32),
            vmem((FLOWS * SUB * SUB, LANES), f32),
            vmem((blocks * FLOWS, LANES), f32),
            dma((1 + devices // SUB,)),
        ],
        flops=10**7,
        ins=[vmem, vmem],
        outs=[hbm, vmem, vmem],
    )(message, table)
    result = lax.all_to_all(
        result.reshape(devices, capacity * FLOWS, 1, LANES), BOTH, split_axis=0, concat_axis=0, tiled=True
    )
    gas_next = call(
        functools.partial(deposit_kernel, capacity=capacity),
        shape(*flat),
        scratch=[
            vmem((tiles * SUB, LANES), f32),
            pltpu.SMEM((devices, LANES), i32),
            vmem(flat, f32),
            dma((2 + extent_x // TILE_X,)),
        ],
        flops=3 * 10**7,
        ins=[vmem, vmem, hbm] + [vmem] * 4,
        outs=[hbm],
    )(ids, source, diffused, *halo)
    speed_next, mass_next = call(
        unpack_kernel,
        (shape(devices, vector, 1, LANES), shape(devices, capacity, 1, LANES)),
        scratch=[dma((2,))],
        ins=[vmem],
        outs=[hbm, hbm],
    )(result)
    speed_next = speed_next.reshape(devices, 3, capacity, LANES).transpose(0, 2, 1, 3)
    return gas_next.reshape(gas_state.shape), speed_next.reshape(parcel_speed.shape), mass_next.reshape(parcel_mass.shape)


def solution(mesh):
    in_specs = (
        P(None, "gx", "yz", None),
        P("gx", "yz", None, None, None, None),
        P("gx", "yz", None, None, None),
        P("gx", "yz", None, None, None, None),
        P("gx", "yz", None, None, None, None),
        P("gx", "yz", None, None),
        P("gx", "yz", None),
    )
    out_specs = (
        P(None, "gx", "yz", None),
        P("gx", "yz", None, None, None, None),
        P("gx", "yz", None, None, None),
    )
    return jax.shard_map(step, mesh=mesh, in_specs=in_specs, out_specs=out_specs, check_vma=False)
```

```python
import functools

import jax
import jax.numpy as jnp
from jax import lax
from jax.experimental import pallas as pl
from jax.experimental.pallas import tpu as pltpu
from jax.sharding import PartitionSpec as P


TILE_X = 4
TILE_Y = 4
TILE_Z = 8
DIFFUSION = 0.1
CELL_MASS = 4.0
DRAG_RATE = 0.5
EVAPORATION = 0.3
LATENT_HEAT = 2.0

LANES = 128
SUB = 8
GRANULES = LANES // TILE_Z
FLOWS = 4
BOTH = ("yz", "gx")


def roll(x, shift, axis):
    shift = shift % x.shape[axis]
    return pltpu.roll(x, shift, axis) if shift else x


def pick(x, rows):
    return jnp.take_along_axis(x, rows, axis=0, mode="promise_in_bounds")


def exchange(upper, lower):
    row = lax.broadcasted_iota(jnp.int32, (SUB, LANES), 0)
    granule = lax.broadcasted_iota(jnp.int32, (SUB, LANES), 1) // TILE_Z
    half = LANES // 2
    turned = [
        pltpu.roll(x, shift, 1, stride=TILE_Z, stride_axis=0) for x, shift in ((upper, 0), (lower, half))
    ]
    back = SUB - 1 - row
    pair = []
    for part in range(2):
        wanted = (granule - back - SUB * part) % GRANULES
        mixed = jnp.where(wanted < SUB, pick(turned[0], wanted % SUB), pick(turned[1], wanted % SUB))
        shift = (-TILE_Z * (SUB - 1) - half * part) % LANES
        pair.append(pick(pltpu.roll(mixed, shift, 1, stride=TILE_Z, stride_axis=0), back))
    return pair


def pack_kernel(
    speed, mass, offsets, cells, tile_ids, counts, message,
    speed_v, mass_v, offsets_v, cells_v, tile_ids_v, counts_v, ids_v, message_v, sems, *, rows, capacity, parts
):
    across_i = speed.shape[0]
    vector = 3 * capacity
    across_j = speed.shape[1] // vector
    each = across_j // parts
    sources = ((speed, speed_v, vector), (offsets, offsets_v, vector), (cells, cells_v, vector), (mass, mass_v, capacity))
    small = [
        pltpu.make_async_copy(tile_ids, tile_ids_v, sems.at[0]),
        pltpu.make_async_copy(counts, counts_v, sems.at[1]),
    ]
    taken = []
    for copy in small:
        copy.start()
    for part in range(parts):
        taken.append([])
        for n, (source, held, count) in enumerate(sources):
            place = pl.ds(part * each * count, each * count)
            copy = pltpu.make_async_copy(source.at[:, place], held.at[:, place], sems.at[2 + part * 5 + n])
            copy.start()
            taken[-1].append(copy)
    for copy in small:
        copy.wait()
    slot = lax.broadcasted_iota(jnp.int32, tile_ids_v.shape, 0)
    ids = jnp.where(slot < counts_v[...], tile_ids_v[...], -1).astype(jnp.float32)
    ids_v[...] = jnp.concatenate([ids, jnp.zeros((LANES - capacity, ids.shape[1]), jnp.float32)], axis=0).T

    sent = []
    for part in range(parts):
        for copy in taken[part]:
            copy.wait()
        for j in range(part * each, (part + 1) * each):
            for i in range(across_i):
                base = (j * across_i + i) * rows
                place = slice(j * vector, (j + 1) * vector)
                message_v[base : base + vector, :] = speed_v[i, place, :]
                message_v[base + vector : base + 2 * vector, :] = offsets_v[i, place, :]
                message_v[base + 2 * vector : base + 3 * vector, :] = cells_v[i, place, :].astype(jnp.float32)
                base += 3 * vector
                message_v[base : base + capacity, :] = mass_v[i, j * capacity : (j + 1) * capacity, :]
                owner = i * across_j + j
                message_v[base + capacity : base + capacity + 1, :] = ids_v[owner : owner + 1, :]
        place = pl.ds(part * each * across_i * rows, each * across_i * rows)
        copy = pltpu.make_async_copy(message_v.at[place], message.at[place], sems.at[2 + part * 5 + 4])
        copy.start()
        sent.append(copy)
    for copy in sent:
        copy.wait()


def faces_kernel(gas_hbm, face_x0, face_x1, face_y0, face_y1, gas, sem):
    extent_x, extent_y = gas_hbm.shape[1:3]
    copy = pltpu.make_async_copy(gas_hbm, gas, sem)
    copy.start()
    copy.wait()
    face_x0[...] = gas[:, 0]
    face_x1[...] = gas[:, extent_x - 1]
    face_y0[...] = gas[:, :, 0, :]
    face_y1[...] = gas[:, :, extent_y - 1, :]


def local_kernel(gas_hbm, table, diffused_hbm, gas, diffused, sems):
    fields, extent_x, extent_y, extent_z = gas.shape
    across_y = extent_y // TILE_Y
    across_z = extent_z // TILE_Z
    lane = lax.broadcasted_iota(jnp.int32, (extent_y, extent_z), 1)
    line = lax.broadcasted_iota(jnp.int32, (extent_y, extent_z), 0)
    copy = pltpu.make_async_copy(gas_hbm, gas, sems.at[fields])
    copy.start()
    copy.wait()

    def sent(f):
        return pltpu.make_async_copy(diffused.at[f], diffused_hbm.at[f], sems.at[f])

    def per_field(f, carry):
        for x in range(extent_x):
            centre = gas[f, x]
            beside = jnp.where(line == 0, 0.0, roll(centre, 1, 0))
            beside += jnp.where(line == extent_y - 1, 0.0, roll(centre, -1, 0))
            beside += jnp.where(lane == 0, 0.0, roll(centre, 1, 1))
            beside += jnp.where(lane == extent_z - 1, 0.0, roll(centre, -1, 1))
            if x > 0:
                beside += gas[f, x - 1]
            if x < extent_x - 1:
                beside += gas[f, x + 1]
            diffused[f, x * extent_y : (x + 1) * extent_y, :] = centre + DIFFUSION * (beside - 6.0 * centre)
        sent(f).start()
        return carry

    lax.fori_loop(0, fields, per_field, 0)

    def per_a(a, carry):
        for f in range(FLOWS):
            for b in range(across_y):
                for h in range(extent_z // LANES):
                    lanes = slice(h * LANES, (h + 1) * LANES)
                    rows = slice(b * TILE_Y, (b + 1) * TILE_Y)
                    parts = []
                    for u in range(TILE_X):
                        piece = gas[f, a * TILE_X + u, rows, lanes]
                        if f == 3:
                            piece = piece - gas[4, a * TILE_X + u, rows, lanes]
                        parts.append(piece)
                    pair = exchange(jnp.concatenate(parts[:2], 0), jnp.concatenate(parts[2:], 0))
                    start = pl.multiple_of((a * across_y + b) * across_z + h * GRANULES, SUB)
                    table[f, pl.ds(start, SUB), :] = pair[0]
                    table[f, pl.ds(start + SUB, SUB), :] = pair[1]
        return carry

    lax.fori_loop(0, extent_x // TILE_X, per_a, 0)
    for f in range(fields):
        sent(f).wait()


def update_kernel(
    message, table, result_hbm, source, ids_vmem, products, result, sems, *, rows, capacity
):
    devices = message.shape[0] // rows
    group = SUB * rows
    for g in range(devices // SUB):
        ids_vmem[g * SUB : (g + 1) * SUB, :] = message[pl.ds(g * group + rows - 1, SUB, stride=rows), :].astype(jnp.int32)
    corner = lax.broadcasted_iota(jnp.int32, (SUB, LANES), 0)
    high = [(corner & bit) != 0 for bit in (4, 2, 1)]
    least = [jnp.where(h, 0.0, 1.0) for h in high]
    slope = [jnp.where(h, 1.0, -1.0) for h in high]
    shift = (
        jnp.where(high[0], TILE_Y * TILE_Z, 0) + jnp.where(high[1], TILE_Z, 0) + jnp.where(high[2], 1, 0)
    )
    row = corner

    def returned(g):
        place = pl.ds(pl.multiple_of(g * SUB * capacity * FLOWS, SUB), SUB * capacity * FLOWS)
        return pltpu.make_async_copy(result.at[place], result_hbm.at[place], sems.at[g])

    def per_group(g, carry):
        numbers = ids_vmem[pl.ds(pl.multiple_of(g * SUB, SUB), SUB), :]
        part = message.at[pl.ds(pl.multiple_of(g * group, SUB), group)]
        for step in range(SUB // 2):

            def both(field):
                starts = [(2 * step + n) * rows + field * capacity for n in range(2)]
                return jnp.concatenate([part[start : start + capacity, :] for start in starts], axis=0)

            first = ((both(6) * TILE_Y + both(7)) * TILE_Z + both(8)).astype(jnp.int32)
            alive = jnp.zeros((SUB, LANES), jnp.int32)
            for j in range(2 * capacity):
                i, k = 2 * step + j // capacity, j % capacity
                base = i * rows
                tile = numbers[i, k]
                alive = jnp.where(row == j, tile, alive)
                safe = jnp.maximum(tile, 0)
                weight = None
                for dim in range(3):
                    start = base + (3 + dim) * capacity + k
                    fraction = part[start : start + 1, :]
                    along = least[dim] + slope[dim] * fraction
                    weight = along if weight is None else weight * along
                index = jnp.broadcast_to(first[j : j + 1], (SUB, LANES)) + shift
                for f in range(FLOWS):
                    held = jnp.broadcast_to(table[f, pl.ds(safe, 1), :], (SUB, LANES))
                    found = jnp.take_along_axis(held, index, axis=1, mode="promise_in_bounds")
                    products[(f * SUB + j) * SUB : (f * SUB + j + 1) * SUB, :] = found * weight
            live = alive >= 0
            sampled = []
            for f in range(FLOWS):
                total = products[pl.ds(f * SUB * SUB, SUB, stride=SUB), :]
                for c in range(1, SUB):
                    total = total + products[pl.ds(f * SUB * SUB + c, SUB, stride=SUB), :]
                sampled.append(total)

            mass_old = both(9)
            radius = jnp.exp(jnp.log(mass_old) * (1.0 / 3.0))
            factor = DRAG_RATE / (radius * radius)
            share = 1.0 / (1.0 + factor)
            gap = sampled[3]
            soft = jnp.maximum(gap, 0.0) + jnp.log(1.0 + jnp.exp(-jnp.abs(gap)))
            mass_new = jnp.where(live, mass_old / (1.0 + EVAPORATION * soft / radius), mass_old)
            vapour = mass_old - mass_new
            fields, sources = [], []
            for f in range(3):
                velocity = both(f)
                moved = jnp.where(live, (velocity + factor * sampled[f]) * share, velocity)
                fields.append(moved)
                sources.append(mass_old * (velocity - moved) + vapour * moved)
            fields.append(mass_new)
            sources.append(vapour)
            for dim in range(3):
                sources.append(both(3 + dim) + both(6 + dim))
            first_block = (g * SUB + 2 * step) * capacity
            out = result.at[pl.ds(pl.multiple_of(first_block * FLOWS, SUB), SUB * FLOWS)]
            for n in range(2):
                for f in range(FLOWS):
                    start = (n * FLOWS + f) * capacity
                    out[start : start + capacity, :] = fields[f][n * capacity : (n + 1) * capacity]
            out = source.at[pl.ds(pl.multiple_of(first_block * SUB, SUB), SUB * SUB)]
            for f in range(7):
                out[pl.ds(f, SUB, stride=SUB), :] = sources[f]
        returned(g).start()
        return carry

    lax.fori_loop(0, devices // SUB, per_group, 0)
    for g in range(devices // SUB):
        returned(g).wait()


def tent(position, cell):
    return jnp.maximum(0.0, 1.0 - jnp.abs(position - cell))


def deposit_kernel(
    ids_vmem, source, diffused, from_x0, from_x1, from_y0, from_y1, gas_next, total, ids, work, sems, *, capacity
):
    fields, extent_x, extent_z = from_y0.shape
    extent_y = from_x0.shape[1]
    across_y = extent_y // TILE_Y
    across_z = extent_z // TILE_Z
    blocks = source.shape[0] // SUB
    copy = pltpu.make_async_copy(ids_vmem, ids, sems.at[0])
    copy.start()
    fetch = pltpu.make_async_copy(diffused, work, sems.at[1])
    fetch.start()
    total[...] = jnp.zeros(total.shape, total.dtype)
    row = lax.broadcasted_iota(jnp.int32, (SUB, LANES), 0)
    along_z = row.astype(jnp.float32)
    along_y = (row % TILE_Y).astype(jnp.float32)
    along_x = (row // TILE_Y).astype(jnp.float32)
    copy.wait()

    def one(n):
        tile = jnp.maximum(ids[n // capacity, n % capacity], 0)
        held = source[pl.ds(pl.multiple_of(n * SUB, SUB), SUB), :]
        given = held[0:FLOWS]
        coarse = given.astype(jnp.bfloat16).astype(jnp.float32)
        left = jnp.concatenate([given, given - coarse], axis=0).astype(jnp.bfloat16)
        x, y, z = held[4:5], held[5:6], held[6:7]
        weight_z = tent(z, along_z)
        weight_y = tent(y, along_y)
        planes = []
        for part in range(2):
            weight_xy = tent(x, along_x + 2.0 * part) * weight_y
            for i in range(SUB):
                planes.append(weight_xy[i : i + 1] * weight_z)
        stencil = jnp.concatenate(planes, axis=0)
        high = stencil.astype(jnp.bfloat16)
        low = (stencil - high.astype(jnp.float32)).astype(jnp.bfloat16)
        right = jnp.concatenate([high, low], axis=0)
        sums = lax.dot_general(left, right, (((1,), (1,)), ((), ())), preferred_element_type=jnp.float32)
        return pl.multiple_of(tile * SUB, SUB), sums[:, :LANES] + sums[:, LANES:]

    unroll = 16

    def per_step(step, carry):
        made = [one(step * unroll + n) for n in range(unroll)]
        for start, sums in made:
            total[pl.ds(start, SUB), :] += sums
        return carry

    lax.fori_loop(0, blocks // unroll, per_step, 0)

    fetch.wait()
    last_x = (extent_x - 1) * extent_y
    for f in range(fields):
        work[f, 0:extent_y, :] += DIFFUSION * from_x0[f]
        work[f, last_x : last_x + extent_y, :] += DIFFUSION * from_x1[f]
        for h in range(extent_z // LANES):
            lanes = slice(h * LANES, (h + 1) * LANES)
            for line, face in ((0, from_y0), (extent_y - 1, from_y1)):
                for x in range(extent_x):
                    spot = x * extent_y + line
                    work[f, spot : spot + 1, lanes] += DIFFUSION * face[f, x : x + 1, lanes]

    def sent(a):
        place = pl.ds(pl.multiple_of(a * TILE_X * extent_y, SUB), TILE_X * extent_y)
        return pltpu.make_async_copy(work.at[:, place], gas_next.at[:, place], sems.at[2 + a])

    def per_a(a, carry):
        held = work.at[:, pl.ds(pl.multiple_of(a * TILE_X * extent_y, SUB), TILE_X * extent_y)]
        for b in range(across_y):
            for h in range(extent_z // LANES):
                start = ((a * across_y + b) * across_z + h * GRANULES) * SUB
                part = total.at[pl.ds(pl.multiple_of(start, SUB), GRANULES * SUB)]
                lanes = slice(h * LANES, (h + 1) * LANES)
                for f in range(FLOWS):
                    pair = [
                        part[pl.ds(n * SUB * SUB + f, SUB, stride=SUB), :]
                        + part[pl.ds(n * SUB * SUB + f + FLOWS, SUB, stride=SUB), :]
                        for n in range(2)
                    ]
                    pair = [x * (1.0 / CELL_MASS) for x in exchange(*pair)]
                    for u in range(TILE_X):
                        piece = pair[u // 2][(u % 2) * TILE_Y : (u % 2 + 1) * TILE_Y]
                        spot = u * extent_y + b * TILE_Y
                        lines = slice(spot, spot + TILE_Y)
                        if f < 3:
                            held[f, lines, lanes] += piece
                        else:
                            held[3, lines, lanes] -= LATENT_HEAT * piece
                            held[4, lines, lanes] += piece
        sent(a).start()
        return carry

    lax.fori_loop(0, extent_x // TILE_X, per_a, 0)
    for a in range(extent_x // TILE_X):
        sent(a).wait()


def unpack_kernel(result, speed, mass, sems):
    vector = speed.shape[2]
    copies = []
    for i in range(speed.shape[0]):
        copies.append(pltpu.make_async_copy(result.at[:, i, :vector], speed.at[i], sems.at[2 * i]))
        copies.append(pltpu.make_async_copy(result.at[:, i, vector:], mass.at[i], sems.at[2 * i + 1]))
    for copy in copies:
        copy.start()
    for copy in copies:
        copy.wait()


def specs(spaces):
    return [pl.BlockSpec(memory_space=space) for space in spaces]


def call(kernel, out_shape, scratch=(), flops=0, moved=0, ins=None, outs=None):
    extra = {}
    if ins is not None:
        extra["in_specs"] = specs(ins)
    if outs is not None:
        extra["out_specs"] = specs(outs) if len(outs) > 1 else specs(outs)[0]
        if pltpu.HBM in outs:
            shapes = out_shape if len(outs) > 1 else (out_shape,)
            shapes = [pltpu.HBM(o.shape, o.dtype) if space == pltpu.HBM else o for o, space in zip(shapes, outs)]
            out_shape = shapes if len(outs) > 1 else shapes[0]
    called = pl.pallas_call(
        kernel,
        out_shape=out_shape,
        scratch_shapes=scratch,
        cost_estimate=pl.CostEstimate(flops=flops, bytes_accessed=moved, transcendentals=0),
        compiler_params=pltpu.CompilerParams(vmem_limit_bytes=32 * 1024 * 1024),
        **extra,
    )

    def with_spaces(*values):
        if ins is not None:
            values = [
                pltpu.with_memory_space_constraint(v, space) if space == pltpu.HBM else v
                for v, space in zip(values, ins)
            ]
        return called(*values)

    return with_spaces


def step(gas_state, parcel_speed, parcel_mass, offsets, cell_base, block_tile, block_count):
    fields, extent_x, extent_y, extent_z = gas_state.shape
    devices, capacity = block_tile.shape[2:]
    rows = 10 * capacity + 1
    tiles = (extent_x // TILE_X) * (extent_y // TILE_Y) * (extent_z // TILE_Z)
    f32 = jnp.float32

    def shape(*dims, dtype=f32):
        return jax.ShapeDtypeStruct(dims, dtype)

    vector = 3 * capacity
    blocks = devices * capacity
    across_i, across_j = lax.axis_size("gx"), lax.axis_size("yz")
    parts = max(1, across_j // 2)
    i32 = jnp.int32
    hbm, vmem = pltpu.HBM, pltpu.VMEM
    dma = pltpu.SemaphoreType.DMA

    def by_component(value):
        return value[0, 0].transpose(0, 2, 1, 3).reshape(across_i, across_j * vector, LANES)

    message = call(
        functools.partial(pack_kernel, rows=rows, capacity=capacity, parts=parts),
        shape(devices * rows, LANES),
        scratch=[
            vmem((across_i, across_j * vector, LANES), f32),
            vmem((across_i, across_j * capacity, LANES), f32),
            vmem((across_i, across_j * vector, LANES), f32),
            vmem((across_i, across_j * vector, LANES), i32),
            vmem((capacity, devices), i32),
            vmem((1, devices), i32),
            vmem((devices, LANES), f32),
            vmem((devices * rows, LANES), f32),
            dma((2 + 5 * parts,)),
        ],
        ins=[hbm] * 6,
        outs=[hbm],
    )(
        by_component(parcel_speed),
        parcel_mass.reshape(across_i, across_j * capacity, LANES),
        by_component(offsets),
        by_component(cell_base),
        block_tile[0, 0].T,
        block_count[0],
    )
    message = lax.all_to_all(message.reshape(devices, rows, 1, LANES), BOTH, split_axis=0, concat_axis=0, tiled=True)
    message = message.reshape(devices * rows, LANES)

    face = shape(fields, extent_x, extent_z)
    side = shape(fields, extent_y, extent_z)
    whole = vmem(gas_state.shape, f32)
    flat = (fields, extent_x * extent_y, extent_z)
    face_x0, face_x1, face_y0, face_y1 = call(
        faces_kernel, (side, side, face, face), scratch=[whole, dma(())], ins=[hbm], outs=[vmem] * 4
    )(gas_state)

    def shifted(value, axis, step):
        count = lax.axis_size(axis)
        pairs = [(i, i + step) for i in range(count) if 0 <= i + step < count]
        return lax.ppermute(value, axis, pairs)

    halo = (
        shifted(face_x1, "gx", 1), shifted(face_x0, "gx", -1), shifted(face_y1, "yz", 1), shifted(face_y0, "yz", -1)
    )
    table, diffused = call(
        local_kernel,
        (shape(FLOWS, tiles, LANES), shape(*flat)),
        scratch=[whole, vmem(flat, f32), dma((fields + 1,))],
        flops=10**7,
        ins=[hbm],
        outs=[vmem, hbm],
    )(gas_state)
    message, table, diffused = lax.optimization_barrier((message, table, diffused))

    result, source, ids = call(
        functools.partial(update_kernel, rows=rows, capacity=capacity),
        (shape(blocks * FLOWS, LANES), shape(blocks * SUB, LANES), shape(devices, LANES, dtype=i32)),
        scratch=[
            vmem((FLOWS * SUB * SUB, LANES), f32),
            vmem((blocks * FLOWS, LANES), f32),
            dma((devices // SUB,)),
        ],
        flops=10**7,
        ins=[vmem, vmem],
        outs=[hbm, vmem, vmem],
    )(message, table)
    result = lax.all_to_all(
        result.reshape(devices, capacity * FLOWS, 1, LANES), BOTH, split_axis=0, concat_axis=0, tiled=True
    )
    gas_next = call(
        functools.partial(deposit_kernel, capacity=capacity),
        shape(*flat),
        scratch=[
            vmem((tiles * SUB, LANES), f32),
            pltpu.SMEM((devices, LANES), i32),
            vmem(flat, f32),
            dma((2 + extent_x // TILE_X,)),
        ],
        flops=3 * 10**7,
        ins=[vmem, vmem, hbm] + [vmem] * 4,
        outs=[hbm],
    )(ids, source, diffused, *halo)
    speed_next, mass_next = call(
        unpack_kernel,
        (shape(across_i, across_j, vector, 1, LANES), shape(across_i, across_j, capacity, 1, LANES)),
        scratch=[dma((2 * across_i,))],
        ins=[vmem],
        outs=[hbm, hbm],
    )(result.reshape(across_j, across_i, capacity * FLOWS, 1, LANES))
    speed_next = speed_next.reshape(devices, 3, capacity, LANES).transpose(0, 2, 1, 3)
    return gas_next.reshape(gas_state.shape), speed_next.reshape(parcel_speed.shape), mass_next.reshape(parcel_mass.shape)


def solution(mesh):
    in_specs = (
        P(None, "gx", "yz", None),
        P("gx", "yz", None, None, None, None),
        P("gx", "yz", None, None, None),
        P("gx", "yz", None, None, None, None),
        P("gx", "yz", None, None, None, None),
        P("gx", "yz", None, None),
        P("gx", "yz", None),
    )
    out_specs = (
        P(None, "gx", "yz", None),
        P("gx", "yz", None, None, None, None),
        P("gx", "yz", None, None, None),
    )
    return jax.shard_map(step, mesh=mesh, in_specs=in_specs, out_specs=out_specs, check_vma=False)
```

```python
import functools

import jax
import jax.numpy as jnp
from jax import lax
from jax.experimental import pallas as pl
from jax.experimental.pallas import tpu as pltpu
from jax.sharding import PartitionSpec as P


TILE_X = 4
TILE_Y = 4
TILE_Z = 8
DIFFUSION = 0.1
CELL_MASS = 4.0
DRAG_RATE = 0.5
EVAPORATION = 0.3
LATENT_HEAT = 2.0

LANES = 128
SUB = 8
GRANULES = LANES // TILE_Z
FLOWS = 4
BOTH = ("yz", "gx")


def roll(x, shift, axis):
    shift = shift % x.shape[axis]
    return pltpu.roll(x, shift, axis) if shift else x


def pick(x, rows):
    return jnp.take_along_axis(x, rows, axis=0, mode="promise_in_bounds")


def exchange(upper, lower):
    row = lax.broadcasted_iota(jnp.int32, (SUB, LANES), 0)
    granule = lax.broadcasted_iota(jnp.int32, (SUB, LANES), 1) // TILE_Z
    half = LANES // 2
    turned = [
        pltpu.roll(x, shift, 1, stride=TILE_Z, stride_axis=0) for x, shift in ((upper, 0), (lower, half))
    ]
    back = SUB - 1 - row
    pair = []
    for part in range(2):
        wanted = (granule - back - SUB * part) % GRANULES
        mixed = jnp.where(wanted < SUB, pick(turned[0], wanted % SUB), pick(turned[1], wanted % SUB))
        shift = (-TILE_Z * (SUB - 1) - half * part) % LANES
        pair.append(pick(pltpu.roll(mixed, shift, 1, stride=TILE_Z, stride_axis=0), back))
    return pair


def pack_kernel(
    speed, mass, offsets, cells, tile_ids, counts, message,
    speed_v, mass_v, offsets_v, cells_v, tile_ids_v, counts_v, ids_v, message_v, sems, *, rows, capacity, parts
):
    across_i = speed.shape[0]
    vector = 3 * capacity
    across_j = speed.shape[1] // vector
    each = across_j // parts
    sources = ((speed, speed_v, vector), (offsets, offsets_v, vector), (cells, cells_v, vector), (mass, mass_v, capacity))
    small = [
        pltpu.make_async_copy(tile_ids, tile_ids_v, sems.at[0]),
        pltpu.make_async_copy(counts, counts_v, sems.at[1]),
    ]
    taken = []
    for copy in small:
        copy.start()
    for part in range(parts):
        taken.append([])
        for n, (source, held, count) in enumerate(sources):
            place = pl.ds(part * each * count, each * count)
            copy = pltpu.make_async_copy(source.at[:, place], held.at[:, place], sems.at[2 + part * 5 + n])
            copy.start()
            taken[-1].append(copy)
    for copy in small:
        copy.wait()
    slot = lax.broadcasted_iota(jnp.int32, tile_ids_v.shape, 0)
    ids = jnp.where(slot < counts_v[...], tile_ids_v[...], -1).astype(jnp.float32)
    ids_v[...] = jnp.concatenate([ids, jnp.zeros((LANES - capacity, ids.shape[1]), jnp.float32)], axis=0).T

    sent = []
    for part in range(parts):
        for copy in taken[part]:
            copy.wait()
        for j in range(part * each, (part + 1) * each):
            for i in range(across_i):
                base = (j * across_i + i) * rows
                place = slice(j * vector, (j + 1) * vector)
                message_v[base : base + vector, :] = speed_v[i, place, :]
                message_v[base + vector : base + 2 * vector, :] = offsets_v[i, place, :]
                message_v[base + 2 * vector : base + 3 * vector, :] = cells_v[i, place, :].astype(jnp.float32)
                base += 3 * vector
                message_v[base : base + capacity, :] = mass_v[i, j * capacity : (j + 1) * capacity, :]
                owner = i * across_j + j
                message_v[base + capacity : base + capacity + 1, :] = ids_v[owner : owner + 1, :]
        place = pl.ds(part * each * across_i * rows, each * across_i * rows)
        copy = pltpu.make_async_copy(message_v.at[place], message.at[place], sems.at[2 + part * 5 + 4])
        copy.start()
        sent.append(copy)
    for copy in sent:
        copy.wait()


def faces_kernel(gas_hbm, face_x0, face_x1, face_y0, face_y1, gas, sem):
    extent_x, extent_y = gas_hbm.shape[1:3]
    copy = pltpu.make_async_copy(gas_hbm, gas, sem)
    copy.start()
    copy.wait()
    face_x0[...] = gas[:, 0]
    face_x1[...] = gas[:, extent_x - 1]
    face_y0[...] = gas[:, :, 0, :]
    face_y1[...] = gas[:, :, extent_y - 1, :]


def local_kernel(gas_hbm, table, diffused_hbm, gas, diffused, sems):
    fields, extent_x, extent_y, extent_z = gas.shape
    across_y = extent_y // TILE_Y
    across_z = extent_z // TILE_Z
    lane = lax.broadcasted_iota(jnp.int32, (extent_y, extent_z), 1)
    line = lax.broadcasted_iota(jnp.int32, (extent_y, extent_z), 0)
    copy = pltpu.make_async_copy(gas_hbm, gas, sems.at[fields])
    copy.start()
    copy.wait()

    def sent(f):
        return pltpu.make_async_copy(diffused.at[f], diffused_hbm.at[f], sems.at[f])

    def per_field(f, carry):
        for x in range(extent_x):
            centre = gas[f, x]
            beside = jnp.where(line == 0, 0.0, roll(centre, 1, 0))
            beside += jnp.where(line == extent_y - 1, 0.0, roll(centre, -1, 0))
            beside += jnp.where(lane == 0, 0.0, roll(centre, 1, 1))
            beside += jnp.where(lane == extent_z - 1, 0.0, roll(centre, -1, 1))
            if x > 0:
                beside += gas[f, x - 1]
            if x < extent_x - 1:
                beside += gas[f, x + 1]
            diffused[f, x * extent_y : (x + 1) * extent_y, :] = centre + DIFFUSION * (beside - 6.0 * centre)
        sent(f).start()
        return carry

    lax.fori_loop(0, fields, per_field, 0)

    def per_a(a, carry):
        for f in range(FLOWS):
            for b in range(across_y):
                for h in range(extent_z // LANES):
                    lanes = slice(h * LANES, (h + 1) * LANES)
                    rows = slice(b * TILE_Y, (b + 1) * TILE_Y)
                    parts = []
                    for u in range(TILE_X):
                        piece = gas[f, a * TILE_X + u, rows, lanes]
                        if f == 3:
                            piece = piece - gas[4, a * TILE_X + u, rows, lanes]
                        parts.append(piece)
                    pair = exchange(jnp.concatenate(parts[:2], 0), jnp.concatenate(parts[2:], 0))
                    start = pl.multiple_of((a * across_y + b) * across_z + h * GRANULES, SUB)
                    table[f, pl.ds(start, SUB), :] = pair[0]
                    table[f, pl.ds(start + SUB, SUB), :] = pair[1]
        return carry

    lax.fori_loop(0, extent_x // TILE_X, per_a, 0)
    for f in range(fields):
        sent(f).wait()


def paired(ref, member, stride, offset, capacity):
    starts = [(member + n) * stride + offset for n in range(2)]
    return jnp.concatenate([ref[start : start + capacity, :] for start in starts], axis=0)


def update_kernel(
    message, table, result_hbm, result, ids_vmem, products, turned, sems, *, rows, capacity
):
    devices = message.shape[0] // rows
    group = SUB * rows
    for g in range(devices // SUB):
        ids_vmem[g * SUB : (g + 1) * SUB, :] = message[pl.ds(g * group + rows - 1, SUB, stride=rows), :].astype(jnp.int32)
    for k in range(capacity):
        turned[k] = roll(ids_vmem[...], -k, 1)
    corner = lax.broadcasted_iota(jnp.int32, (SUB, LANES), 0)
    high = [(corner & bit) != 0 for bit in (4, 2, 1)]
    least = [jnp.where(h, 0.0, 1.0) for h in high]
    slope = [jnp.where(h, 1.0, -1.0) for h in high]
    shift = (
        jnp.where(high[0], TILE_Y * TILE_Z, 0) + jnp.where(high[1], TILE_Z, 0) + jnp.where(high[2], 1, 0)
    )
    row = corner

    def returned(g):
        place = pl.ds(pl.multiple_of(g * SUB * capacity * FLOWS, SUB), SUB * capacity * FLOWS)
        return pltpu.make_async_copy(result.at[place], result_hbm.at[place], sems.at[g])

    def per_group(g, carry):
        here = pl.ds(pl.multiple_of(g * SUB, SUB), SUB)
        numbers = [turned[k, here, :] for k in range(capacity)]
        part = message.at[pl.ds(pl.multiple_of(g * group, SUB), group)]
        for step in range(SUB // 2):

            def both(field):
                return paired(part, 2 * step, rows, field * capacity, capacity)

            first = ((both(6) * TILE_Y + both(7)) * TILE_Z + both(8)).astype(jnp.int32)
            alive = jnp.zeros((SUB, LANES), jnp.int32)
            for j in range(2 * capacity):
                i, k = 2 * step + j // capacity, j % capacity
                base = i * rows
                tile = numbers[k][i, 0]
                alive = jnp.where(row == j, tile, alive)
                safe = jnp.maximum(tile, 0)
                weight = None
                for dim in range(3):
                    start = base + (3 + dim) * capacity + k
                    fraction = part[start : start + 1, :]
                    along = least[dim] + slope[dim] * fraction
                    weight = along if weight is None else weight * along
                index = jnp.broadcast_to(first[j : j + 1], (SUB, LANES)) + shift
                for f in range(FLOWS):
                    held = jnp.broadcast_to(table[f, pl.ds(safe, 1), :], (SUB, LANES))
                    found = jnp.take_along_axis(held, index, axis=1, mode="promise_in_bounds")
                    products[(f * SUB + j) * SUB : (f * SUB + j + 1) * SUB, :] = found * weight
            live = alive >= 0
            sampled = []
            for f in range(FLOWS):
                total = products[pl.ds(f * SUB * SUB, SUB, stride=SUB), :]
                for c in range(1, SUB):
                    total = total + products[pl.ds(f * SUB * SUB + c, SUB, stride=SUB), :]
                sampled.append(total)

            mass_old = both(9)
            radius = jnp.exp(jnp.log(mass_old) * (1.0 / 3.0))
            factor = DRAG_RATE / (radius * radius)
            share = 1.0 / (1.0 + factor)
            gap = sampled[3]
            soft = jnp.maximum(gap, 0.0) + jnp.log(1.0 + jnp.exp(-jnp.abs(gap)))
            mass_new = jnp.where(live, mass_old / (1.0 + EVAPORATION * soft / radius), mass_old)
            fields = [
                jnp.where(live, (both(f) + factor * sampled[f]) * share, both(f)) for f in range(3)
            ] + [mass_new]
            first_block = (g * SUB + 2 * step) * capacity
            out = result.at[pl.ds(pl.multiple_of(first_block * FLOWS, SUB), SUB * FLOWS)]
            for n in range(2):
                for f in range(FLOWS):
                    start = (n * FLOWS + f) * capacity
                    out[start : start + capacity, :] = fields[f][n * capacity : (n + 1) * capacity]
        returned(g).start()
        return carry

    lax.fori_loop(0, devices // SUB, per_group, 0)
    for g in range(devices // SUB):
        returned(g).wait()


def tent(position, cell):
    return jnp.maximum(0.0, 1.0 - jnp.abs(position - cell))


def deposit_kernel(
    ids_vmem, message, result, diffused, from_x0, from_x1, from_y0, from_y1, gas_next,
    total, source, ids, work, sems, *, rows, capacity
):
    fields, extent_x, extent_z = from_y0.shape
    extent_y = from_x0.shape[1]
    across_y = extent_y // TILE_Y
    across_z = extent_z // TILE_Z
    blocks = source.shape[0] // SUB
    group = SUB * rows
    spread = capacity * FLOWS
    copy = pltpu.make_async_copy(ids_vmem, ids, sems.at[0])
    copy.start()
    fetch = pltpu.make_async_copy(diffused, work, sems.at[1])
    fetch.start()
    total[...] = jnp.zeros(total.shape, total.dtype)

    def per_group(g, carry):
        part = message.at[pl.ds(pl.multiple_of(g * group, SUB), group)]
        updated = result.at[pl.ds(pl.multiple_of(g * SUB * spread, SUB), SUB * spread)]
        out = source.at[pl.ds(pl.multiple_of(g * SUB * SUB * capacity, SUB), SUB * SUB * capacity)]
        for step in range(SUB // 2):

            def before(field):
                return paired(part, 2 * step, rows, field * capacity, capacity)

            def after(field):
                return paired(updated, 2 * step, spread, field * capacity, capacity)

            mass_old = before(9)
            vapour = mass_old - after(3)
            found = [mass_old * (before(f) - after(f)) + vapour * after(f) for f in range(3)] + [vapour]
            found += [before(3 + dim) + before(6 + dim) for dim in range(3)]
            for f, value in enumerate(found):
                out[pl.ds(2 * step * capacity * SUB + f, 2 * capacity, stride=SUB), :] = value
        return carry

    lax.fori_loop(0, blocks // (SUB * capacity), per_group, 0)
    row = lax.broadcasted_iota(jnp.int32, (SUB, LANES), 0)
    along_z = row.astype(jnp.float32)
    along_y = (row % TILE_Y).astype(jnp.float32)
    along_x = (row // TILE_Y).astype(jnp.float32)
    copy.wait()

    def one(n):
        tile = jnp.maximum(ids[n // capacity, n % capacity], 0)
        held = source[pl.ds(pl.multiple_of(n * SUB, SUB), SUB), :]
        given = held[0:FLOWS]
        coarse = given.astype(jnp.bfloat16).astype(jnp.float32)
        left = jnp.concatenate([given, given - coarse], axis=0).astype(jnp.bfloat16)
        x, y, z = held[4:5], held[5:6], held[6:7]
        weight_z = tent(z, along_z)
        weight_y = tent(y, along_y)
        planes = []
        for part in range(2):
            weight_xy = tent(x, along_x + 2.0 * part) * weight_y
            for i in range(SUB):
                planes.append(weight_xy[i : i + 1] * weight_z)
        stencil = jnp.concatenate(planes, axis=0)
        high = stencil.astype(jnp.bfloat16)
        low = (stencil - high.astype(jnp.float32)).astype(jnp.bfloat16)
        right = jnp.concatenate([high, low], axis=0)
        sums = lax.dot_general(left, right, (((1,), (1,)), ((), ())), preferred_element_type=jnp.float32)
        return pl.multiple_of(tile * SUB, SUB), sums[:, :LANES] + sums[:, LANES:]

    unroll = 16

    def per_step(step, carry):
        made = [one(step * unroll + n) for n in range(unroll)]
        for start, sums in made:
            total[pl.ds(start, SUB), :] += sums
        return carry

    lax.fori_loop(0, blocks // unroll, per_step, 0)

    fetch.wait()
    last_x = (extent_x - 1) * extent_y
    for f in range(fields):
        work[f, 0:extent_y, :] += DIFFUSION * from_x0[f]
        work[f, last_x : last_x + extent_y, :] += DIFFUSION * from_x1[f]
        for h in range(extent_z // LANES):
            lanes = slice(h * LANES, (h + 1) * LANES)
            for line, face in ((0, from_y0), (extent_y - 1, from_y1)):
                for x in range(extent_x):
                    spot = x * extent_y + line
                    work[f, spot : spot + 1, lanes] += DIFFUSION * face[f, x : x + 1, lanes]

    def sent(a):
        place = pl.ds(pl.multiple_of(a * TILE_X * extent_y, SUB), TILE_X * extent_y)
        return pltpu.make_async_copy(work.at[:, place], gas_next.at[:, place], sems.at[2 + a])

    def per_a(a, carry):
        held = work.at[:, pl.ds(pl.multiple_of(a * TILE_X * extent_y, SUB), TILE_X * extent_y)]
        for b in range(across_y):
            for h in range(extent_z // LANES):
                start = ((a * across_y + b) * across_z + h * GRANULES) * SUB
                part = total.at[pl.ds(pl.multiple_of(start, SUB), GRANULES * SUB)]
                lanes = slice(h * LANES, (h + 1) * LANES)
                for f in range(FLOWS):
                    pair = [
                        part[pl.ds(n * SUB * SUB + f, SUB, stride=SUB), :]
                        + part[pl.ds(n * SUB * SUB + f + FLOWS, SUB, stride=SUB), :]
                        for n in range(2)
                    ]
                    pair = [x * (1.0 / CELL_MASS) for x in exchange(*pair)]
                    for u in range(TILE_X):
                        piece = pair[u // 2][(u % 2) * TILE_Y : (u % 2 + 1) * TILE_Y]
                        spot = u * extent_y + b * TILE_Y
                        lines = slice(spot, spot + TILE_Y)
                        if f < 3:
                            held[f, lines, lanes] += piece
                        else:
                            held[3, lines, lanes] -= LATENT_HEAT * piece
                            held[4, lines, lanes] += piece
        sent(a).start()
        return carry

    lax.fori_loop(0, extent_x // TILE_X, per_a, 0)
    for a in range(extent_x // TILE_X):
        sent(a).wait()


def unpack_kernel(result, speed, mass, sems):
    vector = speed.shape[2]
    copies = []
    for i in range(speed.shape[0]):
        copies.append(pltpu.make_async_copy(result.at[:, i, :vector], speed.at[i], sems.at[2 * i]))
        copies.append(pltpu.make_async_copy(result.at[:, i, vector:], mass.at[i], sems.at[2 * i + 1]))
    for copy in copies:
        copy.start()
    for copy in copies:
        copy.wait()


def specs(spaces):
    return [pl.BlockSpec(memory_space=space) for space in spaces]


def call(kernel, out_shape, scratch=(), flops=0, moved=0, ins=None, outs=None):
    extra = {}
    if ins is not None:
        extra["in_specs"] = specs(ins)
    if outs is not None:
        extra["out_specs"] = specs(outs) if len(outs) > 1 else specs(outs)[0]
        if pltpu.HBM in outs:
            shapes = out_shape if len(outs) > 1 else (out_shape,)
            shapes = [pltpu.HBM(o.shape, o.dtype) if space == pltpu.HBM else o for o, space in zip(shapes, outs)]
            out_shape = shapes if len(outs) > 1 else shapes[0]
    called = pl.pallas_call(
        kernel,
        out_shape=out_shape,
        scratch_shapes=scratch,
        cost_estimate=pl.CostEstimate(flops=flops, bytes_accessed=moved, transcendentals=0),
        compiler_params=pltpu.CompilerParams(vmem_limit_bytes=32 * 1024 * 1024),
        **extra,
    )

    def with_spaces(*values):
        if ins is not None:
            values = [
                pltpu.with_memory_space_constraint(v, space) if space == pltpu.HBM else v
                for v, space in zip(values, ins)
            ]
        return called(*values)

    return with_spaces


def step(gas_state, parcel_speed, parcel_mass, offsets, cell_base, block_tile, block_count):
    fields, extent_x, extent_y, extent_z = gas_state.shape
    devices, capacity = block_tile.shape[2:]
    rows = 10 * capacity + 1
    tiles = (extent_x // TILE_X) * (extent_y // TILE_Y) * (extent_z // TILE_Z)
    f32 = jnp.float32

    def shape(*dims, dtype=f32):
        return jax.ShapeDtypeStruct(dims, dtype)

    vector = 3 * capacity
    blocks = devices * capacity
    across_i, across_j = lax.axis_size("gx"), lax.axis_size("yz")
    parts = max(1, across_j // 2)
    i32 = jnp.int32
    hbm, vmem = pltpu.HBM, pltpu.VMEM
    dma = pltpu.SemaphoreType.DMA

    def by_component(value):
        return value[0, 0].transpose(0, 2, 1, 3).reshape(across_i, across_j * vector, LANES)

    message = call(
        functools.partial(pack_kernel, rows=rows, capacity=capacity, parts=parts),
        shape(devices * rows, LANES),
        scratch=[
            vmem((across_i, across_j * vector, LANES), f32),
            vmem((across_i, across_j * capacity, LANES), f32),
            vmem((across_i, across_j * vector, LANES), f32),
            vmem((across_i, across_j * vector, LANES), i32),
            vmem((capacity, devices), i32),
            vmem((1, devices), i32),
            vmem((devices, LANES), f32),
            vmem((devices * rows, LANES), f32),
            dma((2 + 5 * parts,)),
        ],
        ins=[hbm] * 6,
        outs=[hbm],
    )(
        by_component(parcel_speed),
        parcel_mass.reshape(across_i, across_j * capacity, LANES),
        by_component(offsets),
        by_component(cell_base),
        block_tile[0, 0].T,
        block_count[0],
    )
    message = lax.all_to_all(message.reshape(devices, rows, 1, LANES), BOTH, split_axis=0, concat_axis=0, tiled=True)
    message = message.reshape(devices * rows, LANES)

    face = shape(fields, extent_x, extent_z)
    side = shape(fields, extent_y, extent_z)
    whole = vmem(gas_state.shape, f32)
    flat = (fields, extent_x * extent_y, extent_z)
    face_x0, face_x1, face_y0, face_y1 = call(
        faces_kernel, (side, side, face, face), scratch=[whole, dma(())], ins=[hbm], outs=[vmem] * 4
    )(gas_state)

    def shifted(value, axis, step):
        count = lax.axis_size(axis)
        pairs = [(i, i + step) for i in range(count) if 0 <= i + step < count]
        return lax.ppermute(value, axis, pairs)

    halo = (
        shifted(face_x1, "gx", 1), shifted(face_x0, "gx", -1), shifted(face_y1, "yz", 1), shifted(face_y0, "yz", -1)
    )
    table, diffused = call(
        local_kernel,
        (shape(FLOWS, tiles, LANES), shape(*flat)),
        scratch=[whole, vmem(flat, f32), dma((fields + 1,))],
        flops=10**7,
        ins=[hbm],
        outs=[vmem, hbm],
    )(gas_state)
    message, table, diffused = lax.optimization_barrier((message, table, diffused))

    returned, result, ids = call(
        functools.partial(update_kernel, rows=rows, capacity=capacity),
        (shape(blocks * FLOWS, LANES), shape(blocks * FLOWS, LANES), shape(devices, LANES, dtype=i32)),
        scratch=[
            vmem((FLOWS * SUB * SUB, LANES), f32),
            vmem((capacity, devices, LANES), i32),
            dma((devices // SUB,)),
        ],
        flops=10**7,
        ins=[vmem, vmem],
        outs=[hbm, vmem, vmem],
    )(message, table)
    returned = lax.all_to_all(
        returned.reshape(devices, capacity * FLOWS, 1, LANES), BOTH, split_axis=0, concat_axis=0, tiled=True
    )
    gas_next = call(
        functools.partial(deposit_kernel, rows=rows, capacity=capacity),
        shape(*flat),
        scratch=[
            vmem((tiles * SUB, LANES), f32),
            vmem((blocks * SUB, LANES), f32),
            pltpu.SMEM((devices, LANES), i32),
            vmem(flat, f32),
            dma((2 + extent_x // TILE_X,)),
        ],
        flops=3 * 10**7,
        ins=[vmem, vmem, vmem, hbm] + [vmem] * 4,
        outs=[hbm],
    )(ids, message, result, diffused, *halo)
    speed_next, mass_next = call(
        unpack_kernel,
        (shape(across_i, across_j, vector, 1, LANES), shape(across_i, across_j, capacity, 1, LANES)),
        scratch=[dma((2 * across_i,))],
        ins=[vmem],
        outs=[hbm, hbm],
    )(returned.reshape(across_j, across_i, capacity * FLOWS, 1, LANES))
    speed_next = speed_next.reshape(devices, 3, capacity, LANES).transpose(0, 2, 1, 3)
    return gas_next.reshape(gas_state.shape), speed_next.reshape(parcel_speed.shape), mass_next.reshape(parcel_mass.shape)


def solution(mesh):
    in_specs = (
        P(None, "gx", "yz", None),
        P("gx", "yz", None, None, None, None),
        P("gx", "yz", None, None, None),
        P("gx", "yz", None, None, None, None),
        P("gx", "yz", None, None, None, None),
        P("gx", "yz", None, None),
        P("gx", "yz", None),
    )
    out_specs = (
        P(None, "gx", "yz", None),
        P("gx", "yz", None, None, None, None),
        P("gx", "yz", None, None, None),
    )
    return jax.shard_map(step, mesh=mesh, in_specs=in_specs, out_specs=out_specs, check_vma=False)
```

```python
import functools

import jax
import jax.numpy as jnp
from jax import lax
from jax.experimental import pallas as pl
from jax.experimental.pallas import tpu as pltpu
from jax.sharding import PartitionSpec as P


TILE_X = 4
TILE_Y = 4
TILE_Z = 8
DIFFUSION = 0.1
CELL_MASS = 4.0
DRAG_RATE = 0.5
EVAPORATION = 0.3
LATENT_HEAT = 2.0

LANES = 128
SUB = 8
GRANULES = LANES // TILE_Z
FLOWS = 4
SENT = ("yz", "gx")
RETURNED = ("gx", "yz")


def roll(x, shift, axis):
    shift = shift % x.shape[axis]
    return pltpu.roll(x, shift, axis) if shift else x


def pick(x, rows):
    return jnp.take_along_axis(x, rows, axis=0, mode="promise_in_bounds")


def exchange(upper, lower):
    row = lax.broadcasted_iota(jnp.int32, (SUB, LANES), 0)
    granule = lax.broadcasted_iota(jnp.int32, (SUB, LANES), 1) // TILE_Z
    half = LANES // 2
    turned = [
        pltpu.roll(x, shift, 1, stride=TILE_Z, stride_axis=0) for x, shift in ((upper, 0), (lower, half))
    ]
    back = SUB - 1 - row
    pair = []
    for part in range(2):
        wanted = (granule - back - SUB * part) % GRANULES
        mixed = jnp.where(wanted < SUB, pick(turned[0], wanted % SUB), pick(turned[1], wanted % SUB))
        shift = (-TILE_Z * (SUB - 1) - half * part) % LANES
        pair.append(pick(pltpu.roll(mixed, shift, 1, stride=TILE_Z, stride_axis=0), back))
    return pair


def pack_kernel(
    speed, mass, offsets, cells, tile_ids, counts, message,
    speed_v, mass_v, offsets_v, cells_v, tile_ids_v, counts_v, ids_v, message_v, sems, *, rows, capacity, parts
):
    across_i = speed.shape[0]
    vector = 3 * capacity
    across_j = speed.shape[1] // vector
    each = across_j // parts
    sources = ((speed, speed_v, vector), (offsets, offsets_v, vector), (cells, cells_v, vector), (mass, mass_v, capacity))
    small = [
        pltpu.make_async_copy(tile_ids, tile_ids_v, sems.at[0]),
        pltpu.make_async_copy(counts, counts_v, sems.at[1]),
    ]
    taken = []
    for copy in small:
        copy.start()
    for part in range(parts):
        taken.append([])
        for n, (source, held, count) in enumerate(sources):
            place = pl.ds(part * each * count, each * count)
            copy = pltpu.make_async_copy(source.at[:, place], held.at[:, place], sems.at[2 + part * 5 + n])
            copy.start()
            taken[-1].append(copy)
    for copy in small:
        copy.wait()
    slot = lax.broadcasted_iota(jnp.int32, tile_ids_v.shape, 0)
    ids = jnp.where(slot < counts_v[...], tile_ids_v[...], -1).astype(jnp.float32)
    ids_v[...] = jnp.concatenate([ids, jnp.zeros((LANES - capacity, ids.shape[1]), jnp.float32)], axis=0).T

    sent = []
    for part in range(parts):
        for copy in taken[part]:
            copy.wait()
        for j in range(part * each, (part + 1) * each):
            for i in range(across_i):
                base = (j * across_i + i) * rows
                place = slice(j * vector, (j + 1) * vector)
                message_v[base : base + vector, :] = speed_v[i, place, :]
                message_v[base + vector : base + 2 * vector, :] = offsets_v[i, place, :]
                message_v[base + 2 * vector : base + 3 * vector, :] = cells_v[i, place, :].astype(jnp.float32)
                base += 3 * vector
                message_v[base : base + capacity, :] = mass_v[i, j * capacity : (j + 1) * capacity, :]
                owner = i * across_j + j
                message_v[base + capacity : base + capacity + 1, :] = ids_v[owner : owner + 1, :]
        place = pl.ds(part * each * across_i * rows, each * across_i * rows)
        copy = pltpu.make_async_copy(message_v.at[place], message.at[place], sems.at[2 + part * 5 + 4])
        copy.start()
        sent.append(copy)
    for copy in sent:
        copy.wait()


def faces_kernel(gas_hbm, face_x0, face_x1, face_y0, face_y1, gas, sem):
    extent_x, extent_y = gas_hbm.shape[1:3]
    copy = pltpu.make_async_copy(gas_hbm, gas, sem)
    copy.start()
    copy.wait()
    face_x0[...] = gas[:, 0]
    face_x1[...] = gas[:, extent_x - 1]
    face_y0[...] = gas[:, :, 0, :]
    face_y1[...] = gas[:, :, extent_y - 1, :]


def local_kernel(gas_hbm, table, diffused_hbm, gas, diffused, sems):
    fields, extent_x, extent_y, extent_z = gas.shape
    across_y = extent_y // TILE_Y
    across_z = extent_z // TILE_Z
    lane = lax.broadcasted_iota(jnp.int32, (extent_y, extent_z), 1)
    line = lax.broadcasted_iota(jnp.int32, (extent_y, extent_z), 0)
    copy = pltpu.make_async_copy(gas_hbm, gas, sems.at[fields])
    copy.start()
    copy.wait()

    def sent(f):
        return pltpu.make_async_copy(diffused.at[f], diffused_hbm.at[f], sems.at[f])

    def per_field(f, carry):
        for x in range(extent_x):
            centre = gas[f, x]
            beside = jnp.where(line == 0, 0.0, roll(centre, 1, 0))
            beside += jnp.where(line == extent_y - 1, 0.0, roll(centre, -1, 0))
            beside += jnp.where(lane == 0, 0.0, roll(centre, 1, 1))
            beside += jnp.where(lane == extent_z - 1, 0.0, roll(centre, -1, 1))
            if x > 0:
                beside += gas[f, x - 1]
            if x < extent_x - 1:
                beside += gas[f, x + 1]
            diffused[f, x * extent_y : (x + 1) * extent_y, :] = centre + DIFFUSION * (beside - 6.0 * centre)
        sent(f).start()
        return carry

    lax.fori_loop(0, fields, per_field, 0)

    def per_a(a, carry):
        for f in range(FLOWS):
            for b in range(across_y):
                for h in range(extent_z // LANES):
                    lanes = slice(h * LANES, (h + 1) * LANES)
                    rows = slice(b * TILE_Y, (b + 1) * TILE_Y)
                    parts = []
                    for u in range(TILE_X):
                        piece = gas[f, a * TILE_X + u, rows, lanes]
                        if f == 3:
                            piece = piece - gas[4, a * TILE_X + u, rows, lanes]
                        parts.append(piece)
                    pair = exchange(jnp.concatenate(parts[:2], 0), jnp.concatenate(parts[2:], 0))
                    start = pl.multiple_of((a * across_y + b) * across_z + h * GRANULES, SUB)
                    table[f, pl.ds(start, SUB), :] = pair[0]
                    table[f, pl.ds(start + SUB, SUB), :] = pair[1]
        return carry

    lax.fori_loop(0, extent_x // TILE_X, per_a, 0)
    for f in range(fields):
        sent(f).wait()


def paired(ref, member, stride, offset, capacity):
    starts = [(member + n) * stride + offset for n in range(2)]
    return jnp.concatenate([ref[start : start + capacity, :] for start in starts], axis=0)


def columns(g, across_i, spread):
    size = SUB // across_i * spread
    return pl.ds(pl.multiple_of(g * size, SUB), size)


def update_kernel(
    message, table, result_hbm, result, ids_vmem, products, turned, sems, *, rows, capacity
):
    devices = message.shape[0] // rows
    group = SUB * rows
    for g in range(devices // SUB):
        ids_vmem[g * SUB : (g + 1) * SUB, :] = message[pl.ds(g * group + rows - 1, SUB, stride=rows), :].astype(jnp.int32)
    for k in range(capacity):
        turned[k] = roll(ids_vmem[...], -k, 1)
    corner = lax.broadcasted_iota(jnp.int32, (SUB, LANES), 0)
    high = [(corner & bit) != 0 for bit in (4, 2, 1)]
    least = [jnp.where(h, 0.0, 1.0) for h in high]
    slope = [jnp.where(h, 1.0, -1.0) for h in high]
    shift = (
        jnp.where(high[0], TILE_Y * TILE_Z, 0) + jnp.where(high[1], TILE_Z, 0) + jnp.where(high[2], 1, 0)
    )
    row = corner

    across_i = result.shape[0]
    spread = capacity * FLOWS

    def returned(g):
        place = columns(g, across_i, spread)
        return pltpu.make_async_copy(result.at[:, place], result_hbm.at[:, place], sems.at[g])

    def per_group(g, carry):
        out = result.at[:, columns(g, across_i, spread)]
        here = pl.ds(pl.multiple_of(g * SUB, SUB), SUB)
        numbers = [turned[k, here, :] for k in range(capacity)]
        part = message.at[pl.ds(pl.multiple_of(g * group, SUB), group)]
        for step in range(SUB // 2):

            def both(field):
                return paired(part, 2 * step, rows, field * capacity, capacity)

            first = ((both(6) * TILE_Y + both(7)) * TILE_Z + both(8)).astype(jnp.int32)
            alive = jnp.zeros((SUB, LANES), jnp.int32)
            for j in range(2 * capacity):
                i, k = 2 * step + j // capacity, j % capacity
                base = i * rows
                tile = numbers[k][i, 0]
                alive = jnp.where(row == j, tile, alive)
                safe = jnp.maximum(tile, 0)
                weight = None
                for dim in range(3):
                    start = base + (3 + dim) * capacity + k
                    fraction = part[start : start + 1, :]
                    along = least[dim] + slope[dim] * fraction
                    weight = along if weight is None else weight * along
                index = jnp.broadcast_to(first[j : j + 1], (SUB, LANES)) + shift
                for f in range(FLOWS):
                    held = jnp.broadcast_to(table[f, pl.ds(safe, 1), :], (SUB, LANES))
                    found = jnp.take_along_axis(held, index, axis=1, mode="promise_in_bounds")
                    products[(f * SUB + j) * SUB : (f * SUB + j + 1) * SUB, :] = found * weight
            live = alive >= 0
            sampled = []
            for f in range(FLOWS):
                total = products[pl.ds(f * SUB * SUB, SUB, stride=SUB), :]
                for c in range(1, SUB):
                    total = total + products[pl.ds(f * SUB * SUB + c, SUB, stride=SUB), :]
                sampled.append(total)

            mass_old = both(9)
            radius = jnp.exp(jnp.log(mass_old) * (1.0 / 3.0))
            factor = DRAG_RATE / (radius * radius)
            share = 1.0 / (1.0 + factor)
            gap = sampled[3]
            soft = jnp.maximum(gap, 0.0) + jnp.log(1.0 + jnp.exp(-jnp.abs(gap)))
            mass_new = jnp.where(live, mass_old / (1.0 + EVAPORATION * soft / radius), mass_old)
            fields = [
                jnp.where(live, (both(f) + factor * sampled[f]) * share, both(f)) for f in range(3)
            ] + [mass_new]
            for n in range(2):
                i, start = (2 * step + n) % across_i, (2 * step + n) // across_i * spread
                for f in range(FLOWS):
                    rows_f = slice(start + f * capacity, start + (f + 1) * capacity)
                    out[i, rows_f, :] = fields[f][n * capacity : (n + 1) * capacity]
        returned(g).start()
        return carry

    lax.fori_loop(0, devices // SUB, per_group, 0)
    for g in range(devices // SUB):
        returned(g).wait()


def tent(position, cell):
    return jnp.maximum(0.0, 1.0 - jnp.abs(position - cell))


def deposit_kernel(
    ids_vmem, message, result, diffused, from_x0, from_x1, from_y0, from_y1, gas_next,
    total, source, ids, work, sems, *, rows, capacity
):
    fields, extent_x, extent_z = from_y0.shape
    extent_y = from_x0.shape[1]
    across_y = extent_y // TILE_Y
    across_z = extent_z // TILE_Z
    blocks = source.shape[0] // SUB
    group = SUB * rows
    spread = capacity * FLOWS
    across_i = result.shape[0]
    copy = pltpu.make_async_copy(ids_vmem, ids, sems.at[0])
    copy.start()
    fetch = pltpu.make_async_copy(diffused, work, sems.at[1])
    fetch.start()
    total[...] = jnp.zeros(total.shape, total.dtype)

    def per_group(g, carry):
        part = message.at[pl.ds(pl.multiple_of(g * group, SUB), group)]
        updated = result.at[:, columns(g, across_i, spread)]
        out = source.at[pl.ds(pl.multiple_of(g * SUB * SUB * capacity, SUB), SUB * SUB * capacity)]
        for step in range(SUB // 2):

            def before(field):
                return paired(part, 2 * step, rows, field * capacity, capacity)

            def after(field):
                found = []
                for member in (2 * step, 2 * step + 1):
                    i, start = member % across_i, member // across_i * spread + field * capacity
                    found.append(updated[i, start : start + capacity, :])
                return jnp.concatenate(found, axis=0)

            mass_old = before(9)
            vapour = mass_old - after(3)
            found = [mass_old * (before(f) - after(f)) + vapour * after(f) for f in range(3)] + [vapour]
            found += [before(3 + dim) + before(6 + dim) for dim in range(3)]
            for f, value in enumerate(found):
                out[pl.ds(2 * step * capacity * SUB + f, 2 * capacity, stride=SUB), :] = value
        return carry

    lax.fori_loop(0, blocks // (SUB * capacity), per_group, 0)
    row = lax.broadcasted_iota(jnp.int32, (SUB, LANES), 0)
    along_z = row.astype(jnp.float32)
    along_y = (row % TILE_Y).astype(jnp.float32)
    along_x = (row // TILE_Y).astype(jnp.float32)
    copy.wait()

    def one(n):
        tile = jnp.maximum(ids[n // capacity, n % capacity], 0)
        held = source[pl.ds(pl.multiple_of(n * SUB, SUB), SUB), :]
        given = held[0:FLOWS]
        coarse = given.astype(jnp.bfloat16).astype(jnp.float32)
        left = jnp.concatenate([given, given - coarse], axis=0).astype(jnp.bfloat16)
        x, y, z = held[4:5], held[5:6], held[6:7]
        weight_z = tent(z, along_z)
        weight_y = tent(y, along_y)
        planes = []
        for part in range(2):
            weight_xy = tent(x, along_x + 2.0 * part) * weight_y
            for i in range(SUB):
                planes.append(weight_xy[i : i + 1] * weight_z)
        stencil = jnp.concatenate(planes, axis=0)
        high = stencil.astype(jnp.bfloat16)
        low = (stencil - high.astype(jnp.float32)).astype(jnp.bfloat16)
        right = jnp.concatenate([high, low], axis=0)
        sums = lax.dot_general(left, right, (((1,), (1,)), ((), ())), preferred_element_type=jnp.float32)
        return pl.multiple_of(tile * SUB, SUB), sums[:, :LANES] + sums[:, LANES:]

    unroll = 16

    def per_step(step, carry):
        made = [one(step * unroll + n) for n in range(unroll)]
        for start, sums in made:
            total[pl.ds(start, SUB), :] += sums
        return carry

    lax.fori_loop(0, blocks // unroll, per_step, 0)

    fetch.wait()
    last_x = (extent_x - 1) * extent_y
    for f in range(fields):
        work[f, 0:extent_y, :] += DIFFUSION * from_x0[f]
        work[f, last_x : last_x + extent_y, :] += DIFFUSION * from_x1[f]
        for h in range(extent_z // LANES):
            lanes = slice(h * LANES, (h + 1) * LANES)
            for line, face in ((0, from_y0), (extent_y - 1, from_y1)):
                for x in range(extent_x):
                    spot = x * extent_y + line
                    work[f, spot : spot + 1, lanes] += DIFFUSION * face[f, x : x + 1, lanes]

    def sent(a):
        place = pl.ds(pl.multiple_of(a * TILE_X * extent_y, SUB), TILE_X * extent_y)
        return pltpu.make_async_copy(work.at[:, place], gas_next.at[:, place], sems.at[2 + a])

    def per_a(a, carry):
        held = work.at[:, pl.ds(pl.multiple_of(a * TILE_X * extent_y, SUB), TILE_X * extent_y)]
        for b in range(across_y):
            for h in range(extent_z // LANES):
                start = ((a * across_y + b) * across_z + h * GRANULES) * SUB
                part = total.at[pl.ds(pl.multiple_of(start, SUB), GRANULES * SUB)]
                lanes = slice(h * LANES, (h + 1) * LANES)
                for f in range(FLOWS):
                    pair = [
                        part[pl.ds(n * SUB * SUB + f, SUB, stride=SUB), :]
                        + part[pl.ds(n * SUB * SUB + f + FLOWS, SUB, stride=SUB), :]
                        for n in range(2)
                    ]
                    pair = [x * (1.0 / CELL_MASS) for x in exchange(*pair)]
                    for u in range(TILE_X):
                        piece = pair[u // 2][(u % 2) * TILE_Y : (u % 2 + 1) * TILE_Y]
                        spot = u * extent_y + b * TILE_Y
                        lines = slice(spot, spot + TILE_Y)
                        if f < 3:
                            held[f, lines, lanes] += piece
                        else:
                            held[3, lines, lanes] -= LATENT_HEAT * piece
                            held[4, lines, lanes] += piece
        sent(a).start()
        return carry

    lax.fori_loop(0, extent_x // TILE_X, per_a, 0)
    for a in range(extent_x // TILE_X):
        sent(a).wait()


def unpack_kernel(result, speed, mass, sems):
    vector = speed.shape[1]
    copies = [
        pltpu.make_async_copy(result.at[:, :vector], speed, sems.at[0]),
        pltpu.make_async_copy(result.at[:, vector:], mass, sems.at[1]),
    ]
    for copy in copies:
        copy.start()
    for copy in copies:
        copy.wait()


def specs(spaces):
    return [pl.BlockSpec(memory_space=space) for space in spaces]


def call(kernel, out_shape, scratch=(), flops=0, moved=0, ins=None, outs=None):
    extra = {}
    if ins is not None:
        extra["in_specs"] = specs(ins)
    if outs is not None:
        extra["out_specs"] = specs(outs) if len(outs) > 1 else specs(outs)[0]
        if pltpu.HBM in outs:
            shapes = out_shape if len(outs) > 1 else (out_shape,)
            shapes = [pltpu.HBM(o.shape, o.dtype) if space == pltpu.HBM else o for o, space in zip(shapes, outs)]
            out_shape = shapes if len(outs) > 1 else shapes[0]
    called = pl.pallas_call(
        kernel,
        out_shape=out_shape,
        scratch_shapes=scratch,
        cost_estimate=pl.CostEstimate(flops=flops, bytes_accessed=moved, transcendentals=0),
        compiler_params=pltpu.CompilerParams(vmem_limit_bytes=32 * 1024 * 1024),
        **extra,
    )

    def with_spaces(*values):
        if ins is not None:
            values = [
                pltpu.with_memory_space_constraint(v, space) if space == pltpu.HBM else v
                for v, space in zip(values, ins)
            ]
        return called(*values)

    return with_spaces


def step(gas_state, parcel_speed, parcel_mass, offsets, cell_base, block_tile, block_count):
    fields, extent_x, extent_y, extent_z = gas_state.shape
    devices, capacity = block_tile.shape[2:]
    rows = 10 * capacity + 1
    tiles = (extent_x // TILE_X) * (extent_y // TILE_Y) * (extent_z // TILE_Z)
    f32 = jnp.float32

    def shape(*dims, dtype=f32):
        return jax.ShapeDtypeStruct(dims, dtype)

    vector = 3 * capacity
    blocks = devices * capacity
    across_i, across_j = lax.axis_size("gx"), lax.axis_size("yz")
    parts = max(1, across_j // 2)
    i32 = jnp.int32
    hbm, vmem = pltpu.HBM, pltpu.VMEM
    dma = pltpu.SemaphoreType.DMA

    def by_component(value):
        return value[0, 0].transpose(0, 2, 1, 3).reshape(across_i, across_j * vector, LANES)

    message = call(
        functools.partial(pack_kernel, rows=rows, capacity=capacity, parts=parts),
        shape(devices * rows, LANES),
        scratch=[
            vmem((across_i, across_j * vector, LANES), f32),
            vmem((across_i, across_j * capacity, LANES), f32),
            vmem((across_i, across_j * vector, LANES), f32),
            vmem((across_i, across_j * vector, LANES), i32),
            vmem((capacity, devices), i32),
            vmem((1, devices), i32),
            vmem((devices, LANES), f32),
            vmem((devices * rows, LANES), f32),
            dma((2 + 5 * parts,)),
        ],
        ins=[hbm] * 6,
        outs=[hbm],
    )(
        by_component(parcel_speed),
        parcel_mass.reshape(across_i, across_j * capacity, LANES),
        by_component(offsets),
        by_component(cell_base),
        block_tile[0, 0].T,
        block_count[0],
    )
    message = lax.all_to_all(message.reshape(devices, rows, 1, LANES), SENT, split_axis=0, concat_axis=0, tiled=True)
    message = message.reshape(devices * rows, LANES)

    face = shape(fields, extent_x, extent_z)
    side = shape(fields, extent_y, extent_z)
    whole = vmem(gas_state.shape, f32)
    flat = (fields, extent_x * extent_y, extent_z)
    face_x0, face_x1, face_y0, face_y1 = call(
        faces_kernel, (side, side, face, face), scratch=[whole, dma(())], ins=[hbm], outs=[vmem] * 4
    )(gas_state)

    def shifted(value, axis, step):
        count = lax.axis_size(axis)
        pairs = [(i, i + step) for i in range(count) if 0 <= i + step < count]
        return lax.ppermute(value, axis, pairs)

    halo = (
        shifted(face_x1, "gx", 1), shifted(face_x0, "gx", -1), shifted(face_y1, "yz", 1), shifted(face_y0, "yz", -1)
    )
    table, diffused = call(
        local_kernel,
        (shape(FLOWS, tiles, LANES), shape(*flat)),
        scratch=[whole, vmem(flat, f32), dma((fields + 1,))],
        flops=10**7,
        ins=[hbm],
        outs=[vmem, hbm],
    )(gas_state)
    message, table, diffused = lax.optimization_barrier((message, table, diffused))

    returned, result, ids = call(
        functools.partial(update_kernel, rows=rows, capacity=capacity),
        (
            shape(across_i, across_j * capacity * FLOWS, LANES),
            shape(across_i, across_j * capacity * FLOWS, LANES),
            shape(devices, LANES, dtype=i32),
        ),
        scratch=[
            vmem((FLOWS * SUB * SUB, LANES), f32),
            vmem((capacity, devices, LANES), i32),
            dma((devices // SUB,)),
        ],
        flops=10**7,
        ins=[vmem, vmem],
        outs=[hbm, vmem, vmem],
    )(message, table)
    returned = lax.all_to_all(
        returned.reshape(devices, capacity * FLOWS, 1, LANES), RETURNED, split_axis=0, concat_axis=0, tiled=True
    )
    gas_next = call(
        functools.partial(deposit_kernel, rows=rows, capacity=capacity),
        shape(*flat),
        scratch=[
            vmem((tiles * SUB, LANES), f32),
            vmem((blocks * SUB, LANES), f32),
            pltpu.SMEM((devices, LANES), i32),
            vmem(flat, f32),
            dma((2 + extent_x // TILE_X,)),
        ],
        flops=3 * 10**7,
        ins=[vmem, vmem, vmem, hbm] + [vmem] * 4,
        outs=[hbm],
    )(ids, message, result, diffused, *halo)
    speed_next, mass_next = call(
        unpack_kernel,
        (shape(devices, vector, 1, LANES), shape(devices, capacity, 1, LANES)),
        scratch=[dma((2,))],
        ins=[vmem],
        outs=[hbm, hbm],
    )(returned)
    speed_next = speed_next.reshape(devices, 3, capacity, LANES).transpose(0, 2, 1, 3)
    return gas_next.reshape(gas_state.shape), speed_next.reshape(parcel_speed.shape), mass_next.reshape(parcel_mass.shape)


def solution(mesh):
    in_specs = (
        P(None, "gx", "yz", None),
        P("gx", "yz", None, None, None, None),
        P("gx", "yz", None, None, None),
        P("gx", "yz", None, None, None, None),
        P("gx", "yz", None, None, None, None),
        P("gx", "yz", None, None),
        P("gx", "yz", None),
    )
    out_specs = (
        P(None, "gx", "yz", None),
        P("gx", "yz", None, None, None, None),
        P("gx", "yz", None, None, None),
    )
    return jax.shard_map(step, mesh=mesh, in_specs=in_specs, out_specs=out_specs, check_vma=False)
```

```python
import functools

import jax
import jax.numpy as jnp
from jax import lax
from jax.experimental import pallas as pl
from jax.experimental.pallas import tpu as pltpu
from jax.sharding import PartitionSpec as P


TILE_X = 4
TILE_Y = 4
TILE_Z = 8
DIFFUSION = 0.1
CELL_MASS = 4.0
DRAG_RATE = 0.5
EVAPORATION = 0.3
LATENT_HEAT = 2.0

LANES = 128
SUB = 8
GRANULES = LANES // TILE_Z
FLOWS = 4
SENT = ("yz", "gx")
RETURNED = ("gx", "yz")


def roll(x, shift, axis):
    shift = shift % x.shape[axis]
    return pltpu.roll(x, shift, axis) if shift else x


def pick(x, rows):
    return jnp.take_along_axis(x, rows, axis=0, mode="promise_in_bounds")


def exchange(upper, lower):
    row = lax.broadcasted_iota(jnp.int32, (SUB, LANES), 0)
    granule = lax.broadcasted_iota(jnp.int32, (SUB, LANES), 1) // TILE_Z
    half = LANES // 2
    turned = [
        pltpu.roll(x, shift, 1, stride=TILE_Z, stride_axis=0) for x, shift in ((upper, 0), (lower, half))
    ]
    back = SUB - 1 - row
    pair = []
    for part in range(2):
        wanted = (granule - back - SUB * part) % GRANULES
        mixed = jnp.where(wanted < SUB, pick(turned[0], wanted % SUB), pick(turned[1], wanted % SUB))
        shift = (-TILE_Z * (SUB - 1) - half * part) % LANES
        pair.append(pick(pltpu.roll(mixed, shift, 1, stride=TILE_Z, stride_axis=0), back))
    return pair


def pack_kernel(
    speed, mass, offsets, cells, tile_ids, counts, message,
    speed_v, mass_v, offsets_v, cells_v, tile_ids_v, counts_v, ids_v, message_v, sems, *, rows, capacity, parts
):
    across_i = speed.shape[0]
    vector = 3 * capacity
    across_j = speed.shape[1] // vector
    each = across_j // parts
    sources = ((speed, speed_v, vector), (offsets, offsets_v, vector), (cells, cells_v, vector), (mass, mass_v, capacity))
    small = [
        pltpu.make_async_copy(tile_ids, tile_ids_v, sems.at[0]),
        pltpu.make_async_copy(counts, counts_v, sems.at[1]),
    ]
    taken = []
    for copy in small:
        copy.start()
    for part in range(parts):
        taken.append([])
        for n, (source, held, count) in enumerate(sources):
            place = pl.ds(part * each * count, each * count)
            copy = pltpu.make_async_copy(source.at[:, place], held.at[:, place], sems.at[2 + part * 5 + n])
            copy.start()
            taken[-1].append(copy)
    for copy in small:
        copy.wait()
    slot = lax.broadcasted_iota(jnp.int32, tile_ids_v.shape, 0)
    ids = jnp.where(slot < counts_v[...], tile_ids_v[...], -1).astype(jnp.float32)
    ids_v[...] = jnp.concatenate([ids, jnp.zeros((LANES - capacity, ids.shape[1]), jnp.float32)], axis=0).T

    sent = []
    for part in range(parts):
        for copy in taken[part]:
            copy.wait()
        for j in range(part * each, (part + 1) * each):
            for i in range(across_i):
                base = (j * across_i + i) * rows
                place = slice(j * vector, (j + 1) * vector)
                message_v[base : base + vector, :] = speed_v[i, place, :]
                message_v[base + vector : base + 2 * vector, :] = offsets_v[i, place, :]
                message_v[base + 2 * vector : base + 3 * vector, :] = cells_v[i, place, :].astype(jnp.float32)
                base += 3 * vector
                message_v[base : base + capacity, :] = mass_v[i, j * capacity : (j + 1) * capacity, :]
                owner = i * across_j + j
                message_v[base + capacity : base + capacity + 1, :] = ids_v[owner : owner + 1, :]
        place = pl.ds(part * each * across_i * rows, each * across_i * rows)
        copy = pltpu.make_async_copy(message_v.at[place], message.at[place], sems.at[2 + part * 5 + 4])
        copy.start()
        sent.append(copy)
    for copy in sent:
        copy.wait()


def table_kernel(gas, table, face_x0, face_x1, face_y0, face_y1):
    extent_x, extent_y, extent_z = gas.shape[1:]
    across_y = extent_y // TILE_Y
    across_z = extent_z // TILE_Z
    face_x0[...] = gas[:, 0]
    face_x1[...] = gas[:, extent_x - 1]
    face_y0[...] = gas[:, :, 0, :]
    face_y1[...] = gas[:, :, extent_y - 1, :]

    def per_a(a, carry):
        for f in range(FLOWS):
            for b in range(across_y):
                for h in range(extent_z // LANES):
                    lanes = slice(h * LANES, (h + 1) * LANES)
                    rows = slice(b * TILE_Y, (b + 1) * TILE_Y)
                    parts = []
                    for u in range(TILE_X):
                        piece = gas[f, a * TILE_X + u, rows, lanes]
                        if f == 3:
                            piece = piece - gas[4, a * TILE_X + u, rows, lanes]
                        parts.append(piece)
                    pair = exchange(jnp.concatenate(parts[:2], 0), jnp.concatenate(parts[2:], 0))
                    start = pl.multiple_of((a * across_y + b) * across_z + h * GRANULES, SUB)
                    table[f, pl.ds(start, SUB), :] = pair[0]
                    table[f, pl.ds(start + SUB, SUB), :] = pair[1]
        return carry

    lax.fori_loop(0, extent_x // TILE_X, per_a, 0)


def paired(ref, member, stride, offset, capacity):
    starts = [(member + n) * stride + offset for n in range(2)]
    return jnp.concatenate([ref[start : start + capacity, :] for start in starts], axis=0)


def columns(g, across_i, spread):
    size = SUB // across_i * spread
    return pl.ds(pl.multiple_of(g * size, SUB), size)


def update_kernel(
    message, table, result_hbm, result, ids_vmem, products, turned, sems, *, rows, capacity
):
    devices = message.shape[0] // rows
    group = SUB * rows
    for g in range(devices // SUB):
        ids_vmem[g * SUB : (g + 1) * SUB, :] = message[pl.ds(g * group + rows - 1, SUB, stride=rows), :].astype(jnp.int32)
    for k in range(capacity):
        turned[k] = roll(ids_vmem[...], -k, 1)
    corner = lax.broadcasted_iota(jnp.int32, (SUB, LANES), 0)
    high = [(corner & bit) != 0 for bit in (4, 2, 1)]
    least = [jnp.where(h, 0.0, 1.0) for h in high]
    slope = [jnp.where(h, 1.0, -1.0) for h in high]
    shift = (
        jnp.where(high[0], TILE_Y * TILE_Z, 0) + jnp.where(high[1], TILE_Z, 0) + jnp.where(high[2], 1, 0)
    )
    row = corner

    across_i = result.shape[0]
    spread = capacity * FLOWS

    def returned(g):
        place = columns(g, across_i, spread)
        return pltpu.make_async_copy(result.at[:, place], result_hbm.at[:, place], sems.at[g])

    def per_group(g, carry):
        out = result.at[:, columns(g, across_i, spread)]
        here = pl.ds(pl.multiple_of(g * SUB, SUB), SUB)
        numbers = [turned[k, here, :] for k in range(capacity)]
        part = message.at[pl.ds(pl.multiple_of(g * group, SUB), group)]
        for step in range(SUB // 2):

            def both(field):
                return paired(part, 2 * step, rows, field * capacity, capacity)

            first = ((both(6) * TILE_Y + both(7)) * TILE_Z + both(8)).astype(jnp.int32)
            alive = jnp.zeros((SUB, LANES), jnp.int32)
            for j in range(2 * capacity):
                i, k = 2 * step + j // capacity, j % capacity
                base = i * rows
                tile = numbers[k][i, 0]
                alive = jnp.where(row == j, tile, alive)
                safe = jnp.maximum(tile, 0)
                weight = None
                for dim in range(3):
                    start = base + (3 + dim) * capacity + k
                    fraction = part[start : start + 1, :]
                    along = least[dim] + slope[dim] * fraction
                    weight = along if weight is None else weight * along
                index = jnp.broadcast_to(first[j : j + 1], (SUB, LANES)) + shift
                for f in range(FLOWS):
                    held = jnp.broadcast_to(table[f, pl.ds(safe, 1), :], (SUB, LANES))
                    found = jnp.take_along_axis(held, index, axis=1, mode="promise_in_bounds")
                    products[(f * SUB + j) * SUB : (f * SUB + j + 1) * SUB, :] = found * weight
            live = alive >= 0
            sampled = []
            for f in range(FLOWS):
                total = products[pl.ds(f * SUB * SUB, SUB, stride=SUB), :]
                for c in range(1, SUB):
                    total = total + products[pl.ds(f * SUB * SUB + c, SUB, stride=SUB), :]
                sampled.append(total)

            mass_old = both(9)
            radius = jnp.exp(jnp.log(mass_old) * (1.0 / 3.0))
            factor = DRAG_RATE / (radius * radius)
            share = 1.0 / (1.0 + factor)
            gap = sampled[3]
            soft = jnp.maximum(gap, 0.0) + jnp.log(1.0 + jnp.exp(-jnp.abs(gap)))
            mass_new = jnp.where(live, mass_old / (1.0 + EVAPORATION * soft / radius), mass_old)
            fields = [
                jnp.where(live, (both(f) + factor * sampled[f]) * share, both(f)) for f in range(3)
            ] + [mass_new]
            for n in range(2):
                i, start = (2 * step + n) % across_i, (2 * step + n) // across_i * spread
                for f in range(FLOWS):
                    rows_f = slice(start + f * capacity, start + (f + 1) * capacity)
                    out[i, rows_f, :] = fields[f][n * capacity : (n + 1) * capacity]
        returned(g).start()
        return carry

    lax.fori_loop(0, devices // SUB, per_group, 0)
    for g in range(devices // SUB):
        returned(g).wait()


def tent(position, cell):
    return jnp.maximum(0.0, 1.0 - jnp.abs(position - cell))


def deposit_kernel(
    ids_vmem, message, result, gas_hbm, from_x0, from_x1, from_y0, from_y1, gas_next,
    total, source, ids, gas, work, sems, *, rows, capacity
):
    fields, extent_x, extent_z = from_y0.shape
    extent_y = from_x0.shape[1]
    across_y = extent_y // TILE_Y
    across_z = extent_z // TILE_Z
    blocks = source.shape[0] // SUB
    group = SUB * rows
    spread = capacity * FLOWS
    across_i = result.shape[0]
    copy = pltpu.make_async_copy(ids_vmem, ids, sems.at[0])
    copy.start()
    fetch = pltpu.make_async_copy(gas_hbm, gas, sems.at[1])
    fetch.start()
    total[...] = jnp.zeros(total.shape, total.dtype)

    def per_group(g, carry):
        part = message.at[pl.ds(pl.multiple_of(g * group, SUB), group)]
        updated = result.at[:, columns(g, across_i, spread)]
        out = source.at[pl.ds(pl.multiple_of(g * SUB * SUB * capacity, SUB), SUB * SUB * capacity)]
        for step in range(SUB // 2):

            def before(field):
                return paired(part, 2 * step, rows, field * capacity, capacity)

            def after(field):
                found = []
                for member in (2 * step, 2 * step + 1):
                    i, start = member % across_i, member // across_i * spread + field * capacity
                    found.append(updated[i, start : start + capacity, :])
                return jnp.concatenate(found, axis=0)

            mass_old = before(9)
            vapour = mass_old - after(3)
            found = [mass_old * (before(f) - after(f)) + vapour * after(f) for f in range(3)] + [vapour]
            found += [before(3 + dim) + before(6 + dim) for dim in range(3)]
            for f, value in enumerate(found):
                out[pl.ds(2 * step * capacity * SUB + f, 2 * capacity, stride=SUB), :] = value
        return carry

    lax.fori_loop(0, blocks // (SUB * capacity), per_group, 0)
    row = lax.broadcasted_iota(jnp.int32, (SUB, LANES), 0)
    along_z = row.astype(jnp.float32)
    along_y = (row % TILE_Y).astype(jnp.float32)
    along_x = (row // TILE_Y).astype(jnp.float32)
    copy.wait()

    def one(n):
        tile = jnp.maximum(ids[n // capacity, n % capacity], 0)
        held = source[pl.ds(pl.multiple_of(n * SUB, SUB), SUB), :]
        given = held[0:FLOWS]
        coarse = given.astype(jnp.bfloat16).astype(jnp.float32)
        left = jnp.concatenate([given, given - coarse], axis=0).astype(jnp.bfloat16)
        x, y, z = held[4:5], held[5:6], held[6:7]
        weight_z = tent(z, along_z)
        weight_y = tent(y, along_y)
        planes = []
        for part in range(2):
            weight_xy = tent(x, along_x + 2.0 * part) * weight_y
            for i in range(SUB):
                planes.append(weight_xy[i : i + 1] * weight_z)
        stencil = jnp.concatenate(planes, axis=0)
        high = stencil.astype(jnp.bfloat16)
        low = (stencil - high.astype(jnp.float32)).astype(jnp.bfloat16)
        right = jnp.concatenate([high, low], axis=0)
        sums = lax.dot_general(left, right, (((1,), (1,)), ((), ())), preferred_element_type=jnp.float32)
        return pl.multiple_of(tile * SUB, SUB), sums[:, :LANES] + sums[:, LANES:]

    unroll = 16

    def per_step(step, carry):
        made = [one(step * unroll + n) for n in range(unroll)]
        for start, sums in made:
            total[pl.ds(start, SUB), :] += sums
        return carry

    lax.fori_loop(0, blocks // unroll, per_step, 0)

    fetch.wait()
    lane = lax.broadcasted_iota(jnp.int32, (extent_y, extent_z), 1)
    line = lax.broadcasted_iota(jnp.int32, (extent_y, extent_z), 0)

    def per_field(f, carry):
        for x in range(extent_x):
            centre = gas[f, x]
            beside = from_x0[f] if x == 0 else gas[f, x - 1]
            beside += from_x1[f] if x == extent_x - 1 else gas[f, x + 1]
            beside += jnp.where(line == 0, from_y0[f, x : x + 1, :], roll(centre, 1, 0))
            beside += jnp.where(line == extent_y - 1, from_y1[f, x : x + 1, :], roll(centre, -1, 0))
            beside += jnp.where(lane == 0, 0.0, roll(centre, 1, 1))
            beside += jnp.where(lane == extent_z - 1, 0.0, roll(centre, -1, 1))
            work[f, x * extent_y : (x + 1) * extent_y, :] = centre + DIFFUSION * (beside - 6.0 * centre)
        return carry

    lax.fori_loop(0, fields, per_field, 0)

    def sent(a):
        place = pl.ds(pl.multiple_of(a * TILE_X * extent_y, SUB), TILE_X * extent_y)
        return pltpu.make_async_copy(work.at[:, place], gas_next.at[:, place], sems.at[2 + a])

    def per_a(a, carry):
        held = work.at[:, pl.ds(pl.multiple_of(a * TILE_X * extent_y, SUB), TILE_X * extent_y)]
        for b in range(across_y):
            for h in range(extent_z // LANES):
                start = ((a * across_y + b) * across_z + h * GRANULES) * SUB
                part = total.at[pl.ds(pl.multiple_of(start, SUB), GRANULES * SUB)]
                lanes = slice(h * LANES, (h + 1) * LANES)
                for f in range(FLOWS):
                    pair = [
                        part[pl.ds(n * SUB * SUB + f, SUB, stride=SUB), :]
                        + part[pl.ds(n * SUB * SUB + f + FLOWS, SUB, stride=SUB), :]
                        for n in range(2)
                    ]
                    pair = [x * (1.0 / CELL_MASS) for x in exchange(*pair)]
                    for u in range(TILE_X):
                        piece = pair[u // 2][(u % 2) * TILE_Y : (u % 2 + 1) * TILE_Y]
                        spot = u * extent_y + b * TILE_Y
                        lines = slice(spot, spot + TILE_Y)
                        if f < 3:
                            held[f, lines, lanes] += piece
                        else:
                            held[3, lines, lanes] -= LATENT_HEAT * piece
                            held[4, lines, lanes] += piece
        sent(a).start()
        return carry

    lax.fori_loop(0, extent_x // TILE_X, per_a, 0)
    for a in range(extent_x // TILE_X):
        sent(a).wait()


def unpack_kernel(result, speed, mass, sems):
    vector = speed.shape[1]
    copies = [
        pltpu.make_async_copy(result.at[:, :vector], speed, sems.at[0]),
        pltpu.make_async_copy(result.at[:, vector:], mass, sems.at[1]),
    ]
    for copy in copies:
        copy.start()
    for copy in copies:
        copy.wait()


def specs(spaces):
    return [pl.BlockSpec(memory_space=space) for space in spaces]


def call(kernel, out_shape, scratch=(), flops=0, moved=0, ins=None, outs=None):
    extra = {}
    if ins is not None:
        extra["in_specs"] = specs(ins)
    if outs is not None:
        extra["out_specs"] = specs(outs) if len(outs) > 1 else specs(outs)[0]
        if pltpu.HBM in outs:
            shapes = out_shape if len(outs) > 1 else (out_shape,)
            shapes = [pltpu.HBM(o.shape, o.dtype) if space == pltpu.HBM else o for o, space in zip(shapes, outs)]
            out_shape = shapes if len(outs) > 1 else shapes[0]
    called = pl.pallas_call(
        kernel,
        out_shape=out_shape,
        scratch_shapes=scratch,
        cost_estimate=pl.CostEstimate(flops=flops, bytes_accessed=moved, transcendentals=0),
        compiler_params=pltpu.CompilerParams(vmem_limit_bytes=32 * 1024 * 1024),
        **extra,
    )

    def with_spaces(*values):
        if ins is not None:
            values = [
                pltpu.with_memory_space_constraint(v, space) if space == pltpu.HBM else v
                for v, space in zip(values, ins)
            ]
        return called(*values)

    return with_spaces


def step(gas_state, parcel_speed, parcel_mass, offsets, cell_base, block_tile, block_count):
    fields, extent_x, extent_y, extent_z = gas_state.shape
    devices, capacity = block_tile.shape[2:]
    rows = 10 * capacity + 1
    tiles = (extent_x // TILE_X) * (extent_y // TILE_Y) * (extent_z // TILE_Z)
    f32 = jnp.float32

    def shape(*dims, dtype=f32):
        return jax.ShapeDtypeStruct(dims, dtype)

    vector = 3 * capacity
    blocks = devices * capacity
    across_i, across_j = lax.axis_size("gx"), lax.axis_size("yz")
    parts = max(1, across_j // 2)
    i32 = jnp.int32
    hbm, vmem = pltpu.HBM, pltpu.VMEM
    dma = pltpu.SemaphoreType.DMA

    def by_component(value):
        return value[0, 0].transpose(0, 2, 1, 3).reshape(across_i, across_j * vector, LANES)

    message = call(
        functools.partial(pack_kernel, rows=rows, capacity=capacity, parts=parts),
        shape(devices * rows, LANES),
        scratch=[
            vmem((across_i, across_j * vector, LANES), f32),
            vmem((across_i, across_j * capacity, LANES), f32),
            vmem((across_i, across_j * vector, LANES), f32),
            vmem((across_i, across_j * vector, LANES), i32),
            vmem((capacity, devices), i32),
            vmem((1, devices), i32),
            vmem((devices, LANES), f32),
            vmem((devices * rows, LANES), f32),
            dma((2 + 5 * parts,)),
        ],
        ins=[hbm] * 6,
        outs=[hbm],
    )(
        by_component(parcel_speed),
        parcel_mass.reshape(across_i, across_j * capacity, LANES),
        by_component(offsets),
        by_component(cell_base),
        block_tile[0, 0].T,
        block_count[0],
    )
    message = lax.all_to_all(message.reshape(devices, rows, 1, LANES), SENT, split_axis=0, concat_axis=0, tiled=True)
    message = message.reshape(devices * rows, LANES)

    face = shape(fields, extent_x, extent_z)
    side = shape(fields, extent_y, extent_z)
    whole = vmem(gas_state.shape, f32)
    flat = (fields, extent_x * extent_y, extent_z)
    table, face_x0, face_x1, face_y0, face_y1 = call(
        table_kernel, (shape(FLOWS, tiles, LANES), side, side, face, face), flops=10**7
    )(gas_state)

    def shifted(value, axis, step):
        count = lax.axis_size(axis)
        pairs = [(i, i + step) for i in range(count) if 0 <= i + step < count]
        return lax.ppermute(value, axis, pairs)

    halo = (
        shifted(face_x1, "gx", 1), shifted(face_x0, "gx", -1), shifted(face_y1, "yz", 1), shifted(face_y0, "yz", -1)
    )
    returned, result, ids = call(
        functools.partial(update_kernel, rows=rows, capacity=capacity),
        (
            shape(across_i, across_j * capacity * FLOWS, LANES),
            shape(across_i, across_j * capacity * FLOWS, LANES),
            shape(devices, LANES, dtype=i32),
        ),
        scratch=[
            vmem((FLOWS * SUB * SUB, LANES), f32),
            vmem((capacity, devices, LANES), i32),
            dma((devices // SUB,)),
        ],
        flops=10**7,
        ins=[vmem, vmem],
        outs=[hbm, vmem, vmem],
    )(message, table)
    returned = lax.all_to_all(
        returned.reshape(devices, capacity * FLOWS, 1, LANES), RETURNED, split_axis=0, concat_axis=0, tiled=True
    )
    gas_next = call(
        functools.partial(deposit_kernel, rows=rows, capacity=capacity),
        shape(*flat),
        scratch=[
            vmem((tiles * SUB, LANES), f32),
            vmem((blocks * SUB, LANES), f32),
            pltpu.SMEM((devices, LANES), i32),
            whole,
            vmem(flat, f32),
            dma((2 + extent_x // TILE_X,)),
        ],
        flops=3 * 10**7,
        ins=[vmem, vmem, vmem, hbm] + [vmem] * 4,
        outs=[hbm],
    )(ids, message, result, gas_state, *halo)
    speed_next, mass_next = call(
        unpack_kernel,
        (shape(devices, vector, 1, LANES), shape(devices, capacity, 1, LANES)),
        scratch=[dma((2,))],
        ins=[vmem],
        outs=[hbm, hbm],
    )(returned)
    speed_next = speed_next.reshape(devices, 3, capacity, LANES).transpose(0, 2, 1, 3)
    return gas_next.reshape(gas_state.shape), speed_next.reshape(parcel_speed.shape), mass_next.reshape(parcel_mass.shape)


def solution(mesh):
    in_specs = (
        P(None, "gx", "yz", None),
        P("gx", "yz", None, None, None, None),
        P("gx", "yz", None, None, None),
        P("gx", "yz", None, None, None, None),
        P("gx", "yz", None, None, None, None),
        P("gx", "yz", None, None),
        P("gx", "yz", None),
    )
    out_specs = (
        P(None, "gx", "yz", None),
        P("gx", "yz", None, None, None, None),
        P("gx", "yz", None, None, None),
    )
    return jax.shard_map(step, mesh=mesh, in_specs=in_specs, out_specs=out_specs, check_vma=False)
```

```python
import functools

import jax
import jax.numpy as jnp
from jax import lax
from jax.experimental import pallas as pl
from jax.experimental.pallas import tpu as pltpu
from jax.sharding import PartitionSpec as P


TILE_X = 4
TILE_Y = 4
TILE_Z = 8
DIFFUSION = 0.1
CELL_MASS = 4.0
DRAG_RATE = 0.5
EVAPORATION = 0.3
LATENT_HEAT = 2.0

LANES = 128
SUB = 8
GRANULES = LANES // TILE_Z
FLOWS = 4
SENT = ("yz", "gx")
RETURNED = ("gx", "yz")


def roll(x, shift, axis):
    shift = shift % x.shape[axis]
    return pltpu.roll(x, shift, axis) if shift else x


def pick(x, rows):
    return jnp.take_along_axis(x, rows, axis=0, mode="promise_in_bounds")


def exchange(upper, lower):
    row = lax.broadcasted_iota(jnp.int32, (SUB, LANES), 0)
    granule = lax.broadcasted_iota(jnp.int32, (SUB, LANES), 1) // TILE_Z
    half = LANES // 2
    turned = [
        pltpu.roll(x, shift, 1, stride=TILE_Z, stride_axis=0) for x, shift in ((upper, 0), (lower, half))
    ]
    back = SUB - 1 - row
    pair = []
    for part in range(2):
        wanted = (granule - back - SUB * part) % GRANULES
        mixed = jnp.where(wanted < SUB, pick(turned[0], wanted % SUB), pick(turned[1], wanted % SUB))
        shift = (-TILE_Z * (SUB - 1) - half * part) % LANES
        pair.append(pick(pltpu.roll(mixed, shift, 1, stride=TILE_Z, stride_axis=0), back))
    return pair


def pack_kernel(
    speed, mass, offsets, cells, tile_ids, counts, message,
    speed_v, mass_v, offsets_v, cells_v, tile_ids_v, counts_v, ids_v, message_v, sems, *, rows, capacity, parts
):
    across_i = speed.shape[0]
    vector = 3 * capacity
    across_j = speed.shape[1] // vector
    each = across_j // parts
    sources = ((speed, speed_v, vector), (offsets, offsets_v, vector), (cells, cells_v, vector), (mass, mass_v, capacity))
    small = [
        pltpu.make_async_copy(tile_ids, tile_ids_v, sems.at[0]),
        pltpu.make_async_copy(counts, counts_v, sems.at[1]),
    ]
    taken = []
    for copy in small:
        copy.start()
    for part in range(parts):
        taken.append([])
        for n, (source, held, count) in enumerate(sources):
            place = pl.ds(part * each * count, each * count)
            copy = pltpu.make_async_copy(source.at[:, place], held.at[:, place], sems.at[2 + part * 5 + n])
            copy.start()
            taken[-1].append(copy)
    for copy in small:
        copy.wait()
    slot = lax.broadcasted_iota(jnp.int32, tile_ids_v.shape, 0)
    ids = jnp.where(slot < counts_v[...], tile_ids_v[...], -1).astype(jnp.float32)
    ids_v[...] = jnp.concatenate([ids, jnp.zeros((LANES - capacity, ids.shape[1]), jnp.float32)], axis=0).T

    sent = []
    for part in range(parts):
        for copy in taken[part]:
            copy.wait()
        for j in range(part * each, (part + 1) * each):
            for i in range(across_i):
                base = (j * across_i + i) * rows
                place = slice(j * vector, (j + 1) * vector)
                message_v[base : base + vector, :] = speed_v[i, place, :]
                message_v[base + vector : base + 2 * vector, :] = offsets_v[i, place, :]
                message_v[base + 2 * vector : base + 3 * vector, :] = cells_v[i, place, :].astype(jnp.float32)
                base += 3 * vector
                message_v[base : base + capacity, :] = mass_v[i, j * capacity : (j + 1) * capacity, :]
                owner = i * across_j + j
                message_v[base + capacity : base + capacity + 1, :] = ids_v[owner : owner + 1, :]
        place = pl.ds(part * each * across_i * rows, each * across_i * rows)
        copy = pltpu.make_async_copy(message_v.at[place], message.at[place], sems.at[2 + part * 5 + 4])
        copy.start()
        sent.append(copy)
    for copy in sent:
        copy.wait()


def table_kernel(gas, table, face_x0, face_x1, face_y0, face_y1):
    extent_x, extent_y, extent_z = gas.shape[1:]
    across_y = extent_y // TILE_Y
    across_z = extent_z // TILE_Z
    face_x0[...] = gas[:, 0]
    face_x1[...] = gas[:, extent_x - 1]
    face_y0[...] = gas[:, :, 0, :]
    face_y1[...] = gas[:, :, extent_y - 1, :]

    def per_a(a, carry):
        for f in range(FLOWS):
            for b in range(across_y):
                for h in range(extent_z // LANES):
                    lanes = slice(h * LANES, (h + 1) * LANES)
                    rows = slice(b * TILE_Y, (b + 1) * TILE_Y)
                    parts = []
                    for u in range(TILE_X):
                        piece = gas[f, a * TILE_X + u, rows, lanes]
                        if f == 3:
                            piece = piece - gas[4, a * TILE_X + u, rows, lanes]
                        parts.append(piece)
                    pair = exchange(jnp.concatenate(parts[:2], 0), jnp.concatenate(parts[2:], 0))
                    start = pl.multiple_of((a * across_y + b) * across_z + h * GRANULES, SUB)
                    table[f, pl.ds(start, SUB), :] = pair[0]
                    table[f, pl.ds(start + SUB, SUB), :] = pair[1]
        return carry

    lax.fori_loop(0, extent_x // TILE_X, per_a, 0)


def paired(ref, member, stride, offset, capacity):
    starts = [(member + n) * stride + offset for n in range(2)]
    return jnp.concatenate([ref[start : start + capacity, :] for start in starts], axis=0)


def columns(g, across_i, spread):
    size = SUB // across_i * spread
    return pl.ds(pl.multiple_of(g * size, SUB), size)


def update_kernel(
    message, table, result_hbm, result, ids_vmem, turned, sems, *, rows, capacity
):
    devices = message.shape[0] // rows
    group = SUB * rows
    for g in range(devices // SUB):
        ids_vmem[g * SUB : (g + 1) * SUB, :] = message[pl.ds(g * group + rows - 1, SUB, stride=rows), :].astype(jnp.int32)
    for k in range(capacity):
        turned[k] = roll(ids_vmem[...], -k, 1)
    corner = lax.broadcasted_iota(jnp.int32, (SUB, LANES), 0)
    high = [(corner & bit) != 0 for bit in (4, 2, 1)]
    least = [jnp.where(h, 0.0, 1.0) for h in high]
    slope = [jnp.where(h, 1.0, -1.0) for h in high]
    shift = (
        jnp.where(high[0], TILE_Y * TILE_Z, 0) + jnp.where(high[1], TILE_Z, 0) + jnp.where(high[2], 1, 0)
    )
    row = corner

    across_i = result.shape[0]
    spread = capacity * FLOWS

    def returned(g):
        place = columns(g, across_i, spread)
        return pltpu.make_async_copy(result.at[:, place], result_hbm.at[:, place], sems.at[g])

    def per_group(g, carry):
        out = result.at[:, columns(g, across_i, spread)]
        here = pl.ds(pl.multiple_of(g * SUB, SUB), SUB)
        numbers = [turned[k, here, :] for k in range(capacity)]
        part = message.at[pl.ds(pl.multiple_of(g * group, SUB), group)]
        for step in range(SUB // 2):

            def both(field):
                return paired(part, 2 * step, rows, field * capacity, capacity)

            first = ((both(6) * TILE_Y + both(7)) * TILE_Z + both(8)).astype(jnp.int32)
            alive = jnp.zeros((SUB, LANES), jnp.int32)
            made = [[] for _ in range(FLOWS)]
            for j in range(2 * capacity):
                i, k = 2 * step + j // capacity, j % capacity
                base = i * rows
                tile = numbers[k][i, 0]
                alive = jnp.where(row == j, tile, alive)
                safe = jnp.maximum(tile, 0)
                weight = None
                for dim in range(3):
                    start = base + (3 + dim) * capacity + k
                    fraction = part[start : start + 1, :]
                    along = least[dim] + slope[dim] * fraction
                    weight = along if weight is None else weight * along
                index = jnp.broadcast_to(first[j : j + 1], (SUB, LANES)) + shift
                for f in range(FLOWS):
                    held = jnp.broadcast_to(table[f, pl.ds(safe, 1), :], (SUB, LANES))
                    found = jnp.take_along_axis(held, index, axis=1, mode="promise_in_bounds")
                    made[f].append(found * weight)
            live = alive >= 0
            sampled = []
            for level in made:
                for size in (4, 2, 1):
                    keep = (row & size) == 0
                    half = len(level) // 2
                    level = [
                        jnp.where(keep, x, roll(y, size, 0)) + jnp.where(keep, roll(x, -size, 0), y)
                        for x, y in zip(level[:half], level[half:])
                    ]
                sampled.append(level[0])

            mass_old = both(9)
            radius = jnp.exp(jnp.log(mass_old) * (1.0 / 3.0))
            factor = DRAG_RATE / (radius * radius)
            share = 1.0 / (1.0 + factor)
            gap = sampled[3]
            soft = jnp.maximum(gap, 0.0) + jnp.log(1.0 + jnp.exp(-jnp.abs(gap)))
            mass_new = jnp.where(live, mass_old / (1.0 + EVAPORATION * soft / radius), mass_old)
            fields = [
                jnp.where(live, (both(f) + factor * sampled[f]) * share, both(f)) for f in range(3)
            ] + [mass_new]
            for n in range(2):
                i, start = (2 * step + n) % across_i, (2 * step + n) // across_i * spread
                for f in range(FLOWS):
                    rows_f = slice(start + f * capacity, start + (f + 1) * capacity)
                    out[i, rows_f, :] = fields[f][n * capacity : (n + 1) * capacity]
        returned(g).start()
        return carry

    lax.fori_loop(0, devices // SUB, per_group, 0, unroll=4)
    for g in range(devices // SUB):
        returned(g).wait()


def tent(position, cell):
    return jnp.maximum(0.0, 1.0 - jnp.abs(position - cell))


def deposit_kernel(
    ids_vmem, message, result, gas_hbm, from_x0, from_x1, from_y0, from_y1, gas_next,
    total, source, ids, gas, work, sems, *, rows, capacity
):
    fields, extent_x, extent_z = from_y0.shape
    extent_y = from_x0.shape[1]
    across_y = extent_y // TILE_Y
    across_z = extent_z // TILE_Z
    blocks = source.shape[0] // SUB
    group = SUB * rows
    spread = capacity * FLOWS
    across_i = result.shape[0]
    copy = pltpu.make_async_copy(ids_vmem, ids, sems.at[0])
    copy.start()
    fetch = pltpu.make_async_copy(gas_hbm, gas, sems.at[1])
    fetch.start()
    total[...] = jnp.zeros(total.shape, total.dtype)

    def per_group(g, carry):
        part = message.at[pl.ds(pl.multiple_of(g * group, SUB), group)]
        updated = result.at[:, columns(g, across_i, spread)]
        out = source.at[pl.ds(pl.multiple_of(g * SUB * SUB * capacity, SUB), SUB * SUB * capacity)]
        for step in range(SUB // 2):

            def before(field):
                return paired(part, 2 * step, rows, field * capacity, capacity)

            def after(field):
                found = []
                for member in (2 * step, 2 * step + 1):
                    i, start = member % across_i, member // across_i * spread + field * capacity
                    found.append(updated[i, start : start + capacity, :])
                return jnp.concatenate(found, axis=0)

            mass_old = before(9)
            vapour = mass_old - after(3)
            found = [mass_old * (before(f) - after(f)) + vapour * after(f) for f in range(3)] + [vapour]
            found += [before(3 + dim) + before(6 + dim) for dim in range(3)]
            for f, value in enumerate(found):
                out[pl.ds(2 * step * capacity * SUB + f, 2 * capacity, stride=SUB), :] = value
        return carry

    lax.fori_loop(0, blocks // (SUB * capacity), per_group, 0)
    row = lax.broadcasted_iota(jnp.int32, (SUB, LANES), 0)
    along_z = row.astype(jnp.float32)
    along_y = (row % TILE_Y).astype(jnp.float32)
    along_x = (row // TILE_Y).astype(jnp.float32)
    copy.wait()

    def one(n):
        tile = jnp.maximum(ids[n // capacity, n % capacity], 0)
        held = source[pl.ds(pl.multiple_of(n * SUB, SUB), SUB), :]
        given = held[0:FLOWS]
        coarse = given.astype(jnp.bfloat16).astype(jnp.float32)
        left = jnp.concatenate([given, given - coarse], axis=0).astype(jnp.bfloat16)
        x, y, z = held[4:5], held[5:6], held[6:7]
        weight_z = tent(z, along_z)
        weight_y = tent(y, along_y)
        planes = []
        for part in range(2):
            weight_xy = tent(x, along_x + 2.0 * part) * weight_y
            for i in range(SUB):
                planes.append(weight_xy[i : i + 1] * weight_z)
        stencil = jnp.concatenate(planes, axis=0)
        high = stencil.astype(jnp.bfloat16)
        low = (stencil - high.astype(jnp.float32)).astype(jnp.bfloat16)
        right = jnp.concatenate([high, low], axis=0)
        sums = lax.dot_general(left, right, (((1,), (1,)), ((), ())), preferred_element_type=jnp.float32)
        return pl.multiple_of(tile * SUB, SUB), sums[:, :LANES] + sums[:, LANES:]

    unroll = 16

    def per_step(step, carry):
        made = [one(step * unroll + n) for n in range(unroll)]
        for start, sums in made:
            total[pl.ds(start, SUB), :] += sums
        return carry

    lax.fori_loop(0, blocks // unroll, per_step, 0)

    fetch.wait()
    lane = lax.broadcasted_iota(jnp.int32, (extent_y, extent_z), 1)
    line = lax.broadcasted_iota(jnp.int32, (extent_y, extent_z), 0)

    def per_field(f, carry):
        for x in range(extent_x):
            centre = gas[f, x]
            beside = from_x0[f] if x == 0 else gas[f, x - 1]
            beside += from_x1[f] if x == extent_x - 1 else gas[f, x + 1]
            beside += jnp.where(line == 0, from_y0[f, x : x + 1, :], roll(centre, 1, 0))
            beside += jnp.where(line == extent_y - 1, from_y1[f, x : x + 1, :], roll(centre, -1, 0))
            beside += jnp.where(lane == 0, 0.0, roll(centre, 1, 1))
            beside += jnp.where(lane == extent_z - 1, 0.0, roll(centre, -1, 1))
            work[f, x * extent_y : (x + 1) * extent_y, :] = centre + DIFFUSION * (beside - 6.0 * centre)
        return carry

    lax.fori_loop(0, fields, per_field, 0)

    def sent(a):
        place = pl.ds(pl.multiple_of(a * TILE_X * extent_y, SUB), TILE_X * extent_y)
        return pltpu.make_async_copy(work.at[:, place], gas_next.at[:, place], sems.at[2 + a])

    def per_a(a, carry):
        held = work.at[:, pl.ds(pl.multiple_of(a * TILE_X * extent_y, SUB), TILE_X * extent_y)]
        for b in range(across_y):
            for h in range(extent_z // LANES):
                start = ((a * across_y + b) * across_z + h * GRANULES) * SUB
                part = total.at[pl.ds(pl.multiple_of(start, SUB), GRANULES * SUB)]
                lanes = slice(h * LANES, (h + 1) * LANES)
                for f in range(FLOWS):
                    pair = [
                        part[pl.ds(n * SUB * SUB + f, SUB, stride=SUB), :]
                        + part[pl.ds(n * SUB * SUB + f + FLOWS, SUB, stride=SUB), :]
                        for n in range(2)
                    ]
                    pair = [x * (1.0 / CELL_MASS) for x in exchange(*pair)]
                    for u in range(TILE_X):
                        piece = pair[u // 2][(u % 2) * TILE_Y : (u % 2 + 1) * TILE_Y]
                        spot = u * extent_y + b * TILE_Y
                        lines = slice(spot, spot + TILE_Y)
                        if f < 3:
                            held[f, lines, lanes] += piece
                        else:
                            held[3, lines, lanes] -= LATENT_HEAT * piece
                            held[4, lines, lanes] += piece
        sent(a).start()
        return carry

    lax.fori_loop(0, extent_x // TILE_X, per_a, 0)
    for a in range(extent_x // TILE_X):
        sent(a).wait()


def unpack_kernel(result, speed, mass, sems):
    vector = speed.shape[1]
    copies = [
        pltpu.make_async_copy(result.at[:, :vector], speed, sems.at[0]),
        pltpu.make_async_copy(result.at[:, vector:], mass, sems.at[1]),
    ]
    for copy in copies:
        copy.start()
    for copy in copies:
        copy.wait()


def specs(spaces):
    return [pl.BlockSpec(memory_space=space) for space in spaces]


def call(kernel, out_shape, scratch=(), flops=0, moved=0, ins=None, outs=None):
    extra = {}
    if ins is not None:
        extra["in_specs"] = specs(ins)
    if outs is not None:
        extra["out_specs"] = specs(outs) if len(outs) > 1 else specs(outs)[0]
        if pltpu.HBM in outs:
            shapes = out_shape if len(outs) > 1 else (out_shape,)
            shapes = [pltpu.HBM(o.shape, o.dtype) if space == pltpu.HBM else o for o, space in zip(shapes, outs)]
            out_shape = shapes if len(outs) > 1 else shapes[0]
    called = pl.pallas_call(
        kernel,
        out_shape=out_shape,
        scratch_shapes=scratch,
        cost_estimate=pl.CostEstimate(flops=flops, bytes_accessed=moved, transcendentals=0),
        compiler_params=pltpu.CompilerParams(vmem_limit_bytes=32 * 1024 * 1024),
        **extra,
    )

    def with_spaces(*values):
        if ins is not None:
            values = [
                pltpu.with_memory_space_constraint(v, space) if space == pltpu.HBM else v
                for v, space in zip(values, ins)
            ]
        return called(*values)

    return with_spaces


def step(gas_state, parcel_speed, parcel_mass, offsets, cell_base, block_tile, block_count):
    fields, extent_x, extent_y, extent_z = gas_state.shape
    devices, capacity = block_tile.shape[2:]
    rows = 10 * capacity + 1
    tiles = (extent_x // TILE_X) * (extent_y // TILE_Y) * (extent_z // TILE_Z)
    f32 = jnp.float32

    def shape(*dims, dtype=f32):
        return jax.ShapeDtypeStruct(dims, dtype)

    vector = 3 * capacity
    blocks = devices * capacity
    across_i, across_j = lax.axis_size("gx"), lax.axis_size("yz")
    parts = max(1, across_j // 2)
    i32 = jnp.int32
    hbm, vmem = pltpu.HBM, pltpu.VMEM
    dma = pltpu.SemaphoreType.DMA

    def by_component(value):
        return value[0, 0].transpose(0, 2, 1, 3).reshape(across_i, across_j * vector, LANES)

    message = call(
        functools.partial(pack_kernel, rows=rows, capacity=capacity, parts=parts),
        shape(devices * rows, LANES),
        scratch=[
            vmem((across_i, across_j * vector, LANES), f32),
            vmem((across_i, across_j * capacity, LANES), f32),
            vmem((across_i, across_j * vector, LANES), f32),
            vmem((across_i, across_j * vector, LANES), i32),
            vmem((capacity, devices), i32),
            vmem((1, devices), i32),
            vmem((devices, LANES), f32),
            vmem((devices * rows, LANES), f32),
            dma((2 + 5 * parts,)),
        ],
        ins=[hbm] * 6,
        outs=[hbm],
    )(
        by_component(parcel_speed),
        parcel_mass.reshape(across_i, across_j * capacity, LANES),
        by_component(offsets),
        by_component(cell_base),
        block_tile[0, 0].T,
        block_count[0],
    )
    message = lax.all_to_all(message.reshape(devices, rows, 1, LANES), SENT, split_axis=0, concat_axis=0, tiled=True)
    message = message.reshape(devices * rows, LANES)

    face = shape(fields, extent_x, extent_z)
    side = shape(fields, extent_y, extent_z)
    whole = vmem(gas_state.shape, f32)
    flat = (fields, extent_x * extent_y, extent_z)
    table, face_x0, face_x1, face_y0, face_y1 = call(
        table_kernel, (shape(FLOWS, tiles, LANES), side, side, face, face), flops=10**7
    )(gas_state)

    def shifted(value, axis, step):
        count = lax.axis_size(axis)
        pairs = [(i, i + step) for i in range(count) if 0 <= i + step < count]
        return lax.ppermute(value, axis, pairs)

    halo = (
        shifted(face_x1, "gx", 1), shifted(face_x0, "gx", -1), shifted(face_y1, "yz", 1), shifted(face_y0, "yz", -1)
    )
    returned, result, ids = call(
        functools.partial(update_kernel, rows=rows, capacity=capacity),
        (
            shape(across_i, across_j * capacity * FLOWS, LANES),
            shape(across_i, across_j * capacity * FLOWS, LANES),
            shape(devices, LANES, dtype=i32),
        ),
        scratch=[
            vmem((capacity, devices, LANES), i32),
            dma((devices // SUB,)),
        ],
        flops=10**7,
        ins=[vmem, vmem],
        outs=[hbm, vmem, vmem],
    )(message, table)
    returned = lax.all_to_all(
        returned.reshape(devices, capacity * FLOWS, 1, LANES), RETURNED, split_axis=0, concat_axis=0, tiled=True
    )
    gas_next = call(
        functools.partial(deposit_kernel, rows=rows, capacity=capacity),
        shape(*flat),
        scratch=[
            vmem((tiles * SUB, LANES), f32),
            vmem((blocks * SUB, LANES), f32),
            pltpu.SMEM((devices, LANES), i32),
            whole,
            vmem(flat, f32),
            dma((2 + extent_x // TILE_X,)),
        ],
        flops=3 * 10**7,
        ins=[vmem, vmem, vmem, hbm] + [vmem] * 4,
        outs=[hbm],
    )(ids, message, result, gas_state, *halo)
    speed_next, mass_next = call(
        unpack_kernel,
        (shape(devices, vector, 1, LANES), shape(devices, capacity, 1, LANES)),
        scratch=[dma((2,))],
        ins=[vmem],
        outs=[hbm, hbm],
    )(returned)
    speed_next = speed_next.reshape(devices, 3, capacity, LANES).transpose(0, 2, 1, 3)
    return gas_next.reshape(gas_state.shape), speed_next.reshape(parcel_speed.shape), mass_next.reshape(parcel_mass.shape)


def solution(mesh):
    in_specs = (
        P(None, "gx", "yz", None),
        P("gx", "yz", None, None, None, None),
        P("gx", "yz", None, None, None),
        P("gx", "yz", None, None, None, None),
        P("gx", "yz", None, None, None, None),
        P("gx", "yz", None, None),
        P("gx", "yz", None),
    )
    out_specs = (
        P(None, "gx", "yz", None),
        P("gx", "yz", None, None, None, None),
        P("gx", "yz", None, None, None),
    )
    return jax.shard_map(step, mesh=mesh, in_specs=in_specs, out_specs=out_specs, check_vma=False)
```

```python
import functools

import jax
import jax.numpy as jnp
from jax import lax
from jax.experimental import pallas as pl
from jax.experimental.pallas import tpu as pltpu
from jax.sharding import PartitionSpec as P


TILE_X = 4
TILE_Y = 4
TILE_Z = 8
DIFFUSION = 0.1
CELL_MASS = 4.0
DRAG_RATE = 0.5
EVAPORATION = 0.3
LATENT_HEAT = 2.0

LANES = 128
SUB = 8
GRANULES = LANES // TILE_Z
FLOWS = 4
SENT = ("yz", "gx")
RETURNED = ("gx", "yz")


def roll(x, shift, axis):
    shift = shift % x.shape[axis]
    return pltpu.roll(x, shift, axis) if shift else x


def pick(x, rows):
    return jnp.take_along_axis(x, rows, axis=0, mode="promise_in_bounds")


def exchange(upper, lower):
    row = lax.broadcasted_iota(jnp.int32, (SUB, LANES), 0)
    granule = lax.broadcasted_iota(jnp.int32, (SUB, LANES), 1) // TILE_Z
    half = LANES // 2
    turned = [
        pltpu.roll(x, shift, 1, stride=TILE_Z, stride_axis=0) for x, shift in ((upper, 0), (lower, half))
    ]
    back = SUB - 1 - row
    pair = []
    for part in range(2):
        wanted = (granule - back - SUB * part) % GRANULES
        mixed = jnp.where(wanted < SUB, pick(turned[0], wanted % SUB), pick(turned[1], wanted % SUB))
        shift = (-TILE_Z * (SUB - 1) - half * part) % LANES
        pair.append(pick(pltpu.roll(mixed, shift, 1, stride=TILE_Z, stride_axis=0), back))
    return pair


def pack_kernel(
    speed, mass, offsets, cells, tile_ids, counts, message,
    speed_v, mass_v, offsets_v, cells_v, tile_ids_v, counts_v, message_v, sems, *, rows, capacity, parts
):
    across_i = speed.shape[0]
    vector = 3 * capacity
    across_j = speed.shape[1] // vector
    each = across_j // parts
    sources = ((speed, speed_v, vector), (offsets, offsets_v, vector), (cells, cells_v, vector), (mass, mass_v, capacity))
    small = [
        pltpu.make_async_copy(tile_ids, tile_ids_v, sems.at[0]),
        pltpu.make_async_copy(counts, counts_v, sems.at[1]),
    ]
    taken = []
    for copy in small:
        copy.start()
    for part in range(parts):
        taken.append([])
        for n, (source, held, count) in enumerate(sources):
            place = pl.ds(part * each * count, each * count)
            copy = pltpu.make_async_copy(source.at[:, place], held.at[:, place], sems.at[2 + part * 5 + n])
            copy.start()
            taken[-1].append(copy)
    sent = []
    for part in range(parts):
        for copy in taken[part]:
            copy.wait()
        if part == 0:
            for copy in small:
                copy.wait()
            slot = lax.broadcasted_iota(jnp.int32, tile_ids_v.shape, 0)
            ids = jnp.where(slot < counts_v[...], tile_ids_v[...], -1).astype(jnp.float32)
            ids = jnp.concatenate([ids, jnp.zeros((LANES - capacity, ids.shape[1]), jnp.float32)], axis=0).T
        for j in range(part * each, (part + 1) * each):
            for i in range(across_i):
                base = (j * across_i + i) * rows
                place = slice(j * vector, (j + 1) * vector)
                message_v[base : base + vector, :] = speed_v[i, place, :]
                message_v[base + vector : base + 2 * vector, :] = offsets_v[i, place, :]
                message_v[base + 2 * vector : base + 3 * vector, :] = cells_v[i, place, :].astype(jnp.float32)
                base += 3 * vector
                message_v[base : base + capacity, :] = mass_v[i, j * capacity : (j + 1) * capacity, :]
                owner = i * across_j + j
                message_v[base + capacity : base + capacity + 1, :] = ids[owner : owner + 1, :]
        place = pl.ds(part * each * across_i * rows, each * across_i * rows)
        copy = pltpu.make_async_copy(message_v.at[place], message.at[place], sems.at[2 + part * 5 + 4])
        copy.start()
        sent.append(copy)
    for copy in sent:
        copy.wait()


def table_kernel(gas_hbm, table, face_x0, face_x1, face_y0, face_y1, gas, sem):
    copy = pltpu.make_async_copy(gas_hbm, gas, sem)
    copy.start()
    copy.wait()
    extent_x, extent_y, extent_z = gas.shape[1:]
    across_y = extent_y // TILE_Y
    across_z = extent_z // TILE_Z
    face_x0[...] = gas[:, 0]
    face_x1[...] = gas[:, extent_x - 1]
    face_y0[...] = gas[:, :, 0, :]
    face_y1[...] = gas[:, :, extent_y - 1, :]

    def per_a(a, carry):
        for f in range(FLOWS):
            for b in range(across_y):
                for h in range(extent_z // LANES):
                    lanes = slice(h * LANES, (h + 1) * LANES)
                    rows = slice(b * TILE_Y, (b + 1) * TILE_Y)
                    parts = []
                    for u in range(TILE_X):
                        piece = gas[f, a * TILE_X + u, rows, lanes]
                        if f == 3:
                            piece = piece - gas[4, a * TILE_X + u, rows, lanes]
                        parts.append(piece)
                    pair = exchange(jnp.concatenate(parts[:2], 0), jnp.concatenate(parts[2:], 0))
                    start = pl.multiple_of((a * across_y + b) * across_z + h * GRANULES, SUB)
                    table[f, pl.ds(start, SUB), :] = pair[0]
                    table[f, pl.ds(start + SUB, SUB), :] = pair[1]
        return carry

    lax.fori_loop(0, extent_x // TILE_X, per_a, 0)


def paired(ref, member, stride, offset, capacity):
    starts = [(member + n) * stride + offset for n in range(2)]
    return jnp.concatenate([ref[start : start + capacity, :] for start in starts], axis=0)


def columns(g, across_i, spread):
    size = SUB // across_i * spread
    return pl.ds(pl.multiple_of(g * size, SUB), size)


def update_kernel(
    message, table, result_hbm, result, ids_vmem, turned, sems, *, rows, capacity
):
    devices = message.shape[0] // rows
    group = SUB * rows
    for g in range(devices // SUB):
        ids_vmem[g * SUB : (g + 1) * SUB, :] = message[pl.ds(g * group + rows - 1, SUB, stride=rows), :].astype(jnp.int32)
    for k in range(capacity):
        turned[k] = roll(ids_vmem[...], -k, 1)
    corner = lax.broadcasted_iota(jnp.int32, (SUB, LANES), 0)
    high = [(corner & bit) != 0 for bit in (4, 2, 1)]
    least = [jnp.where(h, 0.0, 1.0) for h in high]
    slope = [jnp.where(h, 1.0, -1.0) for h in high]
    shift = (
        jnp.where(high[0], TILE_Y * TILE_Z, 0) + jnp.where(high[1], TILE_Z, 0) + jnp.where(high[2], 1, 0)
    )
    row = corner

    across_i = result.shape[0]
    spread = capacity * FLOWS

    def returned(g):
        place = columns(g, across_i, spread)
        return pltpu.make_async_copy(result.at[:, place], result_hbm.at[:, place], sems.at[g])

    def per_group(g, carry):
        out = result.at[:, columns(g, across_i, spread)]
        here = pl.ds(pl.multiple_of(g * SUB, SUB), SUB)
        numbers = [turned[k, here, :] for k in range(capacity)]
        part = message.at[pl.ds(pl.multiple_of(g * group, SUB), group)]
        for step in range(SUB // 2):

            def both(field):
                return paired(part, 2 * step, rows, field * capacity, capacity)

            first = ((both(6) * TILE_Y + both(7)) * TILE_Z + both(8)).astype(jnp.int32)
            alive = jnp.zeros((SUB, LANES), jnp.int32)
            made = [[] for _ in range(FLOWS)]
            for j in range(2 * capacity):
                i, k = 2 * step + j // capacity, j % capacity
                base = i * rows
                tile = numbers[k][i, 0]
                alive = jnp.where(row == j, tile, alive)
                safe = jnp.maximum(tile, 0)
                weight = None
                for dim in range(3):
                    start = base + (3 + dim) * capacity + k
                    fraction = part[start : start + 1, :]
                    along = least[dim] + slope[dim] * fraction
                    weight = along if weight is None else weight * along
                index = jnp.broadcast_to(first[j : j + 1], (SUB, LANES)) + shift
                for f in range(FLOWS):
                    held = jnp.broadcast_to(table[f, pl.ds(safe, 1), :], (SUB, LANES))
                    found = jnp.take_along_axis(held, index, axis=1, mode="promise_in_bounds")
                    made[f].append(found * weight)
            live = alive >= 0
            sampled = []
            for level in made:
                for size in (4, 2, 1):
                    keep = (row & size) == 0
                    half = len(level) // 2
                    level = [
                        jnp.where(keep, x, roll(y, size, 0)) + jnp.where(keep, roll(x, -size, 0), y)
                        for x, y in zip(level[:half], level[half:])
                    ]
                sampled.append(level[0])

            mass_old = both(9)
            radius = jnp.exp(jnp.log(mass_old) * (1.0 / 3.0))
            factor = DRAG_RATE / (radius * radius)
            share = 1.0 / (1.0 + factor)
            gap = sampled[3]
            soft = jnp.maximum(gap, 0.0) + jnp.log(1.0 + jnp.exp(-jnp.abs(gap)))
            mass_new = jnp.where(live, mass_old / (1.0 + EVAPORATION * soft / radius), mass_old)
            fields = [
                jnp.where(live, (both(f) + factor * sampled[f]) * share, both(f)) for f in range(3)
            ] + [mass_new]
            for n in range(2):
                i, start = (2 * step + n) % across_i, (2 * step + n) // across_i * spread
                for f in range(FLOWS):
                    rows_f = slice(start + f * capacity, start + (f + 1) * capacity)
                    out[i, rows_f, :] = fields[f][n * capacity : (n + 1) * capacity]
        returned(g).start()
        return carry

    lax.fori_loop(0, devices // SUB, per_group, 0, unroll=4)
    for g in range(devices // SUB):
        returned(g).wait()


def tent(position, cell):
    return jnp.maximum(0.0, 1.0 - jnp.abs(position - cell))


def deposit_kernel(
    ids_vmem, message, result, gas_hbm, from_x0, from_x1, from_y0, from_y1, gas_next,
    total, source, ids, gas, work, sems, *, rows, capacity
):
    fields, extent_x, extent_z = from_y0.shape
    extent_y = from_x0.shape[1]
    across_y = extent_y // TILE_Y
    across_z = extent_z // TILE_Z
    blocks = source.shape[0] // SUB
    group = SUB * rows
    spread = capacity * FLOWS
    across_i = result.shape[0]
    copy = pltpu.make_async_copy(ids_vmem, ids, sems.at[0])
    copy.start()
    fetch = pltpu.make_async_copy(gas_hbm, gas, sems.at[1])
    fetch.start()
    total[...] = jnp.zeros(total.shape, total.dtype)

    def per_group(g, carry):
        part = message.at[pl.ds(pl.multiple_of(g * group, SUB), group)]
        updated = result.at[:, columns(g, across_i, spread)]
        out = source.at[pl.ds(pl.multiple_of(g * SUB * SUB * capacity, SUB), SUB * SUB * capacity)]
        for step in range(SUB // 2):

            def before(field):
                return paired(part, 2 * step, rows, field * capacity, capacity)

            def after(field):
                found = []
                for member in (2 * step, 2 * step + 1):
                    i, start = member % across_i, member // across_i * spread + field * capacity
                    found.append(updated[i, start : start + capacity, :])
                return jnp.concatenate(found, axis=0)

            mass_old = before(9)
            vapour = mass_old - after(3)
            found = [mass_old * (before(f) - after(f)) + vapour * after(f) for f in range(3)] + [vapour]
            found += [before(3 + dim) + before(6 + dim) for dim in range(3)]
            for f, value in enumerate(found):
                out[pl.ds(2 * step * capacity * SUB + f, 2 * capacity, stride=SUB), :] = value
        return carry

    lax.fori_loop(0, blocks // (SUB * capacity), per_group, 0)
    row = lax.broadcasted_iota(jnp.int32, (SUB, LANES), 0)
    along_z = row.astype(jnp.float32)
    along_y = (row % TILE_Y).astype(jnp.float32)
    along_x = (row // TILE_Y).astype(jnp.float32)
    copy.wait()

    def one(n):
        tile = jnp.maximum(ids[n // capacity, n % capacity], 0)
        held = source[pl.ds(pl.multiple_of(n * SUB, SUB), SUB), :]
        given = held[0:FLOWS]
        coarse = given.astype(jnp.bfloat16).astype(jnp.float32)
        left = jnp.concatenate([given, given - coarse], axis=0).astype(jnp.bfloat16)
        x, y, z = held[4:5], held[5:6], held[6:7]
        weight_z = tent(z, along_z)
        weight_y = tent(y, along_y)
        planes = []
        for part in range(2):
            weight_xy = tent(x, along_x + 2.0 * part) * weight_y
            for i in range(SUB):
                planes.append(weight_xy[i : i + 1] * weight_z)
        stencil = jnp.concatenate(planes, axis=0)
        high = stencil.astype(jnp.bfloat16)
        low = (stencil - high.astype(jnp.float32)).astype(jnp.bfloat16)
        right = jnp.concatenate([high, low], axis=0)
        sums = lax.dot_general(left, right, (((1,), (1,)), ((), ())), preferred_element_type=jnp.float32)
        return pl.multiple_of(tile * SUB, SUB), sums[:, :LANES] + sums[:, LANES:]

    unroll = 16

    def per_step(step, carry):
        made = [one(step * unroll + n) for n in range(unroll)]
        for start, sums in made:
            total[pl.ds(start, SUB), :] += sums
        return carry

    lax.fori_loop(0, blocks // unroll, per_step, 0)

    fetch.wait()
    lane = lax.broadcasted_iota(jnp.int32, (extent_y, extent_z), 1)
    line = lax.broadcasted_iota(jnp.int32, (extent_y, extent_z), 0)

    def per_field(f, carry):
        for x in range(extent_x):
            centre = gas[f, x]
            beside = from_x0[f] if x == 0 else gas[f, x - 1]
            beside += from_x1[f] if x == extent_x - 1 else gas[f, x + 1]
            beside += jnp.where(line == 0, from_y0[f, x : x + 1, :], roll(centre, 1, 0))
            beside += jnp.where(line == extent_y - 1, from_y1[f, x : x + 1, :], roll(centre, -1, 0))
            beside += jnp.where(lane == 0, 0.0, roll(centre, 1, 1))
            beside += jnp.where(lane == extent_z - 1, 0.0, roll(centre, -1, 1))
            work[f, x * extent_y : (x + 1) * extent_y, :] = centre + DIFFUSION * (beside - 6.0 * centre)
        return carry

    lax.fori_loop(0, fields, per_field, 0)

    def sent(a):
        place = pl.ds(pl.multiple_of(a * TILE_X * extent_y, SUB), TILE_X * extent_y)
        return pltpu.make_async_copy(work.at[:, place], gas_next.at[:, place], sems.at[2 + a])

    def per_a(a, carry):
        held = work.at[:, pl.ds(pl.multiple_of(a * TILE_X * extent_y, SUB), TILE_X * extent_y)]
        for b in range(across_y):
            for h in range(extent_z // LANES):
                start = ((a * across_y + b) * across_z + h * GRANULES) * SUB
                part = total.at[pl.ds(pl.multiple_of(start, SUB), GRANULES * SUB)]
                lanes = slice(h * LANES, (h + 1) * LANES)
                for f in range(FLOWS):
                    pair = [
                        part[pl.ds(n * SUB * SUB + f, SUB, stride=SUB), :]
                        + part[pl.ds(n * SUB * SUB + f + FLOWS, SUB, stride=SUB), :]
                        for n in range(2)
                    ]
                    pair = [x * (1.0 / CELL_MASS) for x in exchange(*pair)]
                    for u in range(TILE_X):
                        piece = pair[u // 2][(u % 2) * TILE_Y : (u % 2 + 1) * TILE_Y]
                        spot = u * extent_y + b * TILE_Y
                        lines = slice(spot, spot + TILE_Y)
                        if f < 3:
                            held[f, lines, lanes] += piece
                        else:
                            held[3, lines, lanes] -= LATENT_HEAT * piece
                            held[4, lines, lanes] += piece
        sent(a).start()
        return carry

    lax.fori_loop(0, extent_x // TILE_X, per_a, 0)
    for a in range(extent_x // TILE_X):
        sent(a).wait()


def unpack_kernel(result, speed, mass, sems):
    vector = speed.shape[1]
    copies = [
        pltpu.make_async_copy(result.at[:, :vector], speed, sems.at[0]),
        pltpu.make_async_copy(result.at[:, vector:], mass, sems.at[1]),
    ]
    for copy in copies:
        copy.start()
    for copy in copies:
        copy.wait()


def specs(spaces):
    return [pl.BlockSpec(memory_space=space) for space in spaces]


def call(kernel, out_shape, scratch=(), flops=0, moved=0, ins=None, outs=None):
    extra = {}
    if ins is not None:
        extra["in_specs"] = specs(ins)
    if outs is not None:
        extra["out_specs"] = specs(outs) if len(outs) > 1 else specs(outs)[0]
        if pltpu.HBM in outs:
            shapes = out_shape if len(outs) > 1 else (out_shape,)
            shapes = [pltpu.HBM(o.shape, o.dtype) if space == pltpu.HBM else o for o, space in zip(shapes, outs)]
            out_shape = shapes if len(outs) > 1 else shapes[0]
    called = pl.pallas_call(
        kernel,
        out_shape=out_shape,
        scratch_shapes=scratch,
        cost_estimate=pl.CostEstimate(flops=flops, bytes_accessed=moved, transcendentals=0),
        compiler_params=pltpu.CompilerParams(vmem_limit_bytes=32 * 1024 * 1024),
        **extra,
    )

    def with_spaces(*values):
        if ins is not None:
            values = [
                pltpu.with_memory_space_constraint(v, space) if space == pltpu.HBM else v
                for v, space in zip(values, ins)
            ]
        return called(*values)

    return with_spaces


def step(gas_state, parcel_speed, parcel_mass, offsets, cell_base, block_tile, block_count):
    fields, extent_x, extent_y, extent_z = gas_state.shape
    devices, capacity = block_tile.shape[2:]
    rows = 10 * capacity + 1
    tiles = (extent_x // TILE_X) * (extent_y // TILE_Y) * (extent_z // TILE_Z)
    f32 = jnp.float32

    def shape(*dims, dtype=f32):
        return jax.ShapeDtypeStruct(dims, dtype)

    vector = 3 * capacity
    blocks = devices * capacity
    across_i, across_j = lax.axis_size("gx"), lax.axis_size("yz")
    parts = max(1, across_j // 2)
    i32 = jnp.int32
    hbm, vmem = pltpu.HBM, pltpu.VMEM
    dma = pltpu.SemaphoreType.DMA

    def by_component(value):
        return value[0, 0].transpose(0, 2, 1, 3).reshape(across_i, across_j * vector, LANES)

    message = call(
        functools.partial(pack_kernel, rows=rows, capacity=capacity, parts=parts),
        shape(devices * rows, LANES),
        scratch=[
            vmem((across_i, across_j * vector, LANES), f32),
            vmem((across_i, across_j * capacity, LANES), f32),
            vmem((across_i, across_j * vector, LANES), f32),
            vmem((across_i, across_j * vector, LANES), i32),
            vmem((capacity, devices), i32),
            vmem((1, devices), i32),
            vmem((devices * rows, LANES), f32),
            dma((2 + 5 * parts,)),
        ],
        ins=[hbm] * 6,
        outs=[hbm],
    )(
        by_component(parcel_speed),
        parcel_mass.reshape(across_i, across_j * capacity, LANES),
        by_component(offsets),
        by_component(cell_base),
        block_tile[0, 0].T,
        block_count[0],
    )
    message = lax.all_to_all(message.reshape(devices, rows, 1, LANES), SENT, split_axis=0, concat_axis=0, tiled=True)
    message = message.reshape(devices * rows, LANES)

    face = shape(fields, extent_x, extent_z)
    side = shape(fields, extent_y, extent_z)
    whole = vmem(gas_state.shape, f32)
    flat = (fields, extent_x * extent_y, extent_z)
    table, face_x0, face_x1, face_y0, face_y1 = call(
        table_kernel,
        (shape(FLOWS, tiles, LANES), side, side, face, face),
        scratch=[whole, dma(())],
        flops=10**7,
        ins=[hbm],
        outs=[vmem] * 5,
    )(gas_state)

    def shifted(value, axis, step):
        count = lax.axis_size(axis)
        pairs = [(i, i + step) for i in range(count) if 0 <= i + step < count]
        return lax.ppermute(value, axis, pairs)

    from_y0 = shifted(face_y1, "yz", 1)
    from_y1 = shifted(face_y0, "yz", -1)
    from_x0 = shifted(face_x1, "gx", 1)
    from_x1 = shifted(face_x0, "gx", -1)
    halo = (from_x0, from_x1, from_y0, from_y1)
    returned, result, ids = call(
        functools.partial(update_kernel, rows=rows, capacity=capacity),
        (
            shape(across_i, across_j * capacity * FLOWS, LANES),
            shape(across_i, across_j * capacity * FLOWS, LANES),
            shape(devices, LANES, dtype=i32),
        ),
        scratch=[
            vmem((capacity, devices, LANES), i32),
            dma((devices // SUB,)),
        ],
        flops=10**7,
        ins=[vmem, vmem],
        outs=[hbm, vmem, vmem],
    )(message, table)
    returned = lax.all_to_all(
        returned.reshape(devices, capacity * FLOWS, 1, LANES), RETURNED, split_axis=0, concat_axis=0, tiled=True
    )
    gas_next = call(
        functools.partial(deposit_kernel, rows=rows, capacity=capacity),
        shape(*flat),
        scratch=[
            vmem((tiles * SUB, LANES), f32),
            vmem((blocks * SUB, LANES), f32),
            pltpu.SMEM((devices, LANES), i32),
            whole,
            vmem(flat, f32),
            dma((2 + extent_x // TILE_X,)),
        ],
        flops=3 * 10**7,
        ins=[vmem, vmem, vmem, hbm] + [vmem] * 4,
        outs=[hbm],
    )(ids, message, result, gas_state, *halo)
    speed_next, mass_next = call(
        unpack_kernel,
        (shape(devices, vector, 1, LANES), shape(devices, capacity, 1, LANES)),
        scratch=[dma((2,))],
        ins=[vmem],
        outs=[hbm, hbm],
    )(returned)
    speed_next = speed_next.reshape(devices, 3, capacity, LANES).transpose(0, 2, 1, 3)
    return gas_next.reshape(gas_state.shape), speed_next.reshape(parcel_speed.shape), mass_next.reshape(parcel_mass.shape)


def solution(mesh):
    in_specs = (
        P(None, "gx", "yz", None),
        P("gx", "yz", None, None, None, None),
        P("gx", "yz", None, None, None),
        P("gx", "yz", None, None, None, None),
        P("gx", "yz", None, None, None, None),
        P("gx", "yz", None, None),
        P("gx", "yz", None),
    )
    out_specs = (
        P(None, "gx", "yz", None),
        P("gx", "yz", None, None, None, None),
        P("gx", "yz", None, None, None),
    )
    return jax.shard_map(step, mesh=mesh, in_specs=in_specs, out_specs=out_specs, check_vma=False)
```

```python
import functools

import jax
import jax.numpy as jnp
from jax import lax
from jax.experimental import pallas as pl
from jax.experimental.pallas import tpu as pltpu
from jax.sharding import PartitionSpec as P


TILE_X = 4
TILE_Y = 4
TILE_Z = 8
DIFFUSION = 0.1
CELL_MASS = 4.0
DRAG_RATE = 0.5
EVAPORATION = 0.3
LATENT_HEAT = 2.0

LANES = 128
SUB = 8
GRANULES = LANES // TILE_Z
FLOWS = 4
SENT = ("yz", "gx")
RETURNED = ("gx", "yz")


def roll(x, shift, axis):
    shift = shift % x.shape[axis]
    return pltpu.roll(x, shift, axis) if shift else x


def pick(x, rows):
    return jnp.take_along_axis(x, rows, axis=0, mode="promise_in_bounds")


def exchange(upper, lower):
    row = lax.broadcasted_iota(jnp.int32, (SUB, LANES), 0)
    granule = lax.broadcasted_iota(jnp.int32, (SUB, LANES), 1) // TILE_Z
    half = LANES // 2
    turned = [
        pltpu.roll(x, shift, 1, stride=TILE_Z, stride_axis=0) for x, shift in ((upper, 0), (lower, half))
    ]
    back = SUB - 1 - row
    pair = []
    for part in range(2):
        wanted = (granule - back - SUB * part) % GRANULES
        mixed = jnp.where(wanted < SUB, pick(turned[0], wanted % SUB), pick(turned[1], wanted % SUB))
        shift = (-TILE_Z * (SUB - 1) - half * part) % LANES
        pair.append(pick(pltpu.roll(mixed, shift, 1, stride=TILE_Z, stride_axis=0), back))
    return pair


def pack_kernel(
    speed, mass, offsets, cells, tile_ids, counts, message,
    speed_v, mass_v, offsets_v, cells_v, tile_ids_v, counts_v, message_v, sems, *, rows, capacity, parts
):
    across_i = speed.shape[0]
    vector = 3 * capacity
    across_j = speed.shape[1] // vector
    each = across_j // parts
    sources = ((speed, speed_v, vector), (offsets, offsets_v, vector), (cells, cells_v, vector), (mass, mass_v, capacity))
    small = [
        pltpu.make_async_copy(tile_ids, tile_ids_v, sems.at[0]),
        pltpu.make_async_copy(counts, counts_v, sems.at[1]),
    ]
    taken = []
    for part in range(parts):
        taken.append([])
        for n, (source, held, count) in enumerate(sources):
            place = pl.ds(part * each * count, each * count)
            copy = pltpu.make_async_copy(source.at[:, place], held.at[:, place], sems.at[2 + part * 5 + n])
            copy.start()
            taken[-1].append(copy)
        if part == 0:
            for copy in small:
                copy.start()
    sent = []
    for part in range(parts):
        for copy in taken[part]:
            copy.wait()
        if part == 0:
            for copy in small:
                copy.wait()
            slot = lax.broadcasted_iota(jnp.int32, tile_ids_v.shape, 0)
            ids = jnp.where(slot < counts_v[...], tile_ids_v[...], -1).astype(jnp.float32)
            ids = jnp.concatenate([ids, jnp.zeros((LANES - capacity, ids.shape[1]), jnp.float32)], axis=0).T
        for j in range(part * each, (part + 1) * each):
            for i in range(across_i):
                base = (j * across_i + i) * rows
                place = slice(j * vector, (j + 1) * vector)
                message_v[base : base + vector, :] = speed_v[i, place, :]
                message_v[base + vector : base + 2 * vector, :] = offsets_v[i, place, :]
                message_v[base + 2 * vector : base + 3 * vector, :] = cells_v[i, place, :].astype(jnp.float32)
                base += 3 * vector
                message_v[base : base + capacity, :] = mass_v[i, j * capacity : (j + 1) * capacity, :]
                owner = i * across_j + j
                message_v[base + capacity : base + capacity + 1, :] = ids[owner : owner + 1, :]
        place = pl.ds(part * each * across_i * rows, each * across_i * rows)
        copy = pltpu.make_async_copy(message_v.at[place], message.at[place], sems.at[2 + part * 5 + 4])
        copy.start()
        sent.append(copy)
    for copy in sent:
        copy.wait()


def table_kernel(gas_hbm, table, face_x0, face_x1, face_y0, face_y1, gas, sem):
    copy = pltpu.make_async_copy(gas_hbm, gas, sem)
    copy.start()
    copy.wait()
    extent_x, extent_y, extent_z = gas.shape[1:]
    across_y = extent_y // TILE_Y
    across_z = extent_z // TILE_Z
    face_x0[...] = gas[:, 0]
    face_x1[...] = gas[:, extent_x - 1]
    face_y0[...] = gas[:, :, 0, :]
    face_y1[...] = gas[:, :, extent_y - 1, :]

    def per_a(a, carry):
        for f in range(FLOWS):
            for b in range(across_y):
                for h in range(extent_z // LANES):
                    lanes = slice(h * LANES, (h + 1) * LANES)
                    rows = slice(b * TILE_Y, (b + 1) * TILE_Y)
                    parts = []
                    for u in range(TILE_X):
                        piece = gas[f, a * TILE_X + u, rows, lanes]
                        if f == 3:
                            piece = piece - gas[4, a * TILE_X + u, rows, lanes]
                        parts.append(piece)
                    pair = exchange(jnp.concatenate(parts[:2], 0), jnp.concatenate(parts[2:], 0))
                    start = pl.multiple_of((a * across_y + b) * across_z + h * GRANULES, SUB)
                    table[f, pl.ds(start, SUB), :] = pair[0]
                    table[f, pl.ds(start + SUB, SUB), :] = pair[1]
        return carry

    lax.fori_loop(0, extent_x // TILE_X, per_a, 0)


def paired(ref, member, stride, offset, capacity):
    starts = [(member + n) * stride + offset for n in range(2)]
    return jnp.concatenate([ref[start : start + capacity, :] for start in starts], axis=0)


def columns(g, across_i, spread):
    size = SUB // across_i * spread
    return pl.ds(pl.multiple_of(g * size, SUB), size)


def update_kernel(
    message, table, result_hbm, result, ids_vmem, turned, sems, *, rows, capacity
):
    devices = message.shape[0] // rows
    group = SUB * rows
    for g in range(devices // SUB):
        ids_vmem[g * SUB : (g + 1) * SUB, :] = message[pl.ds(g * group + rows - 1, SUB, stride=rows), :].astype(jnp.int32)
    for k in range(capacity):
        turned[k] = roll(ids_vmem[...], -k, 1)
    corner = lax.broadcasted_iota(jnp.int32, (SUB, LANES), 0)
    high = [(corner & bit) != 0 for bit in (4, 2, 1)]
    least = [jnp.where(h, 0.0, 1.0) for h in high]
    slope = [jnp.where(h, 1.0, -1.0) for h in high]
    shift = (
        jnp.where(high[0], TILE_Y * TILE_Z, 0) + jnp.where(high[1], TILE_Z, 0) + jnp.where(high[2], 1, 0)
    )
    row = corner

    across_i = result.shape[0]
    spread = capacity * FLOWS

    def returned(g):
        place = columns(g, across_i, spread)
        return pltpu.make_async_copy(result.at[:, place], result_hbm.at[:, place], sems.at[g])

    def per_group(g, carry):
        out = result.at[:, columns(g, across_i, spread)]
        here = pl.ds(pl.multiple_of(g * SUB, SUB), SUB)
        numbers = [turned[k, here, :] for k in range(capacity)]
        part = message.at[pl.ds(pl.multiple_of(g * group, SUB), group)]
        for step in range(SUB // 2):

            def both(field):
                return paired(part, 2 * step, rows, field * capacity, capacity)

            first = ((both(6) * TILE_Y + both(7)) * TILE_Z + both(8)).astype(jnp.int32)
            alive = jnp.zeros((SUB, LANES), jnp.int32)
            made = [[] for _ in range(FLOWS)]
            for j in range(2 * capacity):
                i, k = 2 * step + j // capacity, j % capacity
                base = i * rows
                tile = numbers[k][i, 0]
                alive = jnp.where(row == j, tile, alive)
                safe = jnp.maximum(tile, 0)
                weight = None
                for dim in range(3):
                    start = base + (3 + dim) * capacity + k
                    fraction = part[start : start + 1, :]
                    along = least[dim] + slope[dim] * fraction
                    weight = along if weight is None else weight * along
                index = jnp.broadcast_to(first[j : j + 1], (SUB, LANES)) + shift
                for f in range(FLOWS):
                    held = jnp.broadcast_to(table[f, pl.ds(safe, 1), :], (SUB, LANES))
                    found = jnp.take_along_axis(held, index, axis=1, mode="promise_in_bounds")
                    made[f].append(found * weight)
            live = alive >= 0
            sampled = []
            for level in made:
                for size in (4, 2, 1):
                    keep = (row & size) == 0
                    half = len(level) // 2
                    level = [
                        jnp.where(keep, x, roll(y, size, 0)) + jnp.where(keep, roll(x, -size, 0), y)
                        for x, y in zip(level[:half], level[half:])
                    ]
                sampled.append(level[0])

            mass_old = both(9)
            radius = jnp.exp(jnp.log(mass_old) * (1.0 / 3.0))
            factor = DRAG_RATE / (radius * radius)
            share = 1.0 / (1.0 + factor)
            gap = sampled[3]
            soft = jnp.maximum(gap, 0.0) + jnp.log(1.0 + jnp.exp(-jnp.abs(gap)))
            mass_new = jnp.where(live, mass_old / (1.0 + EVAPORATION * soft / radius), mass_old)
            fields = [
                jnp.where(live, (both(f) + factor * sampled[f]) * share, both(f)) for f in range(3)
            ] + [mass_new]
            for n in range(2):
                i, start = (2 * step + n) % across_i, (2 * step + n) // across_i * spread
                for f in range(FLOWS):
                    rows_f = slice(start + f * capacity, start + (f + 1) * capacity)
                    out[i, rows_f, :] = fields[f][n * capacity : (n + 1) * capacity]
        returned(g).start()
        return carry

    lax.fori_loop(0, devices // SUB, per_group, 0, unroll=4)
    for g in range(devices // SUB):
        returned(g).wait()


def tent(position, cell):
    return jnp.maximum(0.0, 1.0 - jnp.abs(position - cell))


def deposit_kernel(
    ids_vmem, message, result, gas_hbm, from_x0, from_x1, from_y0, from_y1, gas_next,
    total, source, ids, gas, work, sems, *, rows, capacity
):
    fields, extent_x, extent_z = from_y0.shape
    extent_y = from_x0.shape[1]
    across_y = extent_y // TILE_Y
    across_z = extent_z // TILE_Z
    blocks = source.shape[0] // SUB
    group = SUB * rows
    spread = capacity * FLOWS
    across_i = result.shape[0]
    copy = pltpu.make_async_copy(ids_vmem, ids, sems.at[0])
    copy.start()
    fetch = pltpu.make_async_copy(gas_hbm, gas, sems.at[1])
    fetch.start()
    total[...] = jnp.zeros(total.shape, total.dtype)

    def per_group(g, carry):
        part = message.at[pl.ds(pl.multiple_of(g * group, SUB), group)]
        updated = result.at[:, columns(g, across_i, spread)]
        out = source.at[pl.ds(pl.multiple_of(g * SUB * SUB * capacity, SUB), SUB * SUB * capacity)]
        for step in range(SUB // 2):

            def before(field):
                return paired(part, 2 * step, rows, field * capacity, capacity)

            def after(field):
                found = []
                for member in (2 * step, 2 * step + 1):
                    i, start = member % across_i, member // across_i * spread + field * capacity
                    found.append(updated[i, start : start + capacity, :])
                return jnp.concatenate(found, axis=0)

            mass_old = before(9)
            vapour = mass_old - after(3)
            found = [mass_old * (before(f) - after(f)) + vapour * after(f) for f in range(3)] + [vapour]
            found += [before(3 + dim) + before(6 + dim) for dim in range(3)]
            for f, value in enumerate(found):
                out[pl.ds(2 * step * capacity * SUB + f, 2 * capacity, stride=SUB), :] = value
        return carry

    lax.fori_loop(0, blocks // (SUB * capacity), per_group, 0)
    row = lax.broadcasted_iota(jnp.int32, (SUB, LANES), 0)
    along_z = row.astype(jnp.float32)
    along_y = (row % TILE_Y).astype(jnp.float32)
    along_x = (row // TILE_Y).astype(jnp.float32)
    copy.wait()

    def one(n):
        tile = jnp.maximum(ids[n // capacity, n % capacity], 0)
        held = source[pl.ds(pl.multiple_of(n * SUB, SUB), SUB), :]
        given = held[0:FLOWS]
        coarse = given.astype(jnp.bfloat16).astype(jnp.float32)
        left = jnp.concatenate([given, given - coarse], axis=0).astype(jnp.bfloat16)
        x, y, z = held[4:5], held[5:6], held[6:7]
        weight_z = tent(z, along_z)
        weight_y = tent(y, along_y)
        planes = []
        for part in range(2):
            weight_xy = tent(x, along_x + 2.0 * part) * weight_y
            for i in range(SUB):
                planes.append(weight_xy[i : i + 1] * weight_z)
        stencil = jnp.concatenate(planes, axis=0)
        high = stencil.astype(jnp.bfloat16)
        low = (stencil - high.astype(jnp.float32)).astype(jnp.bfloat16)
        right = jnp.concatenate([high, low], axis=0)
        sums = lax.dot_general(left, right, (((1,), (1,)), ((), ())), preferred_element_type=jnp.float32)
        return pl.multiple_of(tile * SUB, SUB), sums[:, :LANES] + sums[:, LANES:]

    unroll = 32

    def per_step(step, carry):
        made = [one(step * unroll + n) for n in range(unroll)]
        for start, sums in made:
            total[pl.ds(start, SUB), :] += sums
        return carry

    lax.fori_loop(0, blocks // unroll, per_step, 0)

    fetch.wait()
    lane = lax.broadcasted_iota(jnp.int32, (extent_y, extent_z), 1)
    line = lax.broadcasted_iota(jnp.int32, (extent_y, extent_z), 0)

    def per_field(f, carry):
        for x in range(extent_x):
            centre = gas[f, x]
            beside = from_x0[f] if x == 0 else gas[f, x - 1]
            beside += from_x1[f] if x == extent_x - 1 else gas[f, x + 1]
            beside += jnp.where(line == 0, from_y0[f, x : x + 1, :], roll(centre, 1, 0))
            beside += jnp.where(line == extent_y - 1, from_y1[f, x : x + 1, :], roll(centre, -1, 0))
            beside += jnp.where(lane == 0, 0.0, roll(centre, 1, 1))
            beside += jnp.where(lane == extent_z - 1, 0.0, roll(centre, -1, 1))
            work[f, x * extent_y : (x + 1) * extent_y, :] = centre + DIFFUSION * (beside - 6.0 * centre)
        return carry

    lax.fori_loop(0, fields, per_field, 0)

    def sent(a):
        place = pl.ds(pl.multiple_of(a * TILE_X * extent_y, SUB), TILE_X * extent_y)
        return pltpu.make_async_copy(work.at[:, place], gas_next.at[:, place], sems.at[2 + a])

    def per_a(a, carry):
        held = work.at[:, pl.ds(pl.multiple_of(a * TILE_X * extent_y, SUB), TILE_X * extent_y)]
        for b in range(across_y):
            for h in range(extent_z // LANES):
                start = ((a * across_y + b) * across_z + h * GRANULES) * SUB
                part = total.at[pl.ds(pl.multiple_of(start, SUB), GRANULES * SUB)]
                lanes = slice(h * LANES, (h + 1) * LANES)
                for f in range(FLOWS):
                    pair = [
                        part[pl.ds(n * SUB * SUB + f, SUB, stride=SUB), :]
                        + part[pl.ds(n * SUB * SUB + f + FLOWS, SUB, stride=SUB), :]
                        for n in range(2)
                    ]
                    pair = [x * (1.0 / CELL_MASS) for x in exchange(*pair)]
                    for u in range(TILE_X):
                        piece = pair[u // 2][(u % 2) * TILE_Y : (u % 2 + 1) * TILE_Y]
                        spot = u * extent_y + b * TILE_Y
                        lines = slice(spot, spot + TILE_Y)
                        if f < 3:
                            held[f, lines, lanes] += piece
                        else:
                            held[3, lines, lanes] -= LATENT_HEAT * piece
                            held[4, lines, lanes] += piece
        sent(a).start()
        return carry

    lax.fori_loop(0, extent_x // TILE_X, per_a, 0)
    for a in range(extent_x // TILE_X):
        sent(a).wait()


def unpack_kernel(result, speed, mass, sems):
    vector = speed.shape[1]
    copies = [
        pltpu.make_async_copy(result.at[:, :vector], speed, sems.at[0]),
        pltpu.make_async_copy(result.at[:, vector:], mass, sems.at[1]),
    ]
    for copy in copies:
        copy.start()
    for copy in copies:
        copy.wait()


def specs(spaces):
    return [pl.BlockSpec(memory_space=space) for space in spaces]


def call(kernel, out_shape, scratch=(), flops=0, moved=0, ins=None, outs=None):
    extra = {}
    if ins is not None:
        extra["in_specs"] = specs(ins)
    if outs is not None:
        extra["out_specs"] = specs(outs) if len(outs) > 1 else specs(outs)[0]
        if pltpu.HBM in outs:
            shapes = out_shape if len(outs) > 1 else (out_shape,)
            shapes = [pltpu.HBM(o.shape, o.dtype) if space == pltpu.HBM else o for o, space in zip(shapes, outs)]
            out_shape = shapes if len(outs) > 1 else shapes[0]
    called = pl.pallas_call(
        kernel,
        out_shape=out_shape,
        scratch_shapes=scratch,
        cost_estimate=pl.CostEstimate(flops=flops, bytes_accessed=moved, transcendentals=0),
        compiler_params=pltpu.CompilerParams(vmem_limit_bytes=32 * 1024 * 1024),
        **extra,
    )

    def with_spaces(*values):
        if ins is not None:
            values = [
                pltpu.with_memory_space_constraint(v, space) if space == pltpu.HBM else v
                for v, space in zip(values, ins)
            ]
        return called(*values)

    return with_spaces


def step(gas_state, parcel_speed, parcel_mass, offsets, cell_base, block_tile, block_count):
    fields, extent_x, extent_y, extent_z = gas_state.shape
    devices, capacity = block_tile.shape[2:]
    rows = 10 * capacity + 1
    tiles = (extent_x // TILE_X) * (extent_y // TILE_Y) * (extent_z // TILE_Z)
    f32 = jnp.float32

    def shape(*dims, dtype=f32):
        return jax.ShapeDtypeStruct(dims, dtype)

    vector = 3 * capacity
    blocks = devices * capacity
    across_i, across_j = lax.axis_size("gx"), lax.axis_size("yz")
    parts = max(1, across_j // 2)
    i32 = jnp.int32
    hbm, vmem = pltpu.HBM, pltpu.VMEM
    dma = pltpu.SemaphoreType.DMA

    def by_component(value):
        return value[0, 0].transpose(0, 2, 1, 3).reshape(across_i, across_j * vector, LANES)

    message = call(
        functools.partial(pack_kernel, rows=rows, capacity=capacity, parts=parts),
        shape(devices * rows, LANES),
        scratch=[
            vmem((across_i, across_j * vector, LANES), f32),
            vmem((across_i, across_j * capacity, LANES), f32),
            vmem((across_i, across_j * vector, LANES), f32),
            vmem((across_i, across_j * vector, LANES), i32),
            vmem((capacity, devices), i32),
            vmem((1, devices), i32),
            vmem((devices * rows, LANES), f32),
            dma((2 + 5 * parts,)),
        ],
        ins=[hbm] * 6,
        outs=[hbm],
    )(
        by_component(parcel_speed),
        parcel_mass.reshape(across_i, across_j * capacity, LANES),
        by_component(offsets),
        by_component(cell_base),
        block_tile[0, 0].T,
        block_count[0],
    )
    message = lax.all_to_all(message.reshape(devices, rows, 1, LANES), SENT, split_axis=0, concat_axis=0, tiled=True)
    message = message.reshape(devices * rows, LANES)

    face = shape(fields, extent_x, extent_z)
    side = shape(fields, extent_y, extent_z)
    whole = vmem(gas_state.shape, f32)
    flat = (fields, extent_x * extent_y, extent_z)
    table, face_x0, face_x1, face_y0, face_y1 = call(
        table_kernel,
        (shape(FLOWS, tiles, LANES), side, side, face, face),
        scratch=[whole, dma(())],
        flops=10**7,
        ins=[hbm],
        outs=[vmem] * 5,
    )(gas_state)

    def shifted(value, axis, step):
        count = lax.axis_size(axis)
        pairs = [(i, i + step) for i in range(count) if 0 <= i + step < count]
        return lax.ppermute(value, axis, pairs)

    halo = (
        shifted(face_x1, "gx", 1), shifted(face_x0, "gx", -1), shifted(face_y1, "yz", 1), shifted(face_y0, "yz", -1)
    )
    returned, result, ids = call(
        functools.partial(update_kernel, rows=rows, capacity=capacity),
        (
            shape(across_i, across_j * capacity * FLOWS, LANES),
            shape(across_i, across_j * capacity * FLOWS, LANES),
            shape(devices, LANES, dtype=i32),
        ),
        scratch=[
            vmem((capacity, devices, LANES), i32),
            dma((devices // SUB,)),
        ],
        flops=10**7,
        ins=[vmem, vmem],
        outs=[hbm, vmem, vmem],
    )(message, table)
    returned = lax.all_to_all(
        returned.reshape(devices, capacity * FLOWS, 1, LANES), RETURNED, split_axis=0, concat_axis=0, tiled=True
    )
    gas_next = call(
        functools.partial(deposit_kernel, rows=rows, capacity=capacity),
        shape(*flat),
        scratch=[
            vmem((tiles * SUB, LANES), f32),
            vmem((blocks * SUB, LANES), f32),
            pltpu.SMEM((devices, LANES), i32),
            whole,
            vmem(flat, f32),
            dma((2 + extent_x // TILE_X,)),
        ],
        flops=3 * 10**7,
        ins=[vmem, vmem, vmem, hbm] + [vmem] * 4,
        outs=[hbm],
    )(ids, message, result, gas_state, *halo)
    speed_next, mass_next = call(
        unpack_kernel,
        (shape(devices, vector, 1, LANES), shape(devices, capacity, 1, LANES)),
        scratch=[dma((2,))],
        ins=[vmem],
        outs=[hbm, hbm],
    )(returned)
    speed_next = speed_next.reshape(devices, 3, capacity, LANES).transpose(0, 2, 1, 3)
    return gas_next.reshape(gas_state.shape), speed_next.reshape(parcel_speed.shape), mass_next.reshape(parcel_mass.shape)


def solution(mesh):
    in_specs = (
        P(None, "gx", "yz", None),
        P("gx", "yz", None, None, None, None),
        P("gx", "yz", None, None, None),
        P("gx", "yz", None, None, None, None),
        P("gx", "yz", None, None, None, None),
        P("gx", "yz", None, None),
        P("gx", "yz", None),
    )
    out_specs = (
        P(None, "gx", "yz", None),
        P("gx", "yz", None, None, None, None),
        P("gx", "yz", None, None, None),
    )
    return jax.shard_map(step, mesh=mesh, in_specs=in_specs, out_specs=out_specs, check_vma=False)
```
